128 devices in a mesh: gx: 4 (over z_lo, core), gy: 16 (over x, y), gz: 2 (over z_hi).
Axes of the slice: x: 4, y: 4, z: 4 (z_hi: 2, z_lo: 2; z = z_hi * 2 + z_lo), core: 2. Of those that a mesh axis runs over, the one named last changes fastest.
Arguments:
- eigvecs: bfloat16 [64, 128, 96, 512], P('gx', 'gy', 'gz'), may hold values from -7 to 7, as said below
- material: float32 [2, 64, 128, 96], P(None, 'gx', 'gy', 'gz'), may hold values from 0.5 to 2
Outputs:
- stiffness: float32 [512, 512], P(('gx', 'gy', 'gz'))
- mass_matrix: float32 [512, 512], P(('gx', 'gy', 'gz'))
The draws below stay inside these ranges and needn't reach their ends.
Inputs may be any that keep to these rules, and one draw needn't show every extreme that they name: `eigvecs`: entries are a rough part plus a part that varies slowly over the grid.
All inputs are finite; a program needn't handle non-finite values.
Results may differ from the reference program's by a relative error of at most 0.0003.
Values may be sent and summed in bfloat16 or wider, within the bound.
No kernel may reach another device: no remote copies, remote signals or barrier semaphores. Data moves between devices by JAX's collectives and lax.ppermute only.
A program may use at most 128 MiB of HBM per device.

```python
import math
import jax
import jax.numpy as jnp
from jax import lax

K = 512
NX = 64
NY = 128
NZ = 96


def draw_eigvecs(key, part):
    keys = jax.random.split(key, 7)
    rough = jnp.clip(jax.random.normal(keys[0], (NX, NY, NZ, K), jnp.float32), -4.0, 4.0)
    amplitude = 2.0
    freq_x = jax.random.randint(keys[1], (K,), 1, 4).astype(jnp.float32)
    freq_y = jax.random.randint(keys[2], (K,), 1, 4).astype(jnp.float32)
    freq_z = jax.random.randint(keys[3], (K,), 1, 4).astype(jnp.float32)
    phase_x = jax.random.uniform(keys[4], (K,), jnp.float32)
    phase_y = jax.random.uniform(keys[5], (K,), jnp.float32)
    phase_z = jax.random.uniform(keys[6], (K,), jnp.float32)
    coord_x = jnp.arange(NX, dtype=jnp.float32)[:, None] / NX
    coord_y = jnp.arange(NY, dtype=jnp.float32)[:, None] / NY
    coord_z = jnp.arange(NZ, dtype=jnp.float32)[:, None] / NZ
    wave_x = jnp.cos(2.0 * jnp.pi * (coord_x * freq_x + phase_x))
    wave_y = jnp.cos(2.0 * jnp.pi * (coord_y * freq_y + phase_y))
    wave_z = jnp.cos(2.0 * jnp.pi * (coord_z * freq_z + phase_z))
    smooth = wave_x[:, None, None, :] * wave_y[None, :, None, :] * wave_z[None, None, :, :]
    return (rough + amplitude * smooth).astype(jnp.bfloat16)


def shard_levels(own_key, shape, cuts, low, top_value):
    factor_of = 1.0
    for dim, shards_of in cuts:
        heights = jax.random.uniform(jax.random.fold_in(jax.random.fold_in(own_key, 6), dim), (shards_of,), jnp.float32, low / len(cuts), top_value / len(cuts))
        factor_of = factor_of * jnp.repeat(jnp.exp(heights), shape[dim] // shards_of).reshape((-1,) + (1,) * (len(shape) - 1 - dim))
    return factor_of


def setup_inputs(seed: int = 0) -> dict:
    streams_of = jax.random.split(jax.random.key(seed), 3)
    eigvecs = draw_eigvecs(jax.random.fold_in(streams_of[2], 71), 0)
    material = jnp.clip(jnp.exp(math.log(2.0) - 1.3862944 * jax.random.uniform(streams_of[1], (2, NX, NY, NZ), jnp.float32) ** shard_levels(streams_of[1], (2, NX, NY, NZ), ((1, 4), (2, 16), (3, 2)), -0.2, 0.2)), 0.5, 2.0)
    return {"eigvecs": eigvecs, "material": material}


stencil_offsets = [(dx, dy, dz) for dx in (-1, 0, 1) for dy in (-1, 0, 1) for dz in (-1, 0, 1) if (dx, dy, dz) != (0, 0, 0)]


def coupling(offset):
    nonzero = sum(abs(entry) for entry in offset)
    return 0.25 * 0.5 ** (nonzero - 1)


def mass_weight(offset):
    weight = 1.0
    for entry in offset:
        weight = weight * (4.0 / 6.0 if entry == 0 else 1.0 / 6.0)
    return weight


def apply_operators(padded, padded_material):
    size_x = padded.shape[0] - 2
    size_y = padded.shape[1] - 2
    size_z = padded.shape[2] - 2
    centre = padded[1:-1, 1:-1, 1:-1].astype(jnp.float32)
    kappa_centre = padded_material[0, 1:-1, 1:-1, 1:-1]
    rho_centre = padded_material[1, 1:-1, 1:-1, 1:-1]
    stiff_sum = jnp.zeros(centre.shape, jnp.float32)
    mass_sum = mass_weight((0, 0, 0)) * rho_centre[..., None] * centre
    for offset in stencil_offsets:
        lower = (1 + offset[0], 1 + offset[1], 1 + offset[2])
        shifted = padded[lower[0]:lower[0] + size_x, lower[1]:lower[1] + size_y, lower[2]:lower[2] + size_z].astype(jnp.float32)
        kappa_side = padded_material[0, lower[0]:lower[0] + size_x, lower[1]:lower[1] + size_y, lower[2]:lower[2] + size_z]
        rho_side = padded_material[1, lower[0]:lower[0] + size_x, lower[1]:lower[1] + size_y, lower[2]:lower[2] + size_z]
        stiff_sum = stiff_sum + (coupling(offset) * 0.5 * (kappa_centre + kappa_side))[..., None] * (centre - shifted)
        mass_sum = mass_sum + (mass_weight(offset) * 0.5 * (rho_centre + rho_side))[..., None] * shifted
    return stiff_sum.astype(jnp.bfloat16), mass_sum.astype(jnp.bfloat16)


def reference(eigvecs, material):
    cells = NX * NY * NZ
    block_cols = 32
    padded_material = jnp.pad(material, ((0, 0), (1, 1), (1, 1), (1, 1)))
    flat_vectors = eigvecs.reshape(cells, K)

    def column_block(block_index):
        first_col = block_index * block_cols
        col_block = lax.dynamic_slice_in_dim(eigvecs, first_col, block_cols, 3)
        padded = jnp.pad(col_block, ((1, 1), (1, 1), (1, 1), (0, 0)))
        stiff_vecs, mass_vecs = apply_operators(padded, padded_material)
        dims = (((0,), (0,)), ((), ()))
        stiff_cols = lax.dot_general(flat_vectors, stiff_vecs.reshape(cells, block_cols), dims, preferred_element_type=jnp.float32)
        mass_cols = lax.dot_general(flat_vectors, mass_vecs.reshape(cells, block_cols), dims, preferred_element_type=jnp.float32)
        return stiff_cols, mass_cols

    stiff_blocks, mass_blocks = lax.map(column_block, jnp.arange(K // block_cols, dtype=jnp.int32))
    stiffness = jnp.transpose(stiff_blocks, (1, 0, 2)).reshape(K, K) / cells
    mass_matrix = jnp.transpose(mass_blocks, (1, 0, 2)).reshape(K, K) / cells
    return stiffness, mass_matrix
```

```python
import jax
import jax.numpy as jnp
from jax import lax
from jax.experimental import pallas as pl
from jax.experimental.pallas import tpu as pltpu
from jax.sharding import PartitionSpec as P

ALL = ("gx", "gy", "gz")
NGX, NGY, NGZ = 4, 16, 2
SX, SY, SZ, K = 16, 8, 48, 512
PLANES, LINES = SX + 1, SY + 1
GROUPS = (((8, 0, 1, 2, 3), (0, 1, 2)), ((2, 3, 4, 5, 6), (3, 4, 5)), ((5, 6, 7, 8, 0), (6, 7, 8)))
CELLS = LINES * SZ


def linear(x, y, z):
    return (x * NGY + y) * NGZ + z


def pairs(move):
    out = []
    for x in range(NGX):
        for y in range(NGY):
            for z in range(NGZ):
                to = move(x, y, z)
                if 0 <= to[0] < NGX and 0 <= to[1] < NGY and 0 <= to[2] < NGZ:
                    out.append((linear(x, y, z), linear(*to)))
    return out


def send(value, move):
    return lax.ppermute(value, ALL, pairs(move))


def to_z(x, y, z):
    return (x, y, 1 - z)


def to_x(x, y, z):
    return (x - 1, y, z)


def to_y(x, y, z):
    return (x, y + 1, z) if x % 2 else (x, y - 1, z)


def line_links(odd):
    here = jnp.arange(LINES)[:, None]
    there = jnp.arange(LINES)[None, :]
    near = (jnp.abs(here - there) == 1) & (here != 8) & (there != 8)
    inner = jnp.where(odd, 0, 7)
    near = near | ((here == 8) & (there == inner)) | ((there == 8) & (here == inner))
    same = (here == there) & (here != 8)
    return near.astype(jnp.float32), same.astype(jnp.float32)


def band_matrices(odd, upper):
    row = lax.broadcasted_iota(jnp.int32, (3, 6 * SZ, 256), 1)
    col = lax.broadcasted_iota(jnp.int32, (3, 6 * SZ, 256), 2)
    grp = lax.broadcasted_iota(jnp.int32, (3, 6 * SZ, 256), 0)
    mid = jnp.where(row < 3 * SZ, 2.0, 4.0)
    cell = row % (3 * SZ)
    line_out = grp * 3 + cell // SZ
    z_out = cell % SZ
    halo = col >= 5 * SZ
    slot = col // SZ
    first = jnp.where(grp == 0, 8, jnp.where(grp == 1, 2, 5))
    line_in = jnp.where(halo, col - 5 * SZ, (first + slot) % LINES)
    z_in = jnp.where(halo, jnp.where(upper, -1, SZ), col % SZ)
    z_gap = jnp.abs(z_out - z_in)
    z_part = jnp.where(z_gap == 0, mid, jnp.where(z_gap == 1, 1.0, 0.0))
    both_own = (line_out != 8) & (line_in != 8)
    inner = jnp.where(odd, 0, 7)
    near = (both_own & (jnp.abs(line_out - line_in) == 1)) | (
        ((line_out == 8) & (line_in == inner)) | ((line_in == 8) & (line_out == inner))
    )
    same = both_own & (line_out == line_in)
    y_part = jnp.where(same, mid, jnp.where(near, 1.0, 0.0))
    return (y_part * z_part).astype(jnp.bfloat16)


def coefficients(kappa, rho, kappa_z, odd, upper):
    zero = jnp.zeros((PLANES, LINES, 1), jnp.float32)
    edge = kappa_z[..., None]
    below = jnp.concatenate([jnp.where(upper, edge, zero), kappa[..., :-1]], axis=2)
    above = jnp.concatenate([kappa[..., 1:], jnp.where(upper, zero, edge)], axis=2)
    f = 2.0 * kappa + below + above
    own_line = (jnp.arange(LINES) != 8)[None, :, None]
    own_plane = (jnp.arange(PLANES) != SX)[:, None, None]
    zline = jnp.zeros((PLANES, 1, SZ), jnp.float32)
    own = f[:, :8]
    halo = f[:, 8:9]
    lower = jnp.concatenate([jnp.where(odd, halo, zline), own[:, :-1]], axis=1)
    higher = jnp.concatenate([own[:, 1:], jnp.where(odd, zline, halo)], axis=1)
    inner = jnp.where(odd, own[:, 0:1], own[:, 7:8])
    f = jnp.concatenate([2.0 * own + lower + higher, inner], axis=1)
    zplane = jnp.zeros((1, LINES, SZ), jnp.float32)
    before = jnp.concatenate([zplane, f[:-1]], axis=0)
    after = jnp.concatenate([f[1:], zplane], axis=0)
    f = jnp.where(own_plane, 2.0 * f, 0.0) + before + after
    alpha = jnp.where(own_plane & own_line, 2.0 * kappa, 0.0) + f * (1.0 / 32.0)
    table = jnp.stack([alpha, kappa * (1.0 / 16.0), rho * (1.0 / 216.0)], axis=1)
    table = table.reshape(PLANES, 3, CELLS)
    return jnp.pad(table, ((0, 0), (0, 5), (0, 512 - CELLS)))


def project_kernel(v_hbm, xh_hbm, yh_hbm, zt_ref, coef_ref, band_ref, out_ref, ve, w2, t2, u, acc, sem):
    def copies(p):
        own = pltpu.make_async_copy(v_hbm.at[p], ve.at[p, pl.ds(0, 8)], sem.at[p])
        return own

    halo_copies = [
        pltpu.make_async_copy(xh_hbm, ve.at[SX, pl.ds(0, 8)], sem.at[SX]),
        pltpu.make_async_copy(yh_hbm, ve.at[:, 8], sem.at[SX + 1]),
    ]
    for c in halo_copies:
        c.start()
    for p in range(SX):
        copies(p).start()
    acc[...] = jnp.zeros(acc.shape, jnp.float32)
    w2[2] = jnp.zeros(w2.shape[1:], jnp.float32)
    t2[2] = jnp.zeros(t2.shape[1:], jnp.float32)
    for c in halo_copies:
        c.wait()

    def filter_plane(p, slot):
        ztile = zt_ref[p]
        for g, (ins, outs) in enumerate(GROUPS):
            block = jnp.concatenate([ve[p, l] for l in ins] + [ztile], axis=0)
            r = jnp.dot(band_ref[g], block, preferred_element_type=jnp.float32)
            w2[slot, pl.ds(g * 3 * SZ, 3 * SZ)] = r[: 3 * SZ]
            t2[slot, pl.ds(g * 3 * SZ, 3 * SZ)] = r[3 * SZ :]

    def project_plane(p, prev, cur, nxt):
        coef = jnp.transpose(coef_ref[p])
        for l in range(LINES):
            rows = pl.ds(l * SZ, SZ)
            c = coef[l * SZ : (l + 1) * SZ]
            wide = (SZ, K)
            if nxt is None:
                w3 = w2[prev, rows]
                t3 = t2[prev, rows]
            else:
                mid = w2[cur, rows]
                w3 = w2[prev, rows] + (mid + mid) + w2[nxt, rows]
                t3 = t2[prev, rows] + 4.0 * t2[cur, rows] + t2[nxt, rows]
            v = ve[p, l].astype(jnp.float32)
            alpha = jnp.broadcast_to(c[:, 0:1], wide)
            kap = jnp.broadcast_to(c[:, 1:2], wide)
            rho = jnp.broadcast_to(c[:, 2:3], wide)
            u[rows, 0:K] = (alpha * v - kap * w3).astype(jnp.bfloat16)
            u[rows, K : 2 * K] = (rho * t3).astype(jnp.bfloat16)
        left = ve[p].reshape(CELLS, K)
        acc[...] += lax.dot_general(
            left, u[...], (((0,), (0,)), ((), ())), preferred_element_type=jnp.float32
        )

    copies(0).wait()
    filter_plane(0, 0)

    def step(p, carry):
        @pl.when(p + 1 < SX)
        def _():
            copies(p + 1).wait()

        prev = lax.rem(p + 2, 3)
        cur = lax.rem(p, 3)
        nxt = lax.rem(p + 1, 3)
        filter_plane(p + 1, nxt)
        project_plane(p, prev, cur, nxt)
        return carry

    lax.fori_loop(0, SX, step, 0)
    project_plane(SX, (SX + 2) % 3, None, None)
    for half in range(2):
        for i in range(4):
            for j in range(i, 4):
                a = acc[i * 128 : (i + 1) * 128, half * K + j * 128 : half * K + (j + 1) * 128]
                b = acc[j * 128 : (j + 1) * 128, half * K + i * 128 : half * K + (i + 1) * 128]
                s = a + b.T
                out_ref[i * 128 : (i + 1) * 128, half * K + j * 128 : half * K + (j + 1) * 128] = s
                if i != j:
                    out_ref[j * 128 : (j + 1) * 128, half * K + i * 128 : half * K + (i + 1) * 128] = s.T


def project(v, xh, yh, zt, coef, band):
    hbm = pl.BlockSpec(memory_space=pl.ANY)
    vmem = pl.BlockSpec(memory_space=pltpu.VMEM)
    return pl.pallas_call(
        project_kernel,
        out_shape=jax.ShapeDtypeStruct((K, 2 * K), jnp.float32),
        in_specs=[hbm, hbm, hbm, vmem, vmem, vmem],
        out_specs=vmem,
        scratch_shapes=[
            pltpu.VMEM((PLANES, LINES, SZ, K), jnp.bfloat16),
            pltpu.VMEM((3, CELLS, K), jnp.float32),
            pltpu.VMEM((3, CELLS, K), jnp.float32),
            pltpu.VMEM((CELLS, 2 * K), jnp.bfloat16),
            pltpu.VMEM((K, 2 * K), jnp.float32),
            pltpu.SemaphoreType.DMA((SX + 2,)),
        ],
        compiler_params=pltpu.CompilerParams(vmem_limit_bytes=40 * 1024 * 1024),
        cost_estimate=pl.CostEstimate(flops=13_000_000_000, transcendentals=0, bytes_accessed=12_000_000),
        name="project",
    )(v, xh, yh, zt, coef, band)


def pick(x, index, dim):
    return lax.dynamic_index_in_dim(x, index, dim, keepdims=False)


def reduce_to_owner(part):
    ix = lax.axis_index("gx")
    iy = lax.axis_index("gy")
    core = ix % 2
    z_lo = ix // 2
    z_hi = lax.axis_index("gz")
    cx = iy // 4
    cy = iy % 4
    v = part.reshape(2, 2, 4, 4, 8, 2 * K)
    v = pick(v, core, 1) + send(pick(v, 1 - core, 1), lambda x, y, z: (x ^ 1, y, z))
    v = pick(v, z_lo, 0) + send(pick(v, 1 - z_lo, 0), lambda x, y, z: (x ^ 2, y, z))
    parts = [send(pick(v, (cx + d) % 4, 0), lambda x, y, z, d=d: (x, (y + 4 * d) % 16, z)) for d in (1, 2, 3)]
    v = pick(v, cx, 0) + parts[0] + parts[1] + parts[2]
    parts = [send(pick(v, (cy + d) % 4, 0), lambda x, y, z, d=d: (x, y // 4 * 4 + (y + d) % 4, z)) for d in (1, 2, 3)]
    v = pick(v, cy, 0) + parts[0] + parts[1] + parts[2]
    v = v.reshape(2, 4, 2 * K)
    return pick(v, z_hi, 0) + send(pick(v, 1 - z_hi, 0), to_z)


def per_device(eigvecs, material):
    ix = lax.axis_index("gx")
    odd = ix % 2 == 1
    upper = lax.axis_index("gz") == 1
    rho = material[1]
    kappa = material[0]
    kz = send(jnp.where(upper, kappa[:, :, 0], kappa[:, :, SZ - 1]), to_z)
    zh = send(jnp.where(upper, eigvecs[:, :, 0], eigvecs[:, :, SZ - 1]), to_z)
    mx = send(jnp.concatenate([kappa[0], rho[0], kz[0][:, None]], axis=1), to_x)
    vx = send(jnp.concatenate([eigvecs[0].reshape(SY * SZ, K), zh[0]], axis=0), to_x)
    xh = vx[: SY * SZ].reshape(SY, SZ, K)
    xz = vx[SY * SZ :]
    kappa = jnp.concatenate([kappa, mx[None, :, :SZ]], axis=0)
    rho = jnp.concatenate([rho, mx[None, :, SZ : 2 * SZ]], axis=0)
    kz = jnp.concatenate([kz, mx[None, :, 2 * SZ]], axis=0)
    zt = jnp.concatenate([zh, xz[None]], axis=0)
    side = jnp.where(odd, SY - 1, 0)
    my = send(jnp.concatenate([pick(kappa, side, 1), pick(rho, side, 1), pick(kz, side, 1)[:, None]], axis=1), to_y)
    yrow = jnp.concatenate([pick(eigvecs, side, 1), pick(xh, side, 0)[None]], axis=0)
    vy = send(jnp.concatenate([yrow.reshape(PLANES * SZ, K), pick(zt, side, 1)], axis=0), to_y)
    yh = vy[: PLANES * SZ].reshape(PLANES, SZ, K)
    yz = vy[PLANES * SZ :]
    kappa = jnp.concatenate([kappa, my[:, None, :SZ]], axis=1)
    rho = jnp.concatenate([rho, my[:, None, SZ : 2 * SZ]], axis=1)
    kz = jnp.concatenate([kz, my[:, None, 2 * SZ]], axis=1)
    zt = jnp.concatenate([zt, yz[:, None], jnp.zeros((PLANES, 16 - LINES, K), jnp.bfloat16)], axis=1)
    coef = coefficients(kappa, rho, kz, odd, upper)
    band = band_matrices(odd, upper)
    part = project(eigvecs, xh, yh, zt, coef, band)
    total = SX * SY * SZ * NGX * NGY * NGZ
    summed = reduce_to_owner(part) * (0.5 / total)
    return summed[:, :K], summed[:, K:]


def solution(mesh):
    return jax.shard_map(
        per_device,
        mesh=mesh,
        in_specs=(P("gx", "gy", "gz", None), P(None, "gx", "gy", "gz")),
        out_specs=(P(ALL, None), P(ALL, None)),
        check_vma=False,
    )
```

```python
import jax
import jax.numpy as jnp
from jax import lax
from jax.experimental import pallas as pl
from jax.experimental.pallas import tpu as pltpu
from jax.sharding import PartitionSpec as P

ALL = ("gx", "gy", "gz")
NGX, NGY, NGZ = 4, 16, 2
SX, SY, SZ, K = 16, 8, 48, 512
NEAR = (((0, 1, 2, 3), (0, 1, 2)), ((2, 3, 4, 5, 6), (3, 4, 5)), ((5, 6, 7), (6,)))
EDGE = ((6, 7, 8), (7, 8))
INNER = 7 * SZ
OUTER = 2 * SZ
BATCH = 3


def linear(x, y, z):
    return (x * NGY + y) * NGZ + z


def send(value, move):
    links = []
    for x in range(NGX):
        for y in range(NGY):
            for z in range(NGZ):
                to = move(x, y, z)
                if 0 <= to[0] < NGX and 0 <= to[1] < NGY and 0 <= to[2] < NGZ:
                    links.append((linear(x, y, z), linear(*to)))
    return lax.ppermute(value, ALL, links)


def to_z(x, y, z):
    return (x, y, 1 - z)


def to_x(x, y, z):
    return (x - 1, y, z)


def to_y(x, y, z):
    return (x, y + 1, z) if x % 2 else (x, y - 1, z)


def band_matrix(lines_in, lines_out, upper):
    size = len(lines_out) * SZ
    wide = len(lines_in) * SZ + 16
    row = lax.broadcasted_iota(jnp.int32, (2 * size, wide), 0)
    col = lax.broadcasted_iota(jnp.int32, (2 * size, wide), 1)
    mid = jnp.where(row < size, 2.0, 4.0)
    cell = row % size
    line_out = lines_out[0] + cell // SZ
    halo = col >= len(lines_in) * SZ
    line_in = jnp.where(halo, col - len(lines_in) * SZ, lines_in[0] + col // SZ)
    z_in = jnp.where(halo, jnp.where(upper, -1, SZ), col % SZ)
    z_gap = jnp.abs(cell % SZ - z_in)
    z_part = jnp.where(z_gap == 0, mid, jnp.where(z_gap == 1, 1.0, 0.0))
    y_gap = jnp.abs(line_out - line_in)
    y_part = jnp.where((y_gap == 0) & (line_out != 8), mid, jnp.where(y_gap == 1, 1.0, 0.0))
    return (y_part * z_part).astype(jnp.bfloat16)


def apply_band(band, lines, ztile, size):
    block = jnp.concatenate(lines + [ztile], axis=0)
    r = jnp.dot(band, block, preferred_element_type=jnp.float32)
    return r[:size], r[size:]


def kappa_yz(kappa, lines):
    f = 2.0 * kappa + pltpu.roll(kappa, 1, 1) + pltpu.roll(kappa, 127, 1)
    rows = lax.broadcasted_iota(jnp.int32, f.shape, 0)
    below = jnp.where(rows == 0, 0.0, pltpu.roll(f, 1, 0))
    above = jnp.where(rows == f.shape[0] - 1, 0.0, pltpu.roll(f, f.shape[0] - 1, 0))
    mid = jnp.where(rows == 8, 0.0, 2.0 * f)
    return mid + below + above


def weights(kappa, rho, f, plane_own):
    own = 2.0 * kappa if plane_own else jnp.zeros_like(kappa)
    rows = lax.broadcasted_iota(jnp.int32, f.shape, 0)
    alpha = jnp.where(rows == 8, 0.0, own) + f * (1.0 / 32.0)
    return jnp.concatenate([alpha, kappa * (1.0 / 16.0), rho * (1.0 / 216.0)], axis=0).T[:SZ]


def store_products(u, row, v, w3, t3, c, line, stride):
    wide = (SZ, K)
    alpha = jnp.broadcast_to(c[:, line : line + 1], wide)
    kap = jnp.broadcast_to(c[:, stride + line : stride + line + 1], wide)
    rho = jnp.broadcast_to(c[:, 2 * stride + line : 2 * stride + line + 1], wide)
    u[row : row + SZ, 0:K] = (alpha * v.astype(jnp.float32) - kap * w3).astype(jnp.bfloat16)
    u[row : row + SZ, K : 2 * K] = (rho * t3).astype(jnp.bfloat16)


def gram(left, right):
    return lax.dot_general(left, right, (((0,), (0,)), ((), ())), preferred_element_type=jnp.float32)


def line_index(odd, c):
    return c + odd * (7 - 2 * c)


def inner_kernel(odd_ref, v_hbm, zt_ref, mat_ref, band0, band1, band2, out_ref, ve, w2, t2, u, sem):
    odd = odd_ref[0]
    bands = (band0, band1, band2)
    cuts = ((0, 2), (2, 4), (4, 7), (7, 10), (10, 13), (13, 16))
    loads = []
    for n, (a, b) in enumerate(cuts):
        loads.append(
            [
                pltpu.make_async_copy(
                    v_hbm.at[pl.ds(a, b - a), line_index(odd, c)], ve.at[pl.ds(a, b - a), c], sem.at[n, c]
                )
                for c in range(8)
            ]
        )
        for load in loads[-1]:
            load.start()

    def arrive(n):
        for load in loads[n]:
            load.wait()

    def filter_plane(p):
        slot = p % 4
        for g, (ins, outs) in enumerate(NEAR):
            size = len(outs) * SZ
            a, b = apply_band(bands[g][...], [ve[p, l] for l in ins], zt_ref[p], size)
            w2[slot, outs[0] * SZ : outs[0] * SZ + size] = a
            t2[slot, outs[0] * SZ : outs[0] * SZ + size] = b

    yz = {}

    def kappa_of(p):
        if p not in yz:
            yz[p] = kappa_yz(mat_ref[0, p], 8)
        return yz[p]

    def make_products(p, buf, base):
        f = 2.0 * kappa_of(p) + kappa_of(p + 1)
        if p:
            f = f + kappa_of(p - 1)
        c = weights(mat_ref[0, p], mat_ref[1, p], f, True)
        for l in range(7):
            rows = slice(l * SZ, (l + 1) * SZ)
            mid = w2[p % 4, rows]
            w3 = (mid + mid) + w2[(p + 1) % 4, rows]
            t3 = 4.0 * t2[p % 4, rows] + t2[(p + 1) % 4, rows]
            if p:
                w3 = w3 + w2[(p - 1) % 4, rows]
                t3 = t3 + t2[(p - 1) % 4, rows]
            store_products(u.at[buf], base + l * SZ, ve[p, l], w3, t3, c, l, 8)

    arrive(0)
    filter_plane(0)
    for k in range(5):
        arrive(k + 1)
        if k == 0:
            filter_plane(1)
        for q in range(BATCH):
            p = BATCH * k + q
            if p + 1 > 1:
                filter_plane(p + 1)
            make_products(p, k % 2, q * INNER)
        left = jnp.concatenate([ve[BATCH * k + q, 0:7].reshape(INNER, K) for q in range(BATCH)], axis=0)
        m = gram(left, u[k % 2])
        if k == 0:
            out_ref[...] = m
        else:
            out_ref[...] += m


def tile_row(x, y, z_lo, core):
    a = {0: (0, 0), 3: (0, 1), 1: (1, 0), 2: (1, 1)}
    xa, xb = a[x]
    ya, yb = a[y]
    bits = (z_lo, xa, xb, ya, yb) if core == 0 else (xa, z_lo, ya, xb, yb)
    at = core
    for bit in bits:
        at = at * 2 + bit
    return at * 8


def outer_kernel(
    odd_ref, m_ref, v_hbm, xh_hbm, ym_hbm, ye_hbm, zt_ref, mat_ref, band0, band1, band2, band3, out_ref,
    v6, v78, v14, v15, v16, w78, t78, w06, t06, u, sem,
):
    odd = odd_ref[0]
    bands = (band0, band1, band2)
    loads = [
        pltpu.make_async_copy(v_hbm.at[pl.ds(0, 15), line_index(odd, 6)], v6, sem.at[0]),
        pltpu.make_async_copy(v_hbm.at[pl.ds(0, 15), line_index(odd, 7)], v78.at[:, 0], sem.at[1]),
        pltpu.make_async_copy(ym_hbm.at[pl.ds(0, 15)], v78.at[:, 1], sem.at[2]),
        pltpu.make_async_copy(ym_hbm.at[15], v15.at[8], sem.at[3]),
        pltpu.make_async_copy(ye_hbm.at[pl.ds(0, SZ)], v16.at[8], sem.at[4]),
    ]
    for c in range(8):
        loads.append(pltpu.make_async_copy(v_hbm.at[15, line_index(odd, c)], v15.at[c], sem.at[5 + c]))
        loads.append(pltpu.make_async_copy(xh_hbm.at[line_index(odd, c)], v16.at[c], sem.at[13 + c]))
        if c < 6:
            loads.append(pltpu.make_async_copy(v_hbm.at[14, line_index(odd, c)], v14.at[c], sem.at[21 + c]))
    for load in loads:
        load.start()
    for load in loads:
        load.wait()

    def line(p, l):
        if p == 15:
            return v15[l]
        if p == 16:
            return v16[l]
        if l >= 7:
            return v78[p, l - 7]
        if l == 6:
            return v6[p]
        return v14[l]

    def filter_near(p):
        for g, (ins, outs) in enumerate(NEAR):
            size = len(outs) * SZ
            a, b = apply_band(bands[g][...], [line(p, l) for l in ins], zt_ref[p], size)
            w06[p - 14, outs[0] * SZ : outs[0] * SZ + size] = a
            t06[p - 14, outs[0] * SZ : outs[0] * SZ + size] = b

    def filter_edge(p):
        a, b = apply_band(band3[...], [line(p, l) for l in EDGE[0]], zt_ref[p], OUTER)
        w78[p] = a
        t78[p] = b

    def along_x(ref, p, lo, hi, rows, mid):
        if p == hi:
            return ref[p - 1 - lo, rows]
        r = mid * ref[p - lo, rows] + ref[p + 1 - lo, rows]
        if p > 0:
            r = r + ref[p - 1 - lo, rows]
        return r

    yz = [kappa_yz(mat_ref[0, p], 16) for p in range(17)]
    for p in range(17):
        filter_edge(p)
        if p >= 14:
            filter_near(p)
    for p in range(17):
        if p == 16:
            f = yz[15]
        else:
            f = 2.0 * yz[p] + yz[p + 1]
            if p:
                f = f + yz[p - 1]
        c = weights(mat_ref[0, p], mat_ref[1, p], f, p != 16)
        for l in range(0 if p >= 15 else 7, 9):
            if p < 15:
                row = p * OUTER + (l - 7) * SZ
            else:
                row = 15 * OUTER + (p - 15) * 9 * SZ + l * SZ
            if l >= 7:
                rows = slice((l - 7) * SZ, (l - 6) * SZ)
                w3 = along_x(w78, p, 0, 16, rows, 2.0)
                t3 = along_x(t78, p, 0, 16, rows, 4.0)
            else:
                rows = slice(l * SZ, (l + 1) * SZ)
                w3 = along_x(w06, p, 14, 16, rows, 2.0)
                t3 = along_x(t06, p, 14, 16, rows, 4.0)
            store_products(u, row, line(p, l), w3, t3, c, l, 16)
    left = jnp.concatenate(
        [v78[...].reshape(15 * OUTER, K), v15[...].reshape(9 * SZ, K), v16[...].reshape(9 * SZ, K)], axis=0
    )
    m_ref[...] += gram(left, u[...])

    def put(i, j, half, s):
        for x in range(4):
            for y in range(4):
                t = (x * 4 + y) * 8
                at = tile_row(x, y, i // 2, i % 2)
                out_ref[at : at + 8, half * K + j * 128 : half * K + (j + 1) * 128] = s[t : t + 8]

    for half in range(2):
        for i in range(4):
            for j in range(i, 4):
                a = m_ref[i * 128 : (i + 1) * 128, half * K + j * 128 : half * K + (j + 1) * 128]
                b = m_ref[j * 128 : (j + 1) * 128, half * K + i * 128 : half * K + (i + 1) * 128]
                s = a + b.T
                put(i, j, half, s)
                if i != j:
                    put(j, i, half, s.T)


HBM = pl.BlockSpec(memory_space=pl.ANY)
VMEM = pl.BlockSpec(memory_space=pltpu.VMEM)
SMEM = pl.BlockSpec(memory_space=pltpu.SMEM)


def inner_part(odd, v, zt, mat, bands):
    return pl.pallas_call(
        inner_kernel,
        out_shape=jax.ShapeDtypeStruct((K, 2 * K), jnp.float32),
        in_specs=[SMEM, HBM, VMEM, VMEM, VMEM, VMEM, VMEM],
        out_specs=VMEM,
        scratch_shapes=[
            pltpu.VMEM((SX, SY, SZ, K), jnp.bfloat16),
            pltpu.VMEM((4, INNER, K), jnp.float32),
            pltpu.VMEM((4, INNER, K), jnp.float32),
            pltpu.VMEM((2, BATCH * INNER, 2 * K), jnp.bfloat16),
            pltpu.SemaphoreType.DMA((6, 8)),
        ],
        compiler_params=pltpu.CompilerParams(vmem_limit_bytes=36 * 1024 * 1024),
        cost_estimate=pl.CostEstimate(flops=9_000_000_000, transcendentals=0, bytes_accessed=10_000_000),
        name="inner",
    )(odd, v, zt, mat, *bands)


def outer_part(odd, m, v, xh, ym, ye, zt, mat, bands):
    return pl.pallas_call(
        outer_entry,
        out_shape=jax.ShapeDtypeStruct((K, 2 * K), jnp.float32),
        in_specs=[SMEM, VMEM, HBM, HBM, HBM, HBM, VMEM, VMEM, VMEM, VMEM, VMEM, VMEM],
        out_specs=VMEM,
        scratch_shapes=[
            pltpu.VMEM((15, SZ, K), jnp.bfloat16),
            pltpu.VMEM((15, 2, SZ, K), jnp.bfloat16),
            pltpu.VMEM((6, SZ, K), jnp.bfloat16),
            pltpu.VMEM((9, SZ, K), jnp.bfloat16),
            pltpu.VMEM((9, SZ, K), jnp.bfloat16),
            pltpu.VMEM((17, OUTER, K), jnp.float32),
            pltpu.VMEM((17, OUTER, K), jnp.float32),
            pltpu.VMEM((3, INNER, K), jnp.float32),
            pltpu.VMEM((3, INNER, K), jnp.float32),
            pltpu.VMEM((15 * OUTER + 18 * SZ, 2 * K), jnp.bfloat16),
            pltpu.SemaphoreType.DMA((27,)),
            pltpu.VMEM((K, 2 * K), jnp.float32),
        ],
        compiler_params=pltpu.CompilerParams(vmem_limit_bytes=48 * 1024 * 1024),
        cost_estimate=pl.CostEstimate(flops=4_000_000_000, transcendentals=0, bytes_accessed=6_000_000),
        name="outer",
    )(odd, m, v, xh, ym, ye, zt, mat, *bands)


def outer_entry(odd_ref, m_in, *rest):
    *rest, acc = rest
    acc[...] = m_in[...]
    outer_kernel(odd_ref, acc, *rest)


def pick(x, index, dim):
    return lax.dynamic_index_in_dim(x, index, dim, keepdims=False)


def reduce_to_owner(part):
    ix = lax.axis_index("gx")
    iy = lax.axis_index("gy")
    core = ix % 2
    z_lo = ix // 2
    z_hi = lax.axis_index("gz")

    def bits(r):
        return ((r == 1) | (r == 2)).astype(jnp.int32), (r >= 2).astype(jnp.int32)

    def flip_z(x, y, z):
        return (x ^ 2, y, z)

    def flip_xa(x, y, z):
        return (x, (y // 4 ^ 1) * 4 + y % 4, z)

    def flip_xb(x, y, z):
        return (x, (3 - y // 4) * 4 + y % 4, z)

    def flip_ya(x, y, z):
        return (x, y ^ 1, z)

    def flip_yb(x, y, z):
        return (x, y // 4 * 4 + 3 - y % 4, z)

    xa, xb = bits(iy // 4)
    ya, yb = bits(iy % 4)
    stages = (
        (core, core, lambda x, y, z: (x ^ 1, y, z), lambda x, y, z: (x ^ 1, y, z)),
        (z_lo, xa, flip_z, flip_xa),
        (xa, z_lo, flip_xa, flip_z),
        (xb, ya, flip_xb, flip_ya),
        (ya, xb, flip_ya, flip_xb),
        (yb, yb, flip_yb, flip_yb),
    )
    v = part
    for even_bit, odd_bit, even_move, odd_move in stages:
        bit = jnp.where(core == 0, even_bit, odd_bit)
        v = v.reshape(2, v.shape[0] // 2, 2 * K)
        v = pick(v, bit, 0) + send(
            pick(v, 1 - bit, 0),
            lambda x, y, z, e=even_move, o=odd_move: o(x, y, z) if x % 2 else e(x, y, z),
        )
    v = v.reshape(2, 4, 2 * K)
    return pick(v, z_hi, 0) + send(pick(v, 1 - z_hi, 0), to_z)


def per_device(eigvecs, material):
    odd = lax.axis_index("gx") % 2 == 1
    upper = lax.axis_index("gz") == 1
    side = jnp.where(odd, SY - 1, 0)
    odd_flag = odd.astype(jnp.int32).reshape(1)

    def chain(x, dim):
        return jnp.where(odd, lax.rev(x, (dim,)), x)

    ym = send(pick(eigvecs, side, 1), to_y)
    face = jnp.where(upper, 0, SZ - 1)
    kz = send(pick(material[0], face, 2), to_z)
    zh = send(pick(eigvecs, face, 2), to_z)
    lanes = jnp.arange(128)
    halo_lane = jnp.where(upper, 127, SZ)
    own = jnp.pad(material, ((0, 0), (0, 0), (0, 0), (0, 128 - SZ)))
    kap = jnp.where(lanes == halo_lane, kz[..., None], own[0])
    mat = jnp.stack([kap, own[1]])
    mx = send(mat[:, 0], to_x)
    vx = send(jnp.concatenate([eigvecs[0].reshape(SY * SZ, K), zh[0]], axis=0), to_x)
    zt = jnp.pad(chain(zh, 1), ((0, 0), (0, 16 - SY), (0, 0)))
    bands = [band_matrix(ins, outs, upper) for ins, outs in NEAR]
    edge_band = band_matrix(*EDGE, upper)
    m = inner_part(odd_flag, eigvecs, zt, chain(mat, 2), bands)
    xh = vx[: SY * SZ].reshape(SY, SZ, K)
    xz = vx[SY * SZ :]
    mat = chain(jnp.concatenate([mat, mx[:, None]], axis=1), 2)
    zrows = chain(jnp.concatenate([zh, xz[None]], axis=0), 1)
    my = send(mat[:, :, 0], to_y)
    ye = send(jnp.concatenate([pick(xh, side, 0), zrows[:, 0]], axis=0), to_y)
    mat = jnp.pad(jnp.concatenate([mat, my[:, :, None]], axis=2), ((0, 0), (0, 0), (0, 7), (0, 0)))
    zt = jnp.pad(jnp.concatenate([zrows, ye[SZ:][:, None]], axis=1), ((0, 0), (0, 7), (0, 0)))
    part = outer_part(odd_flag, m, eigvecs, xh, ym, ye, zt, mat, bands + [edge_band])
    total = SX * SY * SZ * NGX * NGY * NGZ
    summed = reduce_to_owner(part) * (0.5 / total)
    return summed[:, :K], summed[:, K:]


def solution(mesh):
    return jax.shard_map(
        per_device,
        mesh=mesh,
        in_specs=(P("gx", "gy", "gz", None), P(None, "gx", "gy", "gz")),
        out_specs=(P(ALL, None), P(ALL, None)),
        check_vma=False,
    )
```

```python
import jax
import jax.numpy as jnp
from jax import lax
from jax.experimental import pallas as pl
from jax.experimental.pallas import tpu as pltpu
from jax.sharding import PartitionSpec as P

ALL = ("gx", "gy", "gz")
NGX, NGY, NGZ = 4, 16, 2
SX, SY, SZ, K = 16, 8, 48, 512
NEAR = (((0, 1, 2, 3), (0, 1, 2)), ((2, 3, 4, 5, 6), (3, 4, 5)), ((5, 6, 7), (6,)))
EDGE = ((6, 7, 8), (7, 8))
INNER = 7 * SZ
OUTER = 2 * SZ
BATCH = 3
FACE = 224
PIECES = ((0, 1), (1, 3), (3, 5))


def linear(x, y, z):
    return (x * NGY + y) * NGZ + z


def send(value, move):
    links = []
    for x in range(NGX):
        for y in range(NGY):
            for z in range(NGZ):
                to = move(x, y, z)
                if 0 <= to[0] < NGX and 0 <= to[1] < NGY and 0 <= to[2] < NGZ:
                    links.append((linear(x, y, z), linear(*to)))
    return lax.ppermute(value, ALL, links)


def to_z(x, y, z):
    return (x, y, 1 - z)


def to_x(x, y, z):
    return (x - 1, y, z)


def to_y(x, y, z):
    return (x, y + 1, z) if x % 2 else (x, y - 1, z)


def chain_part(gap, ends, mid):
    return jnp.where(gap == 0, jnp.where(ends, 0.0, mid), jnp.where(gap == 1, 1.0, 0.0))


def band_matrix(lines_in, lines_out):
    size = len(lines_out) * SZ
    row = lax.broadcasted_iota(jnp.int32, (2 * size, len(lines_in) * SZ), 0)
    col = lax.broadcasted_iota(jnp.int32, (2 * size, len(lines_in) * SZ), 1)
    mid = jnp.where(row < size, 2.0, 4.0)
    cell = row % size
    line_out = lines_out[0] + cell // SZ
    line_in = lines_in[0] + col // SZ
    z_part = chain_part(jnp.abs(cell % SZ - col % SZ), False, mid)
    y_part = chain_part(jnp.abs(line_out - line_in), line_out == 8, mid)
    return (y_part * z_part).astype(jnp.bfloat16)


def face_matrix():
    row = lax.broadcasted_iota(jnp.int32, (2 * FACE, FACE), 0)
    col = lax.broadcasted_iota(jnp.int32, (2 * FACE, FACE), 1)
    mid = jnp.where(row < FACE, 2.0, 4.0)
    cell = row % FACE
    x_part = chain_part(jnp.abs(cell % 24 - col % 24), cell % 24 == SX, mid)
    y_part = chain_part(jnp.abs(cell // 24 - col // 24), cell // 24 == SY, mid)
    inside = (cell % 24 <= SX) & (col % 24 <= SX) & (cell // 24 <= SY) & (col // 24 <= SY)
    return jnp.where(inside, x_part * y_part, 0.0).astype(jnp.bfloat16)


def apply_band(band, lines, size):
    r = jnp.dot(band, jnp.concatenate(lines, axis=0), preferred_element_type=jnp.float32)
    return r[:size], r[size:]


def kappa_yz(kappa):
    f = 2.0 * kappa + pltpu.roll(kappa, 1, 1) + pltpu.roll(kappa, 127, 1)
    rows = lax.broadcasted_iota(jnp.int32, f.shape, 0)
    below = jnp.where(rows == 0, 0.0, pltpu.roll(f, 1, 0))
    above = jnp.where(rows == f.shape[0] - 1, 0.0, pltpu.roll(f, f.shape[0] - 1, 0))
    mid = jnp.where(rows == 8, 0.0, 2.0 * f)
    return mid + below + above


def weights(kappa, rho, f, plane_own):
    own = 2.0 * kappa if plane_own else jnp.zeros_like(kappa)
    rows = lax.broadcasted_iota(jnp.int32, f.shape, 0)
    alpha = jnp.where(rows == 8, 0.0, own) + f * (1.0 / 32.0)
    return jnp.concatenate([alpha, kappa * (1.0 / 16.0), rho * (1.0 / 216.0)], axis=0).T[:SZ]


def store_products(u, row, v, w3, t3, c, line, stride):
    wide = (SZ, K)
    alpha = jnp.broadcast_to(c[:, line : line + 1], wide)
    kap = jnp.broadcast_to(c[:, stride + line : stride + line + 1], wide)
    rho = jnp.broadcast_to(c[:, 2 * stride + line : 2 * stride + line + 1], wide)
    u[row : row + SZ, 0:K] = (alpha * v.astype(jnp.float32) - kap * w3).astype(jnp.bfloat16)
    u[row : row + SZ, K : 2 * K] = (rho * t3).astype(jnp.bfloat16)


def gram(left, right):
    return lax.dot_general(left, right, (((0,), (0,)), ((), ())), preferred_element_type=jnp.float32)


def line_index(odd, c):
    return c + odd * (7 - 2 * c)


def inner_kernel(first, last, odd_ref, m_hbm, v_hbm, mat_ref, band0, band1, band2, out_hbm, ve, w2, t2, u, acc, sem, sem_m):
    odd = odd_ref[0]
    bands = (band0, band1, band2)
    low = max(BATCH * first - 1, 0)
    cuts = [low] + [BATCH * k + 1 for k in range(first + 1, last + 1)]
    loads = []
    for n in range(last - first):
        a, b = cuts[n], cuts[n + 1]
        loads.append(
            [
                pltpu.make_async_copy(
                    v_hbm.at[pl.ds(a, b - a), line_index(odd, c)], ve.at[pl.ds(a - low, b - a), c], sem.at[n, c]
                )
                for c in range(8)
            ]
        )
        for load in loads[-1]:
            load.start()
    if m_hbm is not None:
        load_m = pltpu.make_async_copy(m_hbm, acc, sem_m.at[2])
        load_m.start()
    yz = {}

    def kappa_of(p):
        if p not in yz:
            yz[p] = kappa_yz(mat_ref[0, p])
        return yz[p]

    def filter_plane(p):
        for g, (ins, outs) in enumerate(NEAR):
            size = len(outs) * SZ
            a, b = apply_band(bands[g][...], [ve[p - low, l] for l in ins], size)
            w2[p % 4, outs[0] * SZ : outs[0] * SZ + size] = a
            t2[p % 4, outs[0] * SZ : outs[0] * SZ + size] = b

    def make_products(p, buf, base):
        f = 2.0 * kappa_of(p) + kappa_of(p + 1)
        if p:
            f = f + kappa_of(p - 1)
        c = weights(mat_ref[0, p], mat_ref[1, p], f, True)
        for l in range(7):
            rows = slice(l * SZ, (l + 1) * SZ)
            mid = w2[p % 4, rows]
            w3 = (mid + mid) + w2[(p + 1) % 4, rows]
            t3 = 4.0 * t2[p % 4, rows] + t2[(p + 1) % 4, rows]
            if p:
                w3 = w3 + w2[(p - 1) % 4, rows]
                t3 = t3 + t2[(p - 1) % 4, rows]
            store_products(u.at[buf], base + l * SZ, ve[p - low, l], w3, t3, c, l, 8)

    done = low
    for n, k in enumerate(range(first, last)):
        for load in loads[n]:
            load.wait()
        for q in range(BATCH):
            p = BATCH * k + q
            while done <= p + 1:
                filter_plane(done)
                done += 1
            make_products(p, k % 2, q * INNER)
        left = jnp.concatenate(
            [ve[BATCH * k + q - low, 0:7].reshape(INNER, K) for q in range(BATCH)], axis=0
        )
        if n == 0 and m_hbm is not None:
            load_m.wait()
        for half in range(2):
            cols = slice(half * K, (half + 1) * K)
            part = gram(left, u[k % 2, :, cols])
            if n == 0 and m_hbm is None:
                acc[:, cols] = part
            else:
                acc[:, cols] += part
            if k == last - 1:
                pltpu.make_async_copy(acc.at[:, cols], out_hbm.at[:, cols], sem_m.at[half]).start()
    for half in range(2):
        cols = slice(half * K, (half + 1) * K)
        pltpu.make_async_copy(acc.at[:, cols], out_hbm.at[:, cols], sem_m.at[half]).wait()


def tile_row(x, y, z_lo, core):
    a = {0: (0, 0), 3: (0, 1), 1: (1, 0), 2: (1, 1)}
    xa, xb = a[x]
    ya, yb = a[y]
    bits = (z_lo, xa, xb, ya, yb) if core == 0 else (xa, z_lo, ya, xb, yb)
    at = core
    for bit in bits:
        at = at * 2 + bit
    return at * 8


def outer_kernel(
    odd_ref, m_hbm, v_hbm, vx_hbm, ym_hbm, ye_hbm, zf_ref, zh_ref, face_ref, mat_ref,
    band0, band1, band2, band3, bandz, out_ref,
    v6, v78, v14, v15, v16, w78, t78, w06, t06, u, sem, acc,
):
    odd = odd_ref[0]
    bands = (band0, band1, band2)
    loads = [
        pltpu.make_async_copy(v_hbm.at[pl.ds(0, 15), line_index(odd, 6)], v6, sem.at[0]),
        pltpu.make_async_copy(v_hbm.at[pl.ds(0, 15), line_index(odd, 7)], v78.at[:, 0], sem.at[1]),
        pltpu.make_async_copy(ym_hbm.at[pl.ds(0, 15)], v78.at[:, 1], sem.at[2]),
        pltpu.make_async_copy(ym_hbm.at[15], v15.at[8], sem.at[3]),
        pltpu.make_async_copy(ye_hbm.at[pl.ds(0, SZ)], v16.at[8], sem.at[4]),
        pltpu.make_async_copy(m_hbm, acc, sem.at[27]),
    ]
    for c in range(8):
        loads.append(pltpu.make_async_copy(v_hbm.at[15, line_index(odd, c)], v15.at[c], sem.at[5 + c]))
        row = pl.multiple_of(line_index(odd, c) * SZ, SZ)
        loads.append(pltpu.make_async_copy(vx_hbm.at[pl.ds(row, SZ)], v16.at[c], sem.at[13 + c]))
        if c < 6:
            loads.append(pltpu.make_async_copy(v_hbm.at[14, line_index(odd, c)], v14.at[c], sem.at[21 + c]))
    for load in loads:
        load.start()
    wz, tz = apply_band(bandz[...], [zh_ref[...]], FACE)
    kap_face, rho_face, kap_halo = face_ref[0], face_ref[1], face_ref[2]
    planes = lax.broadcasted_iota(jnp.int32, kap_halo.shape, 0)
    lines = lax.broadcasted_iota(jnp.int32, kap_halo.shape, 1)
    f = jnp.where(planes == SX, 0.0, 2.0 * kap_halo) + pltpu.roll(kap_halo, 1, 0) + pltpu.roll(kap_halo, 23, 0)
    f = jnp.where(planes <= SX, f, 0.0)
    f = jnp.where(lines == SY, 0.0, 2.0 * f) + pltpu.roll(f, 1, 1) + pltpu.roll(f, 127, 1)
    f = f * (1.0 / 32.0)
    kap_face = kap_face * (1.0 / 16.0)
    rho_face = rho_face * (1.0 / 216.0)

    def column(grid):
        parts = [jnp.broadcast_to(grid[:, l : l + 1], (24, K)) for l in range(9)]
        return jnp.concatenate(parts + [jnp.zeros((8, K), jnp.float32)], axis=0)

    zf = zf_ref[...]
    uz = jnp.concatenate([column(f) * zf.astype(jnp.float32) - column(kap_face) * wz, column(rho_face) * tz], axis=1)
    zpart = gram(zf, uz.astype(jnp.bfloat16))
    for load in loads:
        load.wait()
    acc[...] += zpart

    def line(p, l):
        if p == 15:
            return v15[l]
        if p == 16:
            return v16[l]
        if l >= 7:
            return v78[p, l - 7]
        if l == 6:
            return v6[p]
        return v14[l]

    def filter_near(p):
        for g, (ins, outs) in enumerate(NEAR):
            size = len(outs) * SZ
            a, b = apply_band(bands[g][...], [line(p, l) for l in ins], size)
            w06[p - 14, outs[0] * SZ : outs[0] * SZ + size] = a
            t06[p - 14, outs[0] * SZ : outs[0] * SZ + size] = b

    def filter_edge(p):
        a, b = apply_band(band3[...], [line(p, l) for l in EDGE[0]], OUTER)
        w78[p] = a
        t78[p] = b

    def along_x(ref, p, lo, hi, rows, mid):
        if p == hi:
            return ref[p - 1 - lo, rows]
        r = mid * ref[p - lo, rows] + ref[p + 1 - lo, rows]
        if p > 0:
            r = r + ref[p - 1 - lo, rows]
        return r

    yz = [kappa_yz(mat_ref[0, p]) for p in range(17)]
    for p in range(17):
        filter_edge(p)
        if p >= 14:
            filter_near(p)
    for p in range(17):
        if p == 16:
            f = yz[15]
        else:
            f = 2.0 * yz[p] + yz[p + 1]
            if p:
                f = f + yz[p - 1]
        c = weights(mat_ref[0, p], mat_ref[1, p], f, p != 16)
        for l in range(0 if p >= 15 else 7, 9):
            if p < 15:
                row = p * OUTER + (l - 7) * SZ
            else:
                row = 15 * OUTER + (p - 15) * 9 * SZ + l * SZ
            if l >= 7:
                rows = slice((l - 7) * SZ, (l - 6) * SZ)
                w3 = along_x(w78, p, 0, 16, rows, 2.0)
                t3 = along_x(t78, p, 0, 16, rows, 4.0)
            else:
                rows = slice(l * SZ, (l + 1) * SZ)
                w3 = along_x(w06, p, 14, 16, rows, 2.0)
                t3 = along_x(t06, p, 14, 16, rows, 4.0)
            store_products(u, row, line(p, l), w3, t3, c, l, 16)
    left = jnp.concatenate(
        [v78[...].reshape(15 * OUTER, K), v15[...].reshape(9 * SZ, K), v16[...].reshape(9 * SZ, K)], axis=0
    )
    acc[...] += gram(left, u[...])

    def put(i, j, half, s):
        for x in range(4):
            for y in range(4):
                t = (x * 4 + y) * 8
                at = tile_row(x, y, i // 2, i % 2)
                out_ref[at : at + 8, half * K + j * 128 : half * K + (j + 1) * 128] = s[t : t + 8]

    for half in range(2):
        for i in range(4):
            for j in range(i, 4):
                a = acc[i * 128 : (i + 1) * 128, half * K + j * 128 : half * K + (j + 1) * 128]
                b = acc[j * 128 : (j + 1) * 128, half * K + i * 128 : half * K + (i + 1) * 128]
                s = a + b.T
                put(i, j, half, s)
                if i != j:
                    put(j, i, half, s.T)


HBM = pl.BlockSpec(memory_space=pltpu.HBM)
VMEM = pl.BlockSpec(memory_space=pltpu.VMEM)
SMEM = pl.BlockSpec(memory_space=pltpu.SMEM)


def inner_part(first, last, odd, m, v, mat, bands):
    def body(odd_ref, *refs):
        if m is None:
            refs = (None,) + refs
        inner_kernel(first, last, odd_ref, *refs)

    planes = BATCH * (last - first) + (2 if first else 1)
    operands = (odd,) + (() if m is None else (m,)) + (v, mat) + tuple(bands)
    specs = [SMEM] + ([] if m is None else [HBM]) + [HBM] + [VMEM] * 4
    return pl.pallas_call(
        body,
        out_shape=pltpu.HBM((K, 2 * K), jnp.float32),
        in_specs=specs,
        out_specs=HBM,
        scratch_shapes=[
            pltpu.VMEM((planes, SY, SZ, K), jnp.bfloat16),
            pltpu.VMEM((4, INNER, K), jnp.float32),
            pltpu.VMEM((4, INNER, K), jnp.float32),
            pltpu.VMEM((2, BATCH * INNER, 2 * K), jnp.bfloat16),
            pltpu.VMEM((K, 2 * K), jnp.float32),
            pltpu.SemaphoreType.DMA((last - first, 8)),
            pltpu.SemaphoreType.DMA((3,)),
        ],
        compiler_params=pltpu.CompilerParams(vmem_limit_bytes=26 * 1024 * 1024),
        cost_estimate=pl.CostEstimate(
            flops=1_800_000_000 * (last - first), transcendentals=0, bytes_accessed=2_000_000 * (last - first)
        ),
        name=f"inner{first}",
    )(*operands)


def outer_part(odd, m, v, vx, ym, ye, zf, zh, face, mat, bands):
    return pl.pallas_call(
        outer_kernel,
        out_shape=jax.ShapeDtypeStruct((K, 2 * K), jnp.float32),
        in_specs=[SMEM, HBM, HBM, HBM, HBM, HBM] + [VMEM] * 9,
        out_specs=VMEM,
        scratch_shapes=[
            pltpu.VMEM((15, SZ, K), jnp.bfloat16),
            pltpu.VMEM((15, 2, SZ, K), jnp.bfloat16),
            pltpu.VMEM((6, SZ, K), jnp.bfloat16),
            pltpu.VMEM((9, SZ, K), jnp.bfloat16),
            pltpu.VMEM((9, SZ, K), jnp.bfloat16),
            pltpu.VMEM((17, OUTER, K), jnp.float32),
            pltpu.VMEM((17, OUTER, K), jnp.float32),
            pltpu.VMEM((3, INNER, K), jnp.float32),
            pltpu.VMEM((3, INNER, K), jnp.float32),
            pltpu.VMEM((15 * OUTER + 18 * SZ, 2 * K), jnp.bfloat16),
            pltpu.SemaphoreType.DMA((28,)),
            pltpu.VMEM((K, 2 * K), jnp.float32),
        ],
        compiler_params=pltpu.CompilerParams(vmem_limit_bytes=32 * 1024 * 1024),
        cost_estimate=pl.CostEstimate(flops=4_000_000_000, transcendentals=0, bytes_accessed=6_000_000),
        name="outer",
    )(odd, m, v, vx, ym, ye, zf, zh, face, mat, *bands)


def pick(x, index, dim):
    return lax.dynamic_index_in_dim(x, index, dim, keepdims=False)


def reduce_to_owner(part):
    ix = lax.axis_index("gx")
    iy = lax.axis_index("gy")
    core = ix % 2
    z_lo = ix // 2
    z_hi = lax.axis_index("gz")

    def bits(r):
        return ((r == 1) | (r == 2)).astype(jnp.int32), (r >= 2).astype(jnp.int32)

    def flip_z(x, y, z):
        return (x ^ 2, y, z)

    def flip_xa(x, y, z):
        return (x, (y // 4 ^ 1) * 4 + y % 4, z)

    def flip_xb(x, y, z):
        return (x, (3 - y // 4) * 4 + y % 4, z)

    def flip_ya(x, y, z):
        return (x, y ^ 1, z)

    def flip_yb(x, y, z):
        return (x, y // 4 * 4 + 3 - y % 4, z)

    xa, xb = bits(iy // 4)
    ya, yb = bits(iy % 4)
    stages = (
        (core, core, lambda x, y, z: (x ^ 1, y, z), lambda x, y, z: (x ^ 1, y, z)),
        (z_lo, xa, flip_z, flip_xa),
        (xa, z_lo, flip_xa, flip_z),
        (xb, ya, flip_xb, flip_ya),
        (ya, xb, flip_ya, flip_xb),
        (yb, yb, flip_yb, flip_yb),
    )
    v = part
    for even_bit, odd_bit, even_move, odd_move in stages:
        bit = jnp.where(core == 0, even_bit, odd_bit)
        v = v.reshape(2, v.shape[0] // 2, 2 * K)
        v = pick(v, bit, 0) + send(
            pick(v, 1 - bit, 0),
            lambda x, y, z, e=even_move, o=odd_move: o(x, y, z) if x % 2 else e(x, y, z),
        )
    v = v.reshape(2, 4, 2 * K)
    return pick(v, z_hi, 0) + send(pick(v, 1 - z_hi, 0), to_z)


def to_parts(x):
    high = lax.reduce_precision(x, 8, 7)
    rest = x - high
    mid = lax.reduce_precision(rest, 8, 7)
    parts = jnp.concatenate([high, mid, rest - mid, jnp.zeros_like(x)], axis=1)
    return parts.astype(jnp.bfloat16)


def from_parts(rows):
    x = rows.astype(jnp.float32)
    return (x[:, 256:384] + x[:, 128:256]) + x[:, :128]


def per_device(eigvecs, material):
    odd = lax.axis_index("gx") % 2 == 1
    upper = lax.axis_index("gz") == 1
    side = jnp.where(odd, SY - 1, 0)
    face = jnp.where(upper, 0, SZ - 1)
    odd_flag = odd.astype(jnp.int32).reshape(1)
    in_hbm = lambda x: pltpu.with_memory_space_constraint(x, pltpu.HBM)
    vectors = in_hbm(eigvecs)

    def chain(x, dim):
        return jnp.where(odd, lax.rev(x, (dim,)), x)

    ym = send(pick(eigvecs, side, 1), to_y)
    zf = pick(eigvecs, face, 2)
    kface = jnp.pad(pick(material[0], face, 2), ((0, 0), (0, 120)))
    zm = send(jnp.concatenate([zf.reshape(SX * SY, K), to_parts(kface)], axis=0), to_z)
    own = jnp.pad(material, ((0, 0), (0, 0), (0, 0), (0, 128 - SZ)))
    mat = chain(own, 2)
    bands = [band_matrix(ins, outs) for ins, outs in NEAR]
    m = inner_part(*PIECES[0], odd_flag, None, vectors, mat, bands)
    zm, m = lax.optimization_barrier((zm, m))
    zh = zm[: SX * SY].reshape(SX, SY, K)
    kz = from_parts(zm[SX * SY :])[:, :SY]
    lanes = jnp.arange(128)
    matz = jnp.stack([jnp.where(lanes == 64, kz[..., None], own[0]), own[1]])
    vx = send(
        jnp.concatenate([eigvecs[0].reshape(SY * SZ, K), zh[0], to_parts(matz[:, 0].reshape(16, 128))], axis=0),
        to_x,
    )
    m = inner_part(*PIECES[1], odd_flag, in_hbm(m), vectors, mat, bands)
    vx, m = lax.optimization_barrier((vx, m))
    xz = vx[SY * SZ : SY * SZ + SY]
    matz = jnp.concatenate([matz, from_parts(vx[SY * SZ + SY :]).reshape(2, 1, SY, 128)], axis=1)
    matz = chain(matz, 2)
    zrows = chain(jnp.concatenate([zh, xz[None]], axis=0), 1)
    xline = lax.dynamic_slice_in_dim(vx, side * SZ, SZ, 0)
    ye = send(jnp.concatenate([xline, zrows[:, 0], to_parts(matz[:, :, 0].reshape(34, 128))], axis=0), to_y)
    m = inner_part(*PIECES[2], odd_flag, in_hbm(m), vectors, mat, bands)
    ym, ye, m = lax.optimization_barrier((ym, ye, m))
    my = from_parts(ye[SZ + 17 :]).reshape(2, 17, 1, 128)
    matz = jnp.concatenate([matz, my], axis=2)
    grids = jnp.stack([pick(matz[0], face, 2), pick(matz[1], face, 2), matz[0, :, :, 64]])
    grids = jnp.pad(grids, ((0, 0), (0, 7), (0, 119)))
    mat = jnp.pad(matz, ((0, 0), (0, 0), (0, 7), (0, 0)))
    mat = jnp.where(lanes < SZ, mat, 0.0)

    def face_rows(main, line):
        rows = jnp.concatenate([main, line[:, None]], axis=1).transpose(1, 0, 2)
        return jnp.pad(jnp.pad(rows, ((0, 0), (0, 7), (0, 0))).reshape(216, K), ((0, FACE - 216), (0, 0)))

    xf = pick(vx[: SY * SZ].reshape(SY, SZ, K), face, 1)
    yf = jnp.concatenate([pick(ym, face, 1), lax.dynamic_slice_in_dim(ye, face, 1, 0)], axis=0)
    zf = face_rows(chain(jnp.concatenate([zf, xf[None]], axis=0), 1), yf)
    zh = face_rows(zrows, ye[SZ : SZ + 17])
    bands = bands + [band_matrix(*EDGE), face_matrix()]
    part = outer_part(odd_flag, in_hbm(m), vectors, vx, in_hbm(ym), ye, zf, zh, grids, mat, bands)
    total = SX * SY * SZ * NGX * NGY * NGZ
    summed = reduce_to_owner(part) * (0.5 / total)
    return summed[:, :K], summed[:, K:]


def solution(mesh):
    return jax.shard_map(
        per_device,
        mesh=mesh,
        in_specs=(P("gx", "gy", "gz", None), P(None, "gx", "gy", "gz")),
        out_specs=(P(ALL, None), P(ALL, None)),
        check_vma=False,
    )
```

```python
import jax
import jax.numpy as jnp
import numpy as np
from jax import lax
from jax.experimental import pallas as pl
from jax.experimental.pallas import tpu as pltpu
from jax.sharding import PartitionSpec as P

ALL = ("gx", "gy", "gz")
NGX, NGY, NGZ = 4, 16, 2
SX, SY, SZ, K = 16, 8, 48, 512
NEAR = (((0, 1, 2, 3), (0, 1, 2)), ((2, 3, 4, 5, 6), (3, 4, 5)), ((5, 6, 7), (6,)))
EDGE = ((6, 7, 8), (7, 8))
INNER = 7 * SZ
OUTER = 2 * SZ
BATCH = 3
FACE = 224
MAIN = 15 * OUTER + 18 * SZ
PIECES = ((0, 1), (1, 3), (3, 5))


def linear(x, y, z):
    return (x * NGY + y) * NGZ + z


def send(value, move):
    links = []
    for x in range(NGX):
        for y in range(NGY):
            for z in range(NGZ):
                to = move(x, y, z)
                if 0 <= to[0] < NGX and 0 <= to[1] < NGY and 0 <= to[2] < NGZ:
                    links.append((linear(x, y, z), linear(*to)))
    return lax.ppermute(value, ALL, links)


def to_z(x, y, z):
    return (x, y, 1 - z)


def to_x(x, y, z):
    return (x - 1, y, z)


def to_y(x, y, z):
    return (x, y + 1, z) if x % 2 else (x, y - 1, z)


def chain_part(gap, ends, mid):
    return np.where(gap == 0, np.where(ends, 0.0, mid), np.where(gap == 1, 1.0, 0.0))


def band_matrix(lines_in, lines_out):
    size = len(lines_out) * SZ
    row, col = np.indices((2 * size, len(lines_in) * SZ))
    mid = np.where(row < size, 2.0, 4.0)
    cell = row % size
    line_out = lines_out[0] + cell // SZ
    line_in = lines_in[0] + col // SZ
    z_part = chain_part(np.abs(cell % SZ - col % SZ), False, mid)
    y_part = chain_part(np.abs(line_out - line_in), line_out == 8, mid)
    return jnp.asarray(y_part * z_part, jnp.bfloat16)


def face_matrix():
    row, col = np.indices((2 * FACE, FACE))
    mid = np.where(row < FACE, 2.0, 4.0)
    cell = row % FACE
    x_part = chain_part(np.abs(cell % 24 - col % 24), cell % 24 == SX, mid)
    y_part = chain_part(np.abs(cell // 24 - col // 24), cell // 24 == SY, mid)
    inside = (cell % 24 <= SX) & (col % 24 <= SX) & (cell // 24 <= SY) & (col // 24 <= SY)
    return jnp.asarray(np.where(inside, x_part * y_part, 0.0), jnp.bfloat16)


def apply_band(band, lines, size):
    r = jnp.dot(band, jnp.concatenate(lines, axis=0), preferred_element_type=jnp.float32)
    return r[:size], r[size:]


def kappa_yz(kappa):
    f = 2.0 * kappa + pltpu.roll(kappa, 1, 1) + pltpu.roll(kappa, 127, 1)
    rows = lax.broadcasted_iota(jnp.int32, f.shape, 0)
    below = jnp.where(rows == 0, 0.0, pltpu.roll(f, 1, 0))
    above = jnp.where(rows == f.shape[0] - 1, 0.0, pltpu.roll(f, f.shape[0] - 1, 0))
    mid = jnp.where(rows == 8, 0.0, 2.0 * f)
    return mid + below + above


def weights(kappa, rho, f, plane_own):
    own = 2.0 * kappa if plane_own else jnp.zeros_like(kappa)
    rows = lax.broadcasted_iota(jnp.int32, f.shape, 0)
    alpha = jnp.where(rows == 8, 0.0, own) + f * (1.0 / 32.0)
    return jnp.concatenate([alpha, kappa * (1.0 / 16.0), rho * (1.0 / 216.0)], axis=0).T[:SZ]


def store_products(u, row, v, w3, t3, c, line, stride):
    wide = (SZ, K)
    alpha = jnp.broadcast_to(c[:, line : line + 1], wide)
    kap = jnp.broadcast_to(c[:, stride + line : stride + line + 1], wide)
    rho = jnp.broadcast_to(c[:, 2 * stride + line : 2 * stride + line + 1], wide)
    u[row : row + SZ, 0:K] = (alpha * v.astype(jnp.float32) - kap * w3).astype(jnp.bfloat16)
    u[row : row + SZ, K : 2 * K] = (rho * t3).astype(jnp.bfloat16)


def gram(left, right):
    return lax.dot_general(left, right, (((0,), (0,)), ((), ())), preferred_element_type=jnp.float32)


def line_index(odd, c):
    return c + odd * (7 - 2 * c)


def inner_kernel(first, last, odd_ref, m_hbm, v_hbm, mat_ref, band0, band1, band2, out_hbm, ve, w2, t2, u, acc, sem, sem_m):
    odd = odd_ref[0]
    bands = (band0, band1, band2)
    low = max(BATCH * first - 1, 0)
    loads = {
        p: [
            pltpu.make_async_copy(v_hbm.at[p, line_index(odd, c)], ve.at[p - low, c], sem.at[p - low, c])
            for c in range(8)
        ]
        for p in range(low, BATCH * last + 1)
    }
    for p in loads:
        for load in loads[p]:
            load.start()
    if m_hbm is not None:
        load_m = pltpu.make_async_copy(m_hbm, acc, sem_m.at[2])
        load_m.start()
    yz = {}

    def kappa_of(p):
        if p not in yz:
            yz[p] = kappa_yz(mat_ref[0, p])
        return yz[p]

    def filter_plane(p):
        for load in loads[p]:
            load.wait()
        for g, (ins, outs) in enumerate(NEAR):
            size = len(outs) * SZ
            a, b = apply_band(bands[g][...], [ve[p - low, l] for l in ins], size)
            w2[p % 4, outs[0] * SZ : outs[0] * SZ + size] = a
            t2[p % 4, outs[0] * SZ : outs[0] * SZ + size] = b

    def make_products(p, buf, base):
        f = 2.0 * kappa_of(p) + kappa_of(p + 1)
        if p:
            f = f + kappa_of(p - 1)
        c = weights(mat_ref[0, p], mat_ref[1, p], f, True)
        for l in range(7):
            rows = slice(l * SZ, (l + 1) * SZ)
            mid = w2[p % 4, rows]
            w3 = (mid + mid) + w2[(p + 1) % 4, rows]
            t3 = 4.0 * t2[p % 4, rows] + t2[(p + 1) % 4, rows]
            if p:
                w3 = w3 + w2[(p - 1) % 4, rows]
                t3 = t3 + t2[(p - 1) % 4, rows]
            store_products(u.at[buf], base + l * SZ, ve[p - low, l], w3, t3, c, l, 8)

    done = low
    for n, k in enumerate(range(first, last)):
        for q in range(BATCH):
            p = BATCH * k + q
            while done <= p + 1:
                filter_plane(done)
                done += 1
            make_products(p, k % 2, q * INNER)
        left = jnp.concatenate(
            [ve[BATCH * k + q - low, 0:7].reshape(INNER, K) for q in range(BATCH)], axis=0
        )
        if n == 0 and m_hbm is not None:
            load_m.wait()
        for half in range(2):
            cols = slice(half * K, (half + 1) * K)
            part = gram(left, u[k % 2, :, cols])
            if n == 0 and m_hbm is None:
                acc[:, cols] = part
            else:
                acc[:, cols] += part
            if k == last - 1:
                pltpu.make_async_copy(acc.at[:, cols], out_hbm.at[:, cols], sem_m.at[half]).start()
    for half in range(2):
        cols = slice(half * K, (half + 1) * K)
        pltpu.make_async_copy(acc.at[:, cols], out_hbm.at[:, cols], sem_m.at[half]).wait()


def outer_kernel(
    odd_ref, m_hbm, v_hbm, vx_hbm, ym_hbm, ye_hbm, zf_ref, zh_ref, face_ref, mat_ref,
    band0, band1, band2, band3, bandz, out_ref,
    v6, v78, v14, v15, v16, w78, t78, w06, t06, u, sem, acc,
):
    odd = odd_ref[0]
    bands = (band0, band1, band2)
    loads = [
        pltpu.make_async_copy(v_hbm.at[pl.ds(0, 15), line_index(odd, 6)], v6, sem.at[0]),
        pltpu.make_async_copy(v_hbm.at[pl.ds(0, 15), line_index(odd, 7)], v78.at[:, 0], sem.at[1]),
        pltpu.make_async_copy(ym_hbm.at[pl.ds(0, 15)], v78.at[:, 1], sem.at[2]),
        pltpu.make_async_copy(ym_hbm.at[15], v15.at[8], sem.at[3]),
        pltpu.make_async_copy(ye_hbm.at[pl.ds(0, SZ)], v16.at[8], sem.at[4]),
    ]
    for c in range(8):
        loads.append(pltpu.make_async_copy(v_hbm.at[15, line_index(odd, c)], v15.at[c], sem.at[5 + c]))
        row = pl.multiple_of(line_index(odd, c) * SZ, SZ)
        loads.append(pltpu.make_async_copy(vx_hbm.at[pl.ds(row, SZ)], v16.at[c], sem.at[13 + c]))
        if c < 6:
            loads.append(pltpu.make_async_copy(v_hbm.at[14, line_index(odd, c)], v14.at[c], sem.at[21 + c]))
    load_m = pltpu.make_async_copy(m_hbm, acc, sem.at[27])
    for load in loads + [load_m]:
        load.start()
    wz, tz = apply_band(bandz[...], [zh_ref[...]], FACE)
    kap_face, rho_face, kap_halo = face_ref[0], face_ref[1], face_ref[2]
    planes = lax.broadcasted_iota(jnp.int32, kap_halo.shape, 0)
    lines = lax.broadcasted_iota(jnp.int32, kap_halo.shape, 1)
    f = jnp.where(planes == SX, 0.0, 2.0 * kap_halo) + pltpu.roll(kap_halo, 1, 0) + pltpu.roll(kap_halo, 23, 0)
    f = jnp.where(planes <= SX, f, 0.0)
    f = jnp.where(lines == SY, 0.0, 2.0 * f) + pltpu.roll(f, 1, 1) + pltpu.roll(f, 127, 1)
    f = f * (1.0 / 32.0)
    kap_face = kap_face * (1.0 / 16.0)
    rho_face = rho_face * (1.0 / 216.0)

    def column(grid):
        parts = [jnp.broadcast_to(grid[:, l : l + 1], (24, K)) for l in range(9)]
        return jnp.concatenate(parts + [jnp.zeros((8, K), jnp.float32)], axis=0)

    zf = zf_ref[...]
    uz = jnp.concatenate([column(f) * zf.astype(jnp.float32) - column(kap_face) * wz, column(rho_face) * tz], axis=1)
    u[MAIN:] = uz.astype(jnp.bfloat16)
    for load in loads:
        load.wait()

    def line(p, l):
        if p == 15:
            return v15[l]
        if p == 16:
            return v16[l]
        if l >= 7:
            return v78[p, l - 7]
        if l == 6:
            return v6[p]
        return v14[l]

    def filter_near(p):
        for g, (ins, outs) in enumerate(NEAR):
            size = len(outs) * SZ
            a, b = apply_band(bands[g][...], [line(p, l) for l in ins], size)
            w06[p - 14, outs[0] * SZ : outs[0] * SZ + size] = a
            t06[p - 14, outs[0] * SZ : outs[0] * SZ + size] = b

    def filter_edge(p):
        a, b = apply_band(band3[...], [line(p, l) for l in EDGE[0]], OUTER)
        w78[p] = a
        t78[p] = b

    def along_x(ref, p, lo, hi, rows, mid):
        if p == hi:
            return ref[p - 1 - lo, rows]
        r = mid * ref[p - lo, rows] + ref[p + 1 - lo, rows]
        if p > 0:
            r = r + ref[p - 1 - lo, rows]
        return r

    yz = [kappa_yz(mat_ref[0, p]) for p in range(17)]
    def make_products(p):
        if p == 16:
            f = yz[15]
        else:
            f = 2.0 * yz[p] + yz[p + 1]
            if p:
                f = f + yz[p - 1]
        c = weights(mat_ref[0, p], mat_ref[1, p], f, p != 16)
        for l in range(0 if p >= 15 else 7, 9):
            if p < 15:
                row = p * OUTER + (l - 7) * SZ
            else:
                row = 15 * OUTER + (p - 15) * 9 * SZ + l * SZ
            if l >= 7:
                rows = slice((l - 7) * SZ, (l - 6) * SZ)
                w3 = along_x(w78, p, 0, 16, rows, 2.0)
                t3 = along_x(t78, p, 0, 16, rows, 4.0)
            else:
                rows = slice(l * SZ, (l + 1) * SZ)
                w3 = along_x(w06, p, 14, 16, rows, 2.0)
                t3 = along_x(t06, p, 14, 16, rows, 4.0)
            store_products(u, row, line(p, l), w3, t3, c, l, 16)

    filter_edge(0)
    for p in range(17):
        if p < 16:
            filter_edge(p + 1)
            if p + 1 >= 14:
                filter_near(p + 1)
        make_products(p)
        if p == 7:
            load_m.wait()
            acc[...] += gram(v78[0:8].reshape(8 * OUTER, K), u[: 8 * OUTER])
    left = jnp.concatenate(
        [v78[8:15].reshape(7 * OUTER, K), v15[...].reshape(9 * SZ, K), v16[...].reshape(9 * SZ, K), zf], axis=0
    )
    acc[...] += gram(left, u[8 * OUTER :])

    def put(i, j, half, s):
        at = ((i % 2) * 2 + i // 2) * 128
        out_ref[half, at : at + 128, j * 128 : (j + 1) * 128] = s

    for half in range(2):
        for i in range(4):
            for j in range(i, 4):
                a = acc[i * 128 : (i + 1) * 128, half * K + j * 128 : half * K + (j + 1) * 128]
                b = acc[j * 128 : (j + 1) * 128, half * K + i * 128 : half * K + (i + 1) * 128]
                s = a + b.T
                put(i, j, half, s)
                if i != j:
                    put(j, i, half, s.T)


HBM = pl.BlockSpec(memory_space=pltpu.HBM)
VMEM = pl.BlockSpec(memory_space=pltpu.VMEM)
SMEM = pl.BlockSpec(memory_space=pltpu.SMEM)


def inner_part(first, last, odd, m, v, mat, bands):
    def body(odd_ref, *refs):
        if m is None:
            refs = (None,) + refs
        inner_kernel(first, last, odd_ref, *refs)

    planes = BATCH * (last - first) + (2 if first else 1)
    operands = (odd,) + (() if m is None else (m,)) + (v, mat) + tuple(bands)
    specs = [SMEM] + ([] if m is None else [HBM]) + [HBM] + [VMEM] * 4
    return pl.pallas_call(
        body,
        out_shape=pltpu.HBM((K, 2 * K), jnp.float32),
        in_specs=specs,
        out_specs=HBM,
        scratch_shapes=[
            pltpu.VMEM((planes, SY, SZ, K), jnp.bfloat16),
            pltpu.VMEM((4, INNER, K), jnp.float32),
            pltpu.VMEM((4, INNER, K), jnp.float32),
            pltpu.VMEM((2, BATCH * INNER, 2 * K), jnp.bfloat16),
            pltpu.VMEM((K, 2 * K), jnp.float32),
            pltpu.SemaphoreType.DMA((planes, 8)),
            pltpu.SemaphoreType.DMA((3,)),
        ],
        compiler_params=pltpu.CompilerParams(vmem_limit_bytes=26 * 1024 * 1024),
        cost_estimate=pl.CostEstimate(
            flops=1_800_000_000 * (last - first), transcendentals=0, bytes_accessed=2_000_000 * (last - first)
        ),
        name=f"inner{first}",
    )(*operands)


def outer_part(odd, m, v, vx, ym, ye, zf, zh, face, mat, bands):
    return pl.pallas_call(
        outer_kernel,
        out_shape=jax.ShapeDtypeStruct((2, K, K), jnp.float32),
        in_specs=[SMEM, HBM, HBM, HBM, HBM, HBM] + [VMEM] * 9,
        out_specs=VMEM,
        scratch_shapes=[
            pltpu.VMEM((15, SZ, K), jnp.bfloat16),
            pltpu.VMEM((15, 2, SZ, K), jnp.bfloat16),
            pltpu.VMEM((6, SZ, K), jnp.bfloat16),
            pltpu.VMEM((9, SZ, K), jnp.bfloat16),
            pltpu.VMEM((9, SZ, K), jnp.bfloat16),
            pltpu.VMEM((17, OUTER, K), jnp.float32),
            pltpu.VMEM((17, OUTER, K), jnp.float32),
            pltpu.VMEM((3, INNER, K), jnp.float32),
            pltpu.VMEM((3, INNER, K), jnp.float32),
            pltpu.VMEM((MAIN + FACE, 2 * K), jnp.bfloat16),
            pltpu.SemaphoreType.DMA((28,)),
            pltpu.VMEM((K, 2 * K), jnp.float32),
        ],
        compiler_params=pltpu.CompilerParams(vmem_limit_bytes=32 * 1024 * 1024),
        cost_estimate=pl.CostEstimate(flops=4_000_000_000, transcendentals=0, bytes_accessed=6_000_000),
        name="outer",
    )(odd, m, v, vx, ym, ye, zf, zh, face, mat, *bands)


def pick(x, index, dim):
    return lax.dynamic_index_in_dim(x, index, dim, keepdims=False)


def reduce_to_owner(part):
    core = lax.axis_index("gx") % 2
    halves = []
    for half in range(2):
        rows = part[half].reshape(2, K // 2, K)
        halves.append(pick(rows, core, 0) + send(pick(rows, 1 - core, 0), lambda x, y, z: (x ^ 1, y, z)))
    groups = [[linear(x, y, z) for x in (c, c + 2) for y in range(NGY) for z in range(NGZ)] for c in range(2)]
    blocks = jnp.concatenate(halves, axis=1).reshape(64, 4, 2 * K)
    blocks = lax.all_to_all(blocks, ALL, 0, 0, tiled=True, axis_index_groups=groups)
    return jnp.sum(blocks, axis=0)


def to_parts(x):
    high = lax.reduce_precision(x, 8, 7)
    rest = x - high
    mid = lax.reduce_precision(rest, 8, 7)
    parts = jnp.concatenate([high, mid, rest - mid, jnp.zeros_like(x)], axis=1)
    return parts.astype(jnp.bfloat16)


def from_parts(rows):
    x = rows.astype(jnp.float32)
    return (x[:, 256:384] + x[:, 128:256]) + x[:, :128]


def per_device(eigvecs, material):
    odd = lax.axis_index("gx") % 2 == 1
    upper = lax.axis_index("gz") == 1
    side = jnp.where(odd, SY - 1, 0)
    face = jnp.where(upper, 0, SZ - 1)
    odd_flag = odd.astype(jnp.int32).reshape(1)
    in_hbm = lambda x: pltpu.with_memory_space_constraint(x, pltpu.HBM)
    vectors = in_hbm(eigvecs)

    def chain(x, dim):
        return jnp.where(odd, lax.rev(x, (dim,)), x)

    ym = send(pick(eigvecs, side, 1), to_y)
    zf = pick(eigvecs, face, 2)
    kface = jnp.pad(pick(material[0], face, 2), ((0, 0), (0, 120)))
    zm = send(jnp.concatenate([zf.reshape(SX * SY, K), to_parts(kface)], axis=0), to_z)
    own = jnp.pad(material, ((0, 0), (0, 0), (0, 0), (0, 128 - SZ)))
    mat = chain(own, 2)
    bands = [band_matrix(ins, outs) for ins, outs in NEAR]
    m = inner_part(*PIECES[0], odd_flag, None, vectors, mat, bands)
    zm, m = lax.optimization_barrier((zm, m))
    zh = zm[: SX * SY].reshape(SX, SY, K)
    kz = from_parts(zm[SX * SY :])[:, :SY]
    lanes = jnp.arange(128)
    matz = jnp.stack([jnp.where(lanes == 64, kz[..., None], own[0]), own[1]])
    vx = send(
        jnp.concatenate([eigvecs[0].reshape(SY * SZ, K), zh[0], to_parts(matz[:, 0].reshape(16, 128))], axis=0),
        to_x,
    )
    m = inner_part(*PIECES[1], odd_flag, in_hbm(m), vectors, mat, bands)
    vx, m = lax.optimization_barrier((vx, m))
    xz = vx[SY * SZ : SY * SZ + SY]
    matz = jnp.concatenate([matz, from_parts(vx[SY * SZ + SY :]).reshape(2, 1, SY, 128)], axis=1)
    matz = chain(matz, 2)
    zrows = chain(jnp.concatenate([zh, xz[None]], axis=0), 1)
    xline = lax.dynamic_slice_in_dim(vx, side * SZ, SZ, 0)
    ye = send(jnp.concatenate([xline, zrows[:, 0], to_parts(matz[:, :, 0].reshape(34, 128))], axis=0), to_y)
    m = inner_part(*PIECES[2], odd_flag, in_hbm(m), vectors, mat, bands)
    ym, ye, m = lax.optimization_barrier((ym, ye, m))
    my = from_parts(ye[SZ + 17 :]).reshape(2, 17, 1, 128)
    matz = jnp.concatenate([matz, my], axis=2)
    grids = jnp.stack([pick(matz[0], face, 2), pick(matz[1], face, 2), matz[0, :, :, 64]])
    grids = jnp.pad(grids, ((0, 0), (0, 7), (0, 119)))
    mat = jnp.pad(matz, ((0, 0), (0, 0), (0, 7), (0, 0)))
    mat = jnp.where(lanes < SZ, mat, 0.0)

    def face_rows(main, line):
        rows = jnp.concatenate([main, line[:, None]], axis=1).transpose(1, 0, 2)
        return jnp.pad(jnp.pad(rows, ((0, 0), (0, 7), (0, 0))).reshape(216, K), ((0, FACE - 216), (0, 0)))

    xf = pick(vx[: SY * SZ].reshape(SY, SZ, K), face, 1)
    yf = jnp.concatenate([pick(ym, face, 1), lax.dynamic_slice_in_dim(ye, face, 1, 0)], axis=0)
    zf = face_rows(chain(jnp.concatenate([zf, xf[None]], axis=0), 1), yf)
    zh = face_rows(zrows, ye[SZ : SZ + 17])
    bands = bands + [band_matrix(*EDGE), face_matrix()]
    part = outer_part(odd_flag, in_hbm(m), vectors, vx, in_hbm(ym), ye, zf, zh, grids, mat, bands)
    total = SX * SY * SZ * NGX * NGY * NGZ
    summed = reduce_to_owner(part) * (0.5 / total)
    return summed[:, :K], summed[:, K:]


def solution(mesh):
    return jax.shard_map(
        per_device,
        mesh=mesh,
        in_specs=(P("gx", "gy", "gz", None), P(None, "gx", "gy", "gz")),
        out_specs=(P(ALL, None), P(ALL, None)),
        check_vma=False,
    )
```

```python
import jax
import jax.numpy as jnp
import numpy as np
from jax import lax
from jax.experimental import pallas as pl
from jax.experimental.pallas import tpu as pltpu
from jax.sharding import PartitionSpec as P

ALL = ("gx", "gy", "gz")
NGX, NGY, NGZ = 4, 16, 2
SX, SY, SZ, K = 16, 8, 48, 512
NEAR = (((0, 1, 2, 3), (0, 1, 2)), ((2, 3, 4, 5, 6), (3, 4, 5)), ((5, 6, 7), (6,)))
EDGE = ((6, 7, 8), (7, 8))
INNER = 7 * SZ
OUTER = 2 * SZ
BATCH = 3
FACE = 224
MAIN = 15 * OUTER + 18 * SZ
PIECES = ((0, 1), (1, 3), (3, 5))


def linear(x, y, z):
    return (x * NGY + y) * NGZ + z


def send(value, move):
    links = []
    for x in range(NGX):
        for y in range(NGY):
            for z in range(NGZ):
                to = move(x, y, z)
                if 0 <= to[0] < NGX and 0 <= to[1] < NGY and 0 <= to[2] < NGZ:
                    links.append((linear(x, y, z), linear(*to)))
    return lax.ppermute(value, ALL, links)


def to_z(x, y, z):
    return (x, y, 1 - z)


def to_x(x, y, z):
    return (x - 1, y, z)


def to_y(x, y, z):
    return (x, y + 1, z) if x % 2 else (x, y - 1, z)


def chain_part(gap, ends, mid):
    return np.where(gap == 0, np.where(ends, 0.0, mid), np.where(gap == 1, 1.0, 0.0))


def band_matrix(lines_in, lines_out):
    size = len(lines_out) * SZ
    row, col = np.indices((2 * size, len(lines_in) * SZ))
    mid = np.where(row < size, 2.0, 4.0)
    cell = row % size
    line_out = lines_out[0] + cell // SZ
    line_in = lines_in[0] + col // SZ
    z_part = chain_part(np.abs(cell % SZ - col % SZ), False, mid)
    y_part = chain_part(np.abs(line_out - line_in), line_out == 8, mid)
    return jnp.asarray(y_part * z_part, jnp.bfloat16)


def face_matrix():
    row, col = np.indices((2 * FACE, FACE))
    mid = np.where(row < FACE, 2.0, 4.0)
    cell = row % FACE
    x_part = chain_part(np.abs(cell % 24 - col % 24), cell % 24 == SX, mid)
    y_part = chain_part(np.abs(cell // 24 - col // 24), cell // 24 == SY, mid)
    inside = (cell % 24 <= SX) & (col % 24 <= SX) & (cell // 24 <= SY) & (col // 24 <= SY)
    return jnp.asarray(np.where(inside, x_part * y_part, 0.0), jnp.bfloat16)


def apply_band(band, lines, size):
    r = jnp.dot(band, jnp.concatenate(lines, axis=0), preferred_element_type=jnp.float32)
    return r[:size], r[size:]


def kappa_yz(kappa):
    f = 2.0 * kappa + pltpu.roll(kappa, 1, 1) + pltpu.roll(kappa, 127, 1)
    rows = lax.broadcasted_iota(jnp.int32, f.shape, 0)
    below = jnp.where(rows == 0, 0.0, pltpu.roll(f, 1, 0))
    above = jnp.where(rows == f.shape[0] - 1, 0.0, pltpu.roll(f, f.shape[0] - 1, 0))
    mid = jnp.where(rows == 8, 0.0, 2.0 * f)
    return mid + below + above


def weights(kappa, rho, f, plane_own):
    own = 2.0 * kappa if plane_own else jnp.zeros_like(kappa)
    rows = lax.broadcasted_iota(jnp.int32, f.shape, 0)
    alpha = jnp.where(rows == 8, 0.0, own) + f * (1.0 / 32.0)
    return jnp.concatenate([alpha, kappa * (1.0 / 16.0), rho * (1.0 / 216.0)], axis=0).T[:SZ]


def store_products(u, row, v, w3, t3, c, line, stride):
    wide = (SZ, K)
    alpha = jnp.broadcast_to(c[:, line : line + 1], wide)
    kap = jnp.broadcast_to(c[:, stride + line : stride + line + 1], wide)
    rho = jnp.broadcast_to(c[:, 2 * stride + line : 2 * stride + line + 1], wide)
    u[row : row + SZ, 0:K] = (alpha * v.astype(jnp.float32) - kap * w3).astype(jnp.bfloat16)
    u[row : row + SZ, K : 2 * K] = (rho * t3).astype(jnp.bfloat16)


def gram(left, right):
    return lax.dot_general(left, right, (((0,), (0,)), ((), ())), preferred_element_type=jnp.float32)


def line_index(odd, c):
    return c + odd * (7 - 2 * c)


def inner_kernel(first, last, odd_ref, m_hbm, v_hbm, mat_ref, band0, band1, band2, out_hbm, ve, w2, t2, u, acc, sem, sem_m):
    odd = odd_ref[0]
    bands = (band0, band1, band2)
    low = max(BATCH * first - 1, 0)
    loads = {
        p: pltpu.make_async_copy(v_hbm.at[p], ve.at[p - low], sem.at[p - low]) for p in range(low, BATCH * last + 1)
    }
    for p in loads:
        loads[p].start()
    place = [line_index(odd, c) for c in range(8)]
    if m_hbm is not None:
        load_m = pltpu.make_async_copy(m_hbm, acc, sem_m.at[4])
        load_m.start()
    yz = {}

    def kappa_of(p):
        if p not in yz:
            yz[p] = kappa_yz(mat_ref[0, p])
        return yz[p]

    def filter_plane(p):
        loads[p].wait()
        for g, (ins, outs) in enumerate(NEAR):
            size = len(outs) * SZ
            a, b = apply_band(bands[g][...], [ve[p - low, place[l]] for l in ins], size)
            w2[p % 4, outs[0] * SZ : outs[0] * SZ + size] = a
            t2[p % 4, outs[0] * SZ : outs[0] * SZ + size] = b

    def make_products(p, buf, base):
        f = 2.0 * kappa_of(p) + kappa_of(p + 1)
        if p:
            f = f + kappa_of(p - 1)
        c = weights(mat_ref[0, p], mat_ref[1, p], f, True)
        for l in range(7):
            rows = slice(l * SZ, (l + 1) * SZ)
            mid = w2[p % 4, rows]
            w3 = (mid + mid) + w2[(p + 1) % 4, rows]
            t3 = 4.0 * t2[p % 4, rows] + t2[(p + 1) % 4, rows]
            if p:
                w3 = w3 + w2[(p - 1) % 4, rows]
                t3 = t3 + t2[(p - 1) % 4, rows]
            store_products(u.at[buf], base + l * SZ, ve[p - low, place[l]], w3, t3, c, l, 8)

    done = low
    for n, k in enumerate(range(first, last)):
        for q in range(BATCH):
            p = BATCH * k + q
            while done <= p + 1:
                filter_plane(done)
                done += 1
            make_products(p, k % 2, q * INNER)
        left = jnp.concatenate(
            [ve[BATCH * k + q - low, place[l]] for q in range(BATCH) for l in range(7)], axis=0
        )
        if n == 0 and m_hbm is not None:
            load_m.wait()
        for piece in range(4):
            cols = slice(piece * 256, (piece + 1) * 256)
            part = gram(left, u[k % 2, :, cols])
            if n == 0 and m_hbm is None:
                acc[:, cols] = part
            else:
                acc[:, cols] += part
            if k == last - 1:
                pltpu.make_async_copy(acc.at[:, cols], out_hbm.at[:, cols], sem_m.at[piece]).start()
    for piece in range(4):
        cols = slice(piece * 256, (piece + 1) * 256)
        pltpu.make_async_copy(acc.at[:, cols], out_hbm.at[:, cols], sem_m.at[piece]).wait()


def outer_kernel(
    odd_ref, m_hbm, v_hbm, vx_hbm, ym_hbm, ye_hbm, zf_ref, zh_ref, face_ref, mat_ref,
    band0, band1, band2, band3, bandz, keep_s, send_s, keep_m, send_m,
    v6, v7, v8, vp, w78, t78, w06, t06, u, sem, acc, res,
):
    odd = odd_ref[0]
    bands = (band0, band1, band2)
    loads = [
        pltpu.make_async_copy(v_hbm.at[pl.ds(0, 14), line_index(odd, 6)], v6, sem.at[0]),
        pltpu.make_async_copy(v_hbm.at[pl.ds(0, 14), line_index(odd, 7)], v7, sem.at[1]),
        pltpu.make_async_copy(ym_hbm, v8.at[pl.ds(0, 16)], sem.at[2]),
        pltpu.make_async_copy(v_hbm.at[pl.ds(14, 2)], vp.at[pl.ds(0, 2)], sem.at[3]),
        pltpu.make_async_copy(ye_hbm.at[pl.ds(0, SZ)], v8.at[16], sem.at[4]),
    ]
    for y in range(SY):
        loads.append(pltpu.make_async_copy(vx_hbm.at[pl.ds(y * SZ, SZ)], vp.at[2, y], sem.at[5 + y]))
    place = [line_index(odd, c) for c in range(8)]
    load_m = pltpu.make_async_copy(m_hbm, acc, sem.at[13])
    for load in loads + [load_m]:
        load.start()
    wz, tz = apply_band(bandz[...], [zh_ref[...]], FACE)
    kap_face, rho_face, kap_halo = face_ref[0], face_ref[1], face_ref[2]
    planes = lax.broadcasted_iota(jnp.int32, kap_halo.shape, 0)
    lines = lax.broadcasted_iota(jnp.int32, kap_halo.shape, 1)
    f = jnp.where(planes == SX, 0.0, 2.0 * kap_halo) + pltpu.roll(kap_halo, 1, 0) + pltpu.roll(kap_halo, 23, 0)
    f = jnp.where(planes <= SX, f, 0.0)
    f = jnp.where(lines == SY, 0.0, 2.0 * f) + pltpu.roll(f, 1, 1) + pltpu.roll(f, 127, 1)
    f = f * (1.0 / 32.0)
    kap_face = kap_face * (1.0 / 16.0)
    rho_face = rho_face * (1.0 / 216.0)

    def column(grid):
        parts = [jnp.broadcast_to(grid[:, l : l + 1], (24, K)) for l in range(9)]
        return jnp.concatenate(parts + [jnp.zeros((8, K), jnp.float32)], axis=0)

    zf = zf_ref[...]
    uz = jnp.concatenate([column(f) * zf.astype(jnp.float32) - column(kap_face) * wz, column(rho_face) * tz], axis=1)
    u[MAIN:] = uz.astype(jnp.bfloat16)
    for load in loads:
        load.wait()

    def line(p, l):
        if l == 8:
            return v8[p]
        if p >= 14:
            return vp[p - 14, place[l]]
        return v7[p] if l == 7 else v6[p]

    def filter_near(p):
        for g, (ins, outs) in enumerate(NEAR):
            size = len(outs) * SZ
            a, b = apply_band(bands[g][...], [line(p, l) for l in ins], size)
            w06[p - 14, outs[0] * SZ : outs[0] * SZ + size] = a
            t06[p - 14, outs[0] * SZ : outs[0] * SZ + size] = b

    def filter_edge(p):
        a, b = apply_band(band3[...], [line(p, l) for l in EDGE[0]], OUTER)
        w78[p] = a
        t78[p] = b

    def along_x(ref, p, lo, hi, rows, mid):
        if p == hi:
            return ref[p - 1 - lo, rows]
        r = mid * ref[p - lo, rows] + ref[p + 1 - lo, rows]
        if p > 0:
            r = r + ref[p - 1 - lo, rows]
        return r

    yz = [kappa_yz(mat_ref[0, p]) for p in range(17)]
    def make_products(p):
        if p == 16:
            f = yz[15]
        else:
            f = 2.0 * yz[p] + yz[p + 1]
            if p:
                f = f + yz[p - 1]
        c = weights(mat_ref[0, p], mat_ref[1, p], f, p != 16)
        for l in range(0 if p >= 15 else 7, 9):
            if p < 15:
                row = p * OUTER + (l - 7) * SZ
            else:
                row = 15 * OUTER + (p - 15) * 9 * SZ + l * SZ
            if l >= 7:
                rows = slice((l - 7) * SZ, (l - 6) * SZ)
                w3 = along_x(w78, p, 0, 16, rows, 2.0)
                t3 = along_x(t78, p, 0, 16, rows, 4.0)
            else:
                rows = slice(l * SZ, (l + 1) * SZ)
                w3 = along_x(w06, p, 14, 16, rows, 2.0)
                t3 = along_x(t06, p, 14, 16, rows, 4.0)
            store_products(u, row, line(p, l), w3, t3, c, l, 16)

    filter_edge(0)
    for p in range(17):
        if p < 16:
            filter_edge(p + 1)
            if p + 1 >= 14:
                filter_near(p + 1)
        make_products(p)
        if p == 7:
            load_m.wait()
            left = jnp.concatenate([line(q, l) for q in range(8) for l in (7, 8)], axis=0)
            acc[...] += gram(left, u[: 8 * OUTER])
    rows = [line(p, l) for p in range(8, 17) for l in range(0 if p >= 15 else 7, 9)]
    left = jnp.concatenate(rows + [zf], axis=0)
    acc[...] += gram(left, u[8 * OUTER :])

    def put(i, j, half, s):
        res[i % 2, half, (i // 2) * 128 : (i // 2 + 1) * 128, j * 128 : (j + 1) * 128] = s

    for half in range(2):
        for i in range(4):
            for j in range(i, 4):
                a = acc[i * 128 : (i + 1) * 128, half * K + j * 128 : half * K + (j + 1) * 128]
                b = acc[j * 128 : (j + 1) * 128, half * K + i * 128 : half * K + (i + 1) * 128]
                s = a + b.T
                put(i, j, half, s)
                if i != j:
                    put(j, i, half, s.T)
    for core in range(2):

        @pl.when(odd == core)
        def _():
            keep_s[...] = res[core, 0]
            send_s[...] = res[1 - core, 0]
            keep_m[...] = res[core, 1]
            send_m[...] = res[1 - core, 1]


HBM = pl.BlockSpec(memory_space=pltpu.HBM)
VMEM = pl.BlockSpec(memory_space=pltpu.VMEM)
SMEM = pl.BlockSpec(memory_space=pltpu.SMEM)


def inner_part(first, last, odd, m, v, mat, bands):
    def body(odd_ref, *refs):
        if m is None:
            refs = (None,) + refs
        inner_kernel(first, last, odd_ref, *refs)

    planes = BATCH * (last - first) + (2 if first else 1)
    operands = (odd,) + (() if m is None else (m,)) + (v, mat) + tuple(bands)
    specs = [SMEM] + ([] if m is None else [HBM]) + [HBM] + [VMEM] * 4
    return pl.pallas_call(
        body,
        out_shape=pltpu.HBM((K, 2 * K), jnp.float32),
        in_specs=specs,
        out_specs=HBM,
        scratch_shapes=[
            pltpu.VMEM((planes, SY, SZ, K), jnp.bfloat16),
            pltpu.VMEM((4, INNER, K), jnp.float32),
            pltpu.VMEM((4, INNER, K), jnp.float32),
            pltpu.VMEM((2, BATCH * INNER, 2 * K), jnp.bfloat16),
            pltpu.VMEM((K, 2 * K), jnp.float32),
            pltpu.SemaphoreType.DMA((planes,)),
            pltpu.SemaphoreType.DMA((5,)),
        ],
        compiler_params=pltpu.CompilerParams(vmem_limit_bytes=26 * 1024 * 1024),
        cost_estimate=pl.CostEstimate(
            flops=1_800_000_000 * (last - first), transcendentals=0, bytes_accessed=2_000_000 * (last - first)
        ),
        name=f"inner{first}",
    )(*operands)


def outer_part(odd, m, v, vx, ym, ye, zf, zh, face, mat, bands):
    return pl.pallas_call(
        outer_kernel,
        out_shape=[jax.ShapeDtypeStruct((K // 2, K), jnp.float32)] * 4,
        in_specs=[SMEM, HBM, HBM, HBM, HBM, HBM] + [VMEM] * 9,
        out_specs=[VMEM] * 4,
        scratch_shapes=[
            pltpu.VMEM((14, SZ, K), jnp.bfloat16),
            pltpu.VMEM((14, SZ, K), jnp.bfloat16),
            pltpu.VMEM((17, SZ, K), jnp.bfloat16),
            pltpu.VMEM((3, SY, SZ, K), jnp.bfloat16),
            pltpu.VMEM((17, OUTER, K), jnp.float32),
            pltpu.VMEM((17, OUTER, K), jnp.float32),
            pltpu.VMEM((3, INNER, K), jnp.float32),
            pltpu.VMEM((3, INNER, K), jnp.float32),
            pltpu.VMEM((MAIN + FACE, 2 * K), jnp.bfloat16),
            pltpu.SemaphoreType.DMA((14,)),
            pltpu.VMEM((K, 2 * K), jnp.float32),
            pltpu.VMEM((2, 2, K // 2, K), jnp.float32),
        ],
        compiler_params=pltpu.CompilerParams(vmem_limit_bytes=32 * 1024 * 1024),
        cost_estimate=pl.CostEstimate(flops=4_000_000_000, transcendentals=0, bytes_accessed=6_000_000),
        name="outer",
    )(odd, m, v, vx, ym, ye, zf, zh, face, mat, *bands)


def pick(x, index, dim):
    return lax.dynamic_index_in_dim(x, index, dim, keepdims=False)


def reduce_to_owner(part):
    halves = [keep + send(other, lambda x, y, z: (x ^ 1, y, z)) for keep, other in (part[:2], part[2:])]
    groups = [[linear(x, y, z) for x in (c, c + 2) for y in range(NGY) for z in range(NGZ)] for c in range(2)]
    blocks = jnp.concatenate(halves, axis=1).reshape(64, 4, 2 * K)
    blocks = lax.all_to_all(blocks, ALL, 0, 0, tiled=True, axis_index_groups=groups)
    return jnp.sum(blocks, axis=0)


def to_parts(x):
    high = lax.reduce_precision(x, 8, 7)
    rest = x - high
    mid = lax.reduce_precision(rest, 8, 7)
    parts = jnp.concatenate([high, mid, rest - mid, jnp.zeros_like(x)], axis=1)
    return parts.astype(jnp.bfloat16)


def from_parts(rows):
    x = rows.astype(jnp.float32)
    return (x[:, 256:384] + x[:, 128:256]) + x[:, :128]


def per_device(eigvecs, material):
    odd = lax.axis_index("gx") % 2 == 1
    upper = lax.axis_index("gz") == 1
    side = jnp.where(odd, SY - 1, 0)
    face = jnp.where(upper, 0, SZ - 1)
    odd_flag = odd.astype(jnp.int32).reshape(1)
    in_hbm = lambda x: pltpu.with_memory_space_constraint(x, pltpu.HBM)
    vectors = in_hbm(eigvecs)

    def chain(x, dim):
        return jnp.where(odd, lax.rev(x, (dim,)), x)

    ym = send(pick(eigvecs, side, 1), to_y)
    zf = pick(eigvecs, face, 2)
    kface = jnp.pad(pick(material[0], face, 2), ((0, 0), (0, 120)))
    zm = send(jnp.concatenate([zf.reshape(SX * SY, K), to_parts(kface)], axis=0), to_z)
    own = jnp.pad(material, ((0, 0), (0, 0), (0, 0), (0, 128 - SZ)))
    mat = chain(own, 2)
    bands = [band_matrix(ins, outs) for ins, outs in NEAR]
    m = inner_part(*PIECES[0], odd_flag, None, vectors, mat, bands)
    zm, m = lax.optimization_barrier((zm, m))
    zh = zm[: SX * SY].reshape(SX, SY, K)
    kz = from_parts(zm[SX * SY :])[:, :SY]
    lanes = jnp.arange(128)
    matz = jnp.stack([jnp.where(lanes == 64, kz[..., None], own[0]), own[1]])
    vx = send(
        jnp.concatenate([eigvecs[0].reshape(SY * SZ, K), zh[0], to_parts(matz[:, 0].reshape(16, 128))], axis=0),
        to_x,
    )
    m = inner_part(*PIECES[1], odd_flag, in_hbm(m), vectors, mat, bands)
    vx, m = lax.optimization_barrier((vx, m))
    xz = vx[SY * SZ : SY * SZ + SY]
    matz = jnp.concatenate([matz, from_parts(vx[SY * SZ + SY :]).reshape(2, 1, SY, 128)], axis=1)
    matz = chain(matz, 2)
    zrows = chain(jnp.concatenate([zh, xz[None]], axis=0), 1)
    xline = lax.dynamic_slice_in_dim(vx, side * SZ, SZ, 0)
    ye = send(jnp.concatenate([xline, zrows[:, 0], to_parts(matz[:, :, 0].reshape(34, 128))], axis=0), to_y)
    m = inner_part(*PIECES[2], odd_flag, in_hbm(m), vectors, mat, bands)
    ym, ye, m = lax.optimization_barrier((ym, ye, m))
    my = from_parts(ye[SZ + 17 :]).reshape(2, 17, 1, 128)
    matz = jnp.concatenate([matz, my], axis=2)
    grids = jnp.stack([pick(matz[0], face, 2), pick(matz[1], face, 2), matz[0, :, :, 64]])
    grids = jnp.pad(grids, ((0, 0), (0, 7), (0, 119)))
    mat = jnp.pad(matz, ((0, 0), (0, 0), (0, 7), (0, 0)))
    mat = jnp.where(lanes < SZ, mat, 0.0)

    def face_rows(main, line):
        rows = jnp.concatenate([main, line[:, None]], axis=1).transpose(1, 0, 2)
        return jnp.pad(jnp.pad(rows, ((0, 0), (0, 7), (0, 0))).reshape(216, K), ((0, FACE - 216), (0, 0)))

    xf = pick(vx[: SY * SZ].reshape(SY, SZ, K), face, 1)
    yf = jnp.concatenate([pick(ym, face, 1), lax.dynamic_slice_in_dim(ye, face, 1, 0)], axis=0)
    zf = face_rows(chain(jnp.concatenate([zf, xf[None]], axis=0), 1), yf)
    zh = face_rows(zrows, ye[SZ : SZ + 17])
    bands = bands + [band_matrix(*EDGE), face_matrix()]
    part = outer_part(odd_flag, in_hbm(m), vectors, vx, in_hbm(ym), ye, zf, zh, grids, mat, bands)
    total = SX * SY * SZ * NGX * NGY * NGZ
    summed = reduce_to_owner(part) * (0.5 / total)
    return summed[:, :K], summed[:, K:]


def solution(mesh):
    return jax.shard_map(
        per_device,
        mesh=mesh,
        in_specs=(P("gx", "gy", "gz", None), P(None, "gx", "gy", "gz")),
        out_specs=(P(ALL, None), P(ALL, None)),
        check_vma=False,
    )
```

```python
import jax
import jax.numpy as jnp
import numpy as np
from jax import lax
from jax.experimental import pallas as pl
from jax.experimental.pallas import tpu as pltpu
from jax.sharding import PartitionSpec as P

ALL = ("gx", "gy", "gz")
NGX, NGY, NGZ = 4, 16, 2
SX, SY, SZ, K = 16, 8, 48, 512
NEAR = (((0, 1, 2, 3), (0, 1, 2)), ((2, 3, 4, 5, 6), (3, 4, 5)), ((5, 6, 7), (6,)))
EDGE = ((6, 7, 8), (7, 8))
INNER = 7 * SZ
OUTER = 2 * SZ
BATCH = 3
FACE = 224
MAIN = 15 * OUTER + 18 * SZ
PIECES = ((0, 1), (1, 2), (2, 5))


def linear(x, y, z):
    return (x * NGY + y) * NGZ + z


def send(value, move):
    links = []
    for x in range(NGX):
        for y in range(NGY):
            for z in range(NGZ):
                to = move(x, y, z)
                if 0 <= to[0] < NGX and 0 <= to[1] < NGY and 0 <= to[2] < NGZ:
                    links.append((linear(x, y, z), linear(*to)))
    return lax.ppermute(value, ALL, links)


def to_z(x, y, z):
    return (x, y, 1 - z)


def to_x(x, y, z):
    return (x - 1, y, z)


def to_y(x, y, z):
    return (x, y + 1, z) if x % 2 else (x, y - 1, z)


def chain_part(gap, ends, mid):
    return np.where(gap == 0, np.where(ends, 0.0, mid), np.where(gap == 1, 1.0, 0.0))


def band_matrix(lines_in, lines_out):
    size = len(lines_out) * SZ
    row, col = np.indices((2 * size, len(lines_in) * SZ))
    mid = np.where(row < size, 2.0, 4.0)
    cell = row % size
    line_out = lines_out[0] + cell // SZ
    line_in = lines_in[0] + col // SZ
    z_part = chain_part(np.abs(cell % SZ - col % SZ), False, mid)
    y_part = chain_part(np.abs(line_out - line_in), line_out == 8, mid)
    return jnp.asarray(y_part * z_part, jnp.bfloat16)


def face_matrix():
    row, col = np.indices((2 * FACE, FACE))
    mid = np.where(row < FACE, 2.0, 4.0)
    cell = row % FACE
    x_part = chain_part(np.abs(cell % 24 - col % 24), cell % 24 == SX, mid)
    y_part = chain_part(np.abs(cell // 24 - col // 24), cell // 24 == SY, mid)
    inside = (cell % 24 <= SX) & (col % 24 <= SX) & (cell // 24 <= SY) & (col // 24 <= SY)
    return jnp.asarray(np.where(inside, x_part * y_part, 0.0), jnp.bfloat16)


def apply_band(band, lines, size):
    r = jnp.dot(band, jnp.concatenate(lines, axis=0), preferred_element_type=jnp.float32)
    return r[:size], r[size:]


def kappa_yz(kappa):
    f = 2.0 * kappa + pltpu.roll(kappa, 1, 1) + pltpu.roll(kappa, 127, 1)
    rows = lax.broadcasted_iota(jnp.int32, f.shape, 0)
    below = jnp.where(rows == 0, 0.0, pltpu.roll(f, 1, 0))
    above = jnp.where(rows == f.shape[0] - 1, 0.0, pltpu.roll(f, f.shape[0] - 1, 0))
    mid = jnp.where(rows == 8, 0.0, 2.0 * f)
    return mid + below + above


def weights(kappa, rho, f, plane_own):
    own = 2.0 * kappa if plane_own else jnp.zeros_like(kappa)
    rows = lax.broadcasted_iota(jnp.int32, f.shape, 0)
    alpha = jnp.where(rows == 8, 0.0, own) + f * (1.0 / 32.0)
    return jnp.concatenate([alpha, kappa * (1.0 / 16.0), rho * (1.0 / 216.0)], axis=0).T[:SZ]


def store_products(u, row, v, w3, t3, c, line, stride):
    wide = (SZ, K)
    alpha = jnp.broadcast_to(c[:, line : line + 1], wide)
    kap = jnp.broadcast_to(c[:, stride + line : stride + line + 1], wide)
    rho = jnp.broadcast_to(c[:, 2 * stride + line : 2 * stride + line + 1], wide)
    u[row : row + SZ, 0:K] = (alpha * v.astype(jnp.float32) - kap * w3).astype(jnp.bfloat16)
    u[row : row + SZ, K : 2 * K] = (rho * t3).astype(jnp.bfloat16)


def gram(left, right):
    return lax.dot_general(left, right, (((0,), (0,)), ((), ())), preferred_element_type=jnp.float32)


def line_index(odd, c):
    return c + odd * (7 - 2 * c)


def mirror(x):
    rows = lax.broadcasted_iota(jnp.int32, x.shape, 0)
    for s in (4, 2, 1):
        x = jnp.where(rows % (2 * s) < s, pltpu.roll(x, 8 - s, 0), pltpu.roll(x, s, 0))
    return x


def inner_kernel(
    first, last, odd_ref, m_hbm, v_hbm, raw_hbm, hbm0, hbm1, hbm2, out_hbm,
    ve, w2, t2, u, acc, raw, mat_ref, band0, band1, band2, sem, sem_m,
):
    odd = odd_ref[0]
    bands = (band0, band1, band2)
    low = max(BATCH * first - 1, 0)
    loads = {
        p: pltpu.make_async_copy(v_hbm.at[p], ve.at[p - low], sem.at[p - low]) for p in range(low, BATCH * last + 1)
    }
    side = [
        pltpu.make_async_copy(a, b, sem_m.at[5 + n])
        for n, (a, b) in enumerate(((hbm0, band0), (hbm1, band1), (hbm2, band2), (raw_hbm, raw)))
    ]
    loads[low].start()
    for load in side:
        load.start()
    for p in range(low + 1, BATCH * last + 1):
        loads[p].start()
    place = [line_index(odd, c) for c in range(8)]
    if m_hbm is not None:
        load_m = pltpu.make_async_copy(m_hbm, acc, sem_m.at[4])
        load_m.start()
    side[3].wait()
    for i in range(2):
        for p in range(low, BATCH * last + 1):
            mat_ref[i, p] = jnp.zeros((SY, 128), jnp.float32)
            mat_ref[i, p, :, 0:SZ] = raw[i, p]
            x = mat_ref[i, p]
            mat_ref[i, p] = jnp.where(odd == 1, mirror(x), x)
    for load in side[:3]:
        load.wait()
    yz = {}

    def kappa_of(p):
        if p not in yz:
            yz[p] = kappa_yz(mat_ref[0, p])
        return yz[p]

    def filter_plane(p):
        loads[p].wait()
        for g, (ins, outs) in enumerate(NEAR):
            size = len(outs) * SZ
            a, b = apply_band(bands[g][...], [ve[p - low, place[l]] for l in ins], size)
            w2[p % 4, outs[0] * SZ : outs[0] * SZ + size] = a
            t2[p % 4, outs[0] * SZ : outs[0] * SZ + size] = b

    def make_products(p, buf, base):
        f = 2.0 * kappa_of(p) + kappa_of(p + 1)
        if p:
            f = f + kappa_of(p - 1)
        c = weights(mat_ref[0, p], mat_ref[1, p], f, True)
        for l in range(7):
            rows = slice(l * SZ, (l + 1) * SZ)
            mid = w2[p % 4, rows]
            w3 = (mid + mid) + w2[(p + 1) % 4, rows]
            t3 = 4.0 * t2[p % 4, rows] + t2[(p + 1) % 4, rows]
            if p:
                w3 = w3 + w2[(p - 1) % 4, rows]
                t3 = t3 + t2[(p - 1) % 4, rows]
            store_products(u.at[buf], base + l * SZ, ve[p - low, place[l]], w3, t3, c, l, 8)

    done = low
    for n, k in enumerate(range(first, last)):
        for q in range(BATCH):
            p = BATCH * k + q
            while done <= p + 1:
                filter_plane(done)
                done += 1
            make_products(p, k % 2, q * INNER)
        left = jnp.concatenate(
            [ve[BATCH * k + q - low, place[l]] for q in range(BATCH) for l in range(7)], axis=0
        )
        if n == 0 and m_hbm is not None:
            load_m.wait()
        for piece in range(4):
            cols = slice(piece * 256, (piece + 1) * 256)
            part = gram(left, u[k % 2, :, cols])
            if n == 0 and m_hbm is None:
                acc[:, cols] = part
            else:
                acc[:, cols] += part
            if k == last - 1:
                pltpu.make_async_copy(acc.at[:, cols], out_hbm.at[:, cols], sem_m.at[piece]).start()
    for piece in range(4):
        cols = slice(piece * 256, (piece + 1) * 256)
        pltpu.make_async_copy(acc.at[:, cols], out_hbm.at[:, cols], sem_m.at[piece]).wait()


def outer_kernel(
    odd_ref, m_hbm, v_hbm, vx_hbm, vy_hbm, hbm0, hbm1, hbm2, hbm3, hbmz, zf_ref, zh_ref, face_ref, mat_ref,
    keep_s, send_s, keep_m, send_m,
    v6, v7, v8, vp, zl, w78, t78, w06, t06, u, sem, acc, res, band0, band1, band2, band3, bandz,
):
    odd = odd_ref[0]
    bands = (band0, band1, band2)
    loads = [
        pltpu.make_async_copy(v_hbm.at[pl.ds(0, 14), line_index(odd, 6)], v6, sem.at[0]),
        pltpu.make_async_copy(v_hbm.at[pl.ds(0, 14), line_index(odd, 7)], v7, sem.at[1]),
        pltpu.make_async_copy(vy_hbm.at[pl.ds(0, 17 * SZ)], v8, sem.at[2]),
        pltpu.make_async_copy(v_hbm.at[pl.ds(14, 2)], vp.at[pl.ds(0, 2)], sem.at[3]),
    ]
    for y in range(SY):
        loads.append(pltpu.make_async_copy(vx_hbm.at[pl.ds(y * SZ, SZ)], vp.at[2, y], sem.at[5 + y]))
    place = [line_index(odd, c) for c in range(8)]
    load_m = pltpu.make_async_copy(m_hbm, acc, sem.at[13])
    early = [
        pltpu.make_async_copy(hbmz, bandz, sem.at[14]),
        pltpu.make_async_copy(vy_hbm.at[pl.ds(17 * SZ, 64)], zl, sem.at[15]),
    ]
    for n, (a, b) in enumerate(((hbm0, band0), (hbm1, band1), (hbm2, band2), (hbm3, band3))):
        loads.append(pltpu.make_async_copy(a, b, sem.at[16 + n]))
    for load in early + loads + [load_m]:
        load.start()
    for load in early:
        load.wait()
    wz, tz = apply_band(bandz[...], [zh_ref[...], zl[32:64]], FACE)
    kap_face, rho_face, kap_halo = face_ref[0], face_ref[1], face_ref[2]
    planes = lax.broadcasted_iota(jnp.int32, kap_halo.shape, 0)
    lines = lax.broadcasted_iota(jnp.int32, kap_halo.shape, 1)
    f = jnp.where(planes == SX, 0.0, 2.0 * kap_halo) + pltpu.roll(kap_halo, 1, 0) + pltpu.roll(kap_halo, 23, 0)
    f = jnp.where(planes <= SX, f, 0.0)
    f = jnp.where(lines == SY, 0.0, 2.0 * f) + pltpu.roll(f, 1, 1) + pltpu.roll(f, 127, 1)
    f = f * (1.0 / 32.0)
    kap_face = kap_face * (1.0 / 16.0)
    rho_face = rho_face * (1.0 / 216.0)

    def column(grid):
        parts = [jnp.broadcast_to(grid[:, l : l + 1], (24, K)) for l in range(9)]
        return jnp.concatenate(parts + [jnp.zeros((8, K), jnp.float32)], axis=0)

    zf = jnp.concatenate([zf_ref[...], zl[0:32]], axis=0)
    uz = jnp.concatenate([column(f) * zf.astype(jnp.float32) - column(kap_face) * wz, column(rho_face) * tz], axis=1)
    u[MAIN:] = uz.astype(jnp.bfloat16)
    for load in loads:
        load.wait()

    def line(p, l):
        if l == 8:
            return v8[p * SZ : (p + 1) * SZ]
        if p >= 14:
            return vp[p - 14, place[l]]
        return v7[p] if l == 7 else v6[p]

    def filter_near(p):
        for g, (ins, outs) in enumerate(NEAR):
            size = len(outs) * SZ
            a, b = apply_band(bands[g][...], [line(p, l) for l in ins], size)
            w06[p - 14, outs[0] * SZ : outs[0] * SZ + size] = a
            t06[p - 14, outs[0] * SZ : outs[0] * SZ + size] = b

    def filter_edge(p):
        a, b = apply_band(band3[...], [line(p, l) for l in EDGE[0]], OUTER)
        w78[p] = a
        t78[p] = b

    def along_x(ref, p, lo, hi, rows, mid):
        if p == hi:
            return ref[p - 1 - lo, rows]
        r = mid * ref[p - lo, rows] + ref[p + 1 - lo, rows]
        if p > 0:
            r = r + ref[p - 1 - lo, rows]
        return r

    yz = [kappa_yz(mat_ref[0, p]) for p in range(17)]
    def make_products(p):
        if p == 16:
            f = yz[15]
        else:
            f = 2.0 * yz[p] + yz[p + 1]
            if p:
                f = f + yz[p - 1]
        c = weights(mat_ref[0, p], mat_ref[1, p], f, p != 16)
        for l in range(0 if p >= 15 else 7, 9):
            if p < 15:
                row = p * OUTER + (l - 7) * SZ
            else:
                row = 15 * OUTER + (p - 15) * 9 * SZ + l * SZ
            if l >= 7:
                rows = slice((l - 7) * SZ, (l - 6) * SZ)
                w3 = along_x(w78, p, 0, 16, rows, 2.0)
                t3 = along_x(t78, p, 0, 16, rows, 4.0)
            else:
                rows = slice(l * SZ, (l + 1) * SZ)
                w3 = along_x(w06, p, 14, 16, rows, 2.0)
                t3 = along_x(t06, p, 14, 16, rows, 4.0)
            store_products(u, row, line(p, l), w3, t3, c, l, 16)

    filter_edge(0)
    for p in range(17):
        if p < 16:
            filter_edge(p + 1)
            if p + 1 >= 14:
                filter_near(p + 1)
        make_products(p)
        if p == 7:
            load_m.wait()
            left = jnp.concatenate([line(q, l) for q in range(8) for l in (7, 8)], axis=0)
            acc[...] += gram(left, u[: 8 * OUTER])
    rows = [line(p, l) for p in range(8, 17) for l in range(0 if p >= 15 else 7, 9)]
    left = jnp.concatenate(rows + [zf], axis=0)
    acc[...] += gram(left, u[8 * OUTER :])

    def put(i, j, half, s):
        res[i % 2, half, (i // 2) * 128 : (i // 2 + 1) * 128, j * 128 : (j + 1) * 128] = s

    for half in range(2):
        for i in range(4):
            for j in range(i, 4):
                a = acc[i * 128 : (i + 1) * 128, half * K + j * 128 : half * K + (j + 1) * 128]
                b = acc[j * 128 : (j + 1) * 128, half * K + i * 128 : half * K + (i + 1) * 128]
                s = a + b.T
                put(i, j, half, s)
                if i != j:
                    put(j, i, half, s.T)
    for core in range(2):

        @pl.when(odd == core)
        def _():
            keep_s[...] = res[core, 0]
            send_s[...] = res[1 - core, 0]
            keep_m[...] = res[core, 1]
            send_m[...] = res[1 - core, 1]


HBM = pl.BlockSpec(memory_space=pltpu.HBM)
VMEM = pl.BlockSpec(memory_space=pltpu.VMEM)
SMEM = pl.BlockSpec(memory_space=pltpu.SMEM)


def inner_part(first, last, odd, m, v, mat, bands):
    def body(odd_ref, *refs):
        if m is None:
            refs = (None,) + refs
        inner_kernel(first, last, odd_ref, *refs)

    planes = BATCH * (last - first) + (2 if first else 1)
    operands = (odd,) + (() if m is None else (m,)) + (v, mat) + tuple(bands)
    specs = [SMEM] + [HBM] * (len(operands) - 1)
    return pl.pallas_call(
        body,
        out_shape=pltpu.HBM((K, 2 * K), jnp.float32),
        in_specs=specs,
        out_specs=HBM,
        scratch_shapes=[
            pltpu.VMEM((planes, SY, SZ, K), jnp.bfloat16),
            pltpu.VMEM((4, INNER, K), jnp.float32),
            pltpu.VMEM((4, INNER, K), jnp.float32),
            pltpu.VMEM((2, BATCH * INNER, 2 * K), jnp.bfloat16),
            pltpu.VMEM((K, 2 * K), jnp.float32),
            pltpu.VMEM((2, SX, SY, SZ), jnp.float32),
            pltpu.VMEM((2, SX, SY, 128), jnp.float32),
            pltpu.VMEM((6 * SZ, 4 * SZ), jnp.bfloat16),
            pltpu.VMEM((6 * SZ, 5 * SZ), jnp.bfloat16),
            pltpu.VMEM((2 * SZ, 3 * SZ), jnp.bfloat16),
            pltpu.SemaphoreType.DMA((planes,)),
            pltpu.SemaphoreType.DMA((9,)),
        ],
        compiler_params=pltpu.CompilerParams(vmem_limit_bytes=26 * 1024 * 1024),
        cost_estimate=pl.CostEstimate(
            flops=1_800_000_000 * (last - first), transcendentals=0, bytes_accessed=2_000_000 * (last - first)
        ),
        name=f"inner{first}",
    )(*operands)


def outer_part(odd, m, v, vx, vy, bands, zf, zh, face, mat):
    return pl.pallas_call(
        outer_kernel,
        out_shape=[jax.ShapeDtypeStruct((K // 2, K), jnp.float32)] * 4,
        in_specs=[SMEM] + [HBM] * 9 + [VMEM] * 4,
        out_specs=[VMEM] * 4,
        scratch_shapes=[
            pltpu.VMEM((14, SZ, K), jnp.bfloat16),
            pltpu.VMEM((14, SZ, K), jnp.bfloat16),
            pltpu.VMEM((17 * SZ, K), jnp.bfloat16),
            pltpu.VMEM((3, SY, SZ, K), jnp.bfloat16),
            pltpu.VMEM((64, K), jnp.bfloat16),
            pltpu.VMEM((17, OUTER, K), jnp.float32),
            pltpu.VMEM((17, OUTER, K), jnp.float32),
            pltpu.VMEM((3, INNER, K), jnp.float32),
            pltpu.VMEM((3, INNER, K), jnp.float32),
            pltpu.VMEM((MAIN + FACE, 2 * K), jnp.bfloat16),
            pltpu.SemaphoreType.DMA((20,)),
            pltpu.VMEM((K, 2 * K), jnp.float32),
            pltpu.VMEM((2, 2, K // 2, K), jnp.float32),
            pltpu.VMEM((6 * SZ, 4 * SZ), jnp.bfloat16),
            pltpu.VMEM((6 * SZ, 5 * SZ), jnp.bfloat16),
            pltpu.VMEM((2 * SZ, 3 * SZ), jnp.bfloat16),
            pltpu.VMEM((4 * SZ, 3 * SZ), jnp.bfloat16),
            pltpu.VMEM((2 * FACE, FACE), jnp.bfloat16),
        ],
        compiler_params=pltpu.CompilerParams(vmem_limit_bytes=32 * 1024 * 1024),
        cost_estimate=pl.CostEstimate(flops=4_000_000_000, transcendentals=0, bytes_accessed=6_000_000),
        name="outer",
    )(odd, m, v, vx, vy, *bands, zf, zh, face, mat)


def pick(x, index, dim):
    return lax.dynamic_index_in_dim(x, index, dim, keepdims=False)


def reduce_to_owner(part):
    halves = [keep + send(other, lambda x, y, z: (x ^ 1, y, z)) for keep, other in (part[:2], part[2:])]
    groups = [[linear(x, y, z) for x in (c, c + 2) for y in range(NGY) for z in range(NGZ)] for c in range(2)]
    blocks = jnp.concatenate(halves, axis=1).reshape(64, 4, 2 * K)
    blocks = lax.all_to_all(blocks, ALL, 0, 0, tiled=True, axis_index_groups=groups)
    return jnp.sum(blocks, axis=0)


def to_parts(x):
    high = lax.reduce_precision(x, 8, 7)
    rest = x - high
    mid = lax.reduce_precision(rest, 8, 7)
    parts = jnp.concatenate([high, mid, rest - mid, jnp.zeros_like(x)], axis=1)
    return parts.astype(jnp.bfloat16)


def from_parts(rows):
    x = rows.astype(jnp.float32)
    return (x[:, 256:384] + x[:, 128:256]) + x[:, :128]


def face_rows(rows):
    return jnp.pad(rows.transpose(1, 0, 2), ((0, 0), (0, 7), (0, 0))).reshape(192, K)


def per_device(eigvecs, material):
    odd = lax.axis_index("gx") % 2 == 1
    upper = lax.axis_index("gz") == 1
    side = jnp.where(odd, SY - 1, 0)
    face = jnp.where(upper, 0, SZ - 1)
    odd_flag = odd.astype(jnp.int32).reshape(1)
    in_hbm = lambda x: pltpu.with_memory_space_constraint(x, pltpu.HBM)
    vectors = in_hbm(eigvecs)

    def chain(x, dim):
        return jnp.where(odd, lax.rev(x, (dim,)), x)

    zf = pick(eigvecs, face, 2)
    kface = jnp.pad(pick(material[0], face, 2), ((0, 0), (0, 120)))
    zm = send(jnp.concatenate([zf.reshape(SX * SY, K), to_parts(kface)], axis=0), to_z)
    bands = [in_hbm(band_matrix(ins, outs)) for ins, outs in NEAR]
    raw = in_hbm(material)
    m = inner_part(*PIECES[0], odd_flag, None, vectors, raw, bands)
    zm, m = lax.optimization_barrier((zm, m))
    zh = zm[: SX * SY].reshape(SX, SY, K)
    kz = from_parts(zm[SX * SY :])[:, :SY]
    lanes = jnp.arange(128)
    own = jnp.pad(material, ((0, 0), (0, 0), (0, 0), (0, 128 - SZ)))
    matz = jnp.stack([jnp.where(lanes == 64, kz[..., None], own[0]), own[1]])
    plane = eigvecs[0].reshape(SY * SZ, K)
    vx = send(jnp.concatenate([plane, zf[0], zh[0], to_parts(matz[:, 0].reshape(16, 128))], axis=0), to_x)
    m = inner_part(*PIECES[1], odd_flag, in_hbm(m), vectors, raw, bands)
    vx, m = lax.optimization_barrier((vx, m))
    at = SY * SZ
    xf, xz = vx[at : at + SY], vx[at + SY : at + 2 * SY]
    xmat = from_parts(vx[at + 2 * SY :]).reshape(2, 1, SY, 128)
    matz = chain(jnp.concatenate([matz, xmat], axis=1), 2)
    frows = chain(jnp.concatenate([zf, xf[None]], axis=0), 1)
    zrows = chain(jnp.concatenate([zh, xz[None]], axis=0), 1)
    lines = pick(eigvecs, side, 1).reshape(SX * SZ, K)
    xline = lax.dynamic_slice_in_dim(vx, side * SZ, SZ, 0)
    gap = jnp.zeros((15, K), jnp.bfloat16)
    parts = to_parts(matz[:, :, 0].reshape(34, 128))
    vy = send(jnp.concatenate([lines, xline, frows[:, 0], gap, zrows[:, 0], gap, parts], axis=0), to_y)
    zf = face_rows(frows)
    zh = face_rows(zrows)
    m = inner_part(*PIECES[2], odd_flag, in_hbm(m), vectors, raw, bands)
    vy, m, zf, zh = lax.optimization_barrier((vy, m, zf, zh))
    my = from_parts(vy[17 * SZ + 64 :]).reshape(2, 17, 1, 128)
    matz = jnp.concatenate([matz, my], axis=2)
    grids = jnp.stack([pick(matz[0], face, 2), pick(matz[1], face, 2), matz[0, :, :, 64]])
    grids = jnp.pad(grids, ((0, 0), (0, 7), (0, 119)))
    mat = jnp.pad(matz, ((0, 0), (0, 0), (0, 7), (0, 0)))
    mat = jnp.where(lanes < SZ, mat, 0.0)
    bands = bands + [in_hbm(band_matrix(*EDGE)), in_hbm(face_matrix())]
    part = outer_part(odd_flag, in_hbm(m), vectors, vx, vy, bands, zf, zh, grids, mat)
    total = SX * SY * SZ * NGX * NGY * NGZ
    summed = reduce_to_owner(part) * (0.5 / total)
    return summed[:, :K], summed[:, K:]


def solution(mesh):
    return jax.shard_map(
        per_device,
        mesh=mesh,
        in_specs=(P("gx", "gy", "gz", None), P(None, "gx", "gy", "gz")),
        out_specs=(P(ALL, None), P(ALL, None)),
        check_vma=False,
    )
```

```python
import jax
import jax.numpy as jnp
import numpy as np
from jax import lax
from jax.experimental import pallas as pl
from jax.experimental.pallas import tpu as pltpu
from jax.sharding import PartitionSpec as P

ALL = ("gx", "gy", "gz")
NGX, NGY, NGZ = 4, 16, 2
SX, SY, SZ, K = 16, 8, 48, 512
NEAR = (((0, 1, 2, 3), (0, 1, 2)), ((2, 3, 4, 5, 6), (3, 4, 5)), ((5, 6, 7), (6,)))
EDGE = ((6, 7, 8), (7, 8))
INNER = 7 * SZ
OUTER = 2 * SZ
BATCH = 3
FACE = 224
MAIN = 15 * OUTER + 18 * SZ
PIECES = ((0, 1), (1, 2), (2, 5))


def linear(x, y, z):
    return (x * NGY + y) * NGZ + z


def send(value, move):
    links = []
    for x in range(NGX):
        for y in range(NGY):
            for z in range(NGZ):
                to = move(x, y, z)
                if 0 <= to[0] < NGX and 0 <= to[1] < NGY and 0 <= to[2] < NGZ:
                    links.append((linear(x, y, z), linear(*to)))
    return lax.ppermute(value, ALL, links)


def to_z(x, y, z):
    return (x, y, 1 - z)


def to_x(x, y, z):
    return (x - 1, y, z)


def to_y(x, y, z):
    return (x, y + 1, z) if x % 2 else (x, y - 1, z)


def chain_part(gap, ends, mid):
    return np.where(gap == 0, np.where(ends, 0.0, mid), np.where(gap == 1, 1.0, 0.0))


def band_matrix(lines_in, lines_out):
    size = len(lines_out) * SZ
    row, col = np.indices((2 * size, len(lines_in) * SZ))
    mid = np.where(row < size, 2.0, 4.0)
    cell = row % size
    line_out = lines_out[0] + cell // SZ
    line_in = lines_in[0] + col // SZ
    z_part = chain_part(np.abs(cell % SZ - col % SZ), False, mid)
    y_part = chain_part(np.abs(line_out - line_in), line_out == 8, mid)
    return jnp.asarray(y_part * z_part, jnp.bfloat16)


def face_matrix():
    row, col = np.indices((2 * FACE, FACE))
    mid = np.where(row < FACE, 2.0, 4.0)
    cell = row % FACE
    x_part = chain_part(np.abs(cell % 24 - col % 24), cell % 24 == SX, mid)
    y_part = chain_part(np.abs(cell // 24 - col // 24), cell // 24 == SY, mid)
    inside = (cell % 24 <= SX) & (col % 24 <= SX) & (cell // 24 <= SY) & (col // 24 <= SY)
    return jnp.asarray(np.where(inside, x_part * y_part, 0.0), jnp.bfloat16)


def apply_band(band, lines, size):
    r = jnp.dot(band, jnp.concatenate(lines, axis=0), preferred_element_type=jnp.float32)
    return r[:size], r[size:]


def kappa_yz(kappa):
    f = 2.0 * kappa + pltpu.roll(kappa, 1, 1) + pltpu.roll(kappa, 127, 1)
    rows = lax.broadcasted_iota(jnp.int32, f.shape, 0)
    below = jnp.where(rows == 0, 0.0, pltpu.roll(f, 1, 0))
    above = jnp.where(rows == f.shape[0] - 1, 0.0, pltpu.roll(f, f.shape[0] - 1, 0))
    mid = jnp.where(rows == 8, 0.0, 2.0 * f)
    return mid + below + above


def weights(kappa, rho, f, plane_own):
    own = 2.0 * kappa if plane_own else jnp.zeros_like(kappa)
    rows = lax.broadcasted_iota(jnp.int32, f.shape, 0)
    alpha = jnp.where(rows == 8, 0.0, own) + f * (1.0 / 32.0)
    return jnp.concatenate([alpha, kappa * (1.0 / 16.0), rho * (1.0 / 216.0)], axis=0).T[:SZ]


def store_products(u, row, v, w3, t3, c, line, stride):
    wide = (SZ, K)
    alpha = jnp.broadcast_to(c[:, line : line + 1], wide)
    kap = jnp.broadcast_to(c[:, stride + line : stride + line + 1], wide)
    rho = jnp.broadcast_to(c[:, 2 * stride + line : 2 * stride + line + 1], wide)
    u[row : row + SZ, 0:K] = (alpha * v.astype(jnp.float32) - kap * w3).astype(jnp.bfloat16)
    u[row : row + SZ, K : 2 * K] = (rho * t3).astype(jnp.bfloat16)


def gram(left, right):
    return lax.dot_general(left, right, (((0,), (0,)), ((), ())), preferred_element_type=jnp.float32)


def line_index(odd, c):
    return c + odd * (7 - 2 * c)


def mirror(x):
    rows = lax.broadcasted_iota(jnp.int32, x.shape, 0)
    for s in (4, 2, 1):
        x = jnp.where(rows % (2 * s) < s, pltpu.roll(x, 8 - s, 0), pltpu.roll(x, s, 0))
    return x


def inner_kernel(
    first, last, odd_ref, m_hbm, v_hbm, raw_hbm, hbm0, hbm1, hbm2, out_hbm,
    ve, w2, t2, u, acc, raw, mat_ref, band0, band1, band2, sem, sem_m,
):
    odd = odd_ref[0]
    bands = (band0, band1, band2)
    low = max(BATCH * first - 1, 0)
    loads = {
        p: pltpu.make_async_copy(v_hbm.at[p], ve.at[p - low], sem.at[p - low]) for p in range(low, BATCH * last + 1)
    }
    side = [
        pltpu.make_async_copy(a, b, sem_m.at[5 + n])
        for n, (a, b) in enumerate(((hbm0, band0), (hbm1, band1), (hbm2, band2), (raw_hbm, raw)))
    ]
    loads[low].start()
    for load in side:
        load.start()
    for p in range(low + 1, BATCH * last + 1):
        loads[p].start()
    place = [line_index(odd, c) for c in range(8)]
    if m_hbm is not None:
        load_m = pltpu.make_async_copy(m_hbm, acc, sem_m.at[4])
        load_m.start()
    side[3].wait()
    for i in range(2):
        for p in range(low, BATCH * last + 1):
            mat_ref[i, p] = jnp.zeros((SY, 128), jnp.float32)
            mat_ref[i, p, :, 0:SZ] = raw[i, p]
            x = mat_ref[i, p]
            mat_ref[i, p] = jnp.where(odd == 1, mirror(x), x)
    for load in side[:3]:
        load.wait()
    yz = {}

    def kappa_of(p):
        if p not in yz:
            yz[p] = kappa_yz(mat_ref[0, p])
        return yz[p]

    def filter_plane(p):
        for g, (ins, outs) in enumerate(NEAR):
            size = len(outs) * SZ
            a, b = apply_band(bands[g][...], [ve[p - low, place[l]] for l in ins], size)
            w2[p % 4, outs[0] * SZ : outs[0] * SZ + size] = a
            t2[p % 4, outs[0] * SZ : outs[0] * SZ + size] = b

    def plane_weights(p):
        f = 2.0 * kappa_of(p) + kappa_of(p + 1)
        if p:
            f = f + kappa_of(p - 1)
        return weights(mat_ref[0, p], mat_ref[1, p], f, True)

    def make_products(p, l, c, buf, base):
        rows = slice(l * SZ, (l + 1) * SZ)
        mid = w2[p % 4, rows]
        w3 = (mid + mid) + w2[(p + 1) % 4, rows]
        t3 = 4.0 * t2[p % 4, rows] + t2[(p + 1) % 4, rows]
        if p:
            w3 = w3 + w2[(p - 1) % 4, rows]
            t3 = t3 + t2[(p - 1) % 4, rows]
        store_products(u.at[buf], base + l * SZ, ve[p - low, place[l]], w3, t3, c, l, 8)

    def gram_piece(k, piece):
        cols = slice(piece * K, (piece + 1) * K)
        left = jnp.concatenate([ve[BATCH * k + q - low, place[l]] for q in range(BATCH) for l in range(7)], axis=0)
        part = gram(left, u[k % 2, :, cols])
        if k == first and m_hbm is None:
            acc[:, cols] = part
        else:
            acc[:, cols] += part
        if k == last - 1:
            pltpu.make_async_copy(acc.at[:, cols], out_hbm.at[:, cols], sem_m.at[piece]).start()

    ready = min(low + 4, BATCH * last + 1)
    for p in range(low, ready):
        loads[p].wait()
    done = low
    for k in range(first, last):
        if k == first + 1:
            for p in range(ready, BATCH * last + 1):
                loads[p].wait()
            if m_hbm is not None:
                load_m.wait()
        elif last == first + 1:
            for p in range(ready, BATCH * last + 1):
                loads[p].wait()
        pieces = list(range(2)) if k > first else []
        for q in range(BATCH):
            p = BATCH * k + q
            while done <= p + 1:
                filter_plane(done)
                done += 1
            c = plane_weights(p)
            for l in range(7):
                make_products(p, l, c, k % 2, q * INNER)
                if pieces and (q * 7 + l) % 10 == 0:
                    gram_piece(k - 1, pieces.pop(0))
        while pieces:
            gram_piece(k - 1, pieces.pop(0))
    if m_hbm is not None and last == first + 1:
        load_m.wait()
    for piece in range(2):
        gram_piece(last - 1, piece)
    for piece in range(2):
        cols = slice(piece * K, (piece + 1) * K)
        pltpu.make_async_copy(acc.at[:, cols], out_hbm.at[:, cols], sem_m.at[piece]).wait()


def outer_kernel(
    odd_ref, m_hbm, v_hbm, vx_hbm, vy_hbm, hbm0, hbm1, hbm2, hbm3, hbmz, zf_ref, zh_ref, face_ref, mat_ref,
    keep_s, send_s, keep_m, send_m,
    v6, v7, v8, vp, zl, w78, t78, w06, t06, u, sem, acc, res, band0, band1, band2, band3, bandz,
):
    odd = odd_ref[0]
    bands = (band0, band1, band2)
    loads = [
        pltpu.make_async_copy(v_hbm.at[pl.ds(0, 14), line_index(odd, 6)], v6, sem.at[0]),
        pltpu.make_async_copy(v_hbm.at[pl.ds(0, 14), line_index(odd, 7)], v7, sem.at[1]),
        pltpu.make_async_copy(vy_hbm.at[pl.ds(0, 17 * SZ)], v8, sem.at[2]),
        pltpu.make_async_copy(v_hbm.at[pl.ds(14, 2)], vp.at[pl.ds(0, 2)], sem.at[3]),
    ]
    for y in range(SY):
        loads.append(pltpu.make_async_copy(vx_hbm.at[pl.ds(y * SZ, SZ)], vp.at[2, y], sem.at[5 + y]))
    place = [line_index(odd, c) for c in range(8)]
    load_m = pltpu.make_async_copy(m_hbm, acc, sem.at[13])
    early = [
        pltpu.make_async_copy(hbmz, bandz, sem.at[14]),
        pltpu.make_async_copy(vy_hbm.at[pl.ds(17 * SZ, 64)], zl, sem.at[15]),
    ]
    for n, (a, b) in enumerate(((hbm0, band0), (hbm1, band1), (hbm2, band2), (hbm3, band3))):
        loads.append(pltpu.make_async_copy(a, b, sem.at[16 + n]))
    for load in early + loads + [load_m]:
        load.start()
    for load in early:
        load.wait()
    wz, tz = apply_band(bandz[...], [zh_ref[...], zl[32:64]], FACE)
    kap_face, rho_face, kap_halo = face_ref[0], face_ref[1], face_ref[2]
    planes = lax.broadcasted_iota(jnp.int32, kap_halo.shape, 0)
    lines = lax.broadcasted_iota(jnp.int32, kap_halo.shape, 1)
    f = jnp.where(planes == SX, 0.0, 2.0 * kap_halo) + pltpu.roll(kap_halo, 1, 0) + pltpu.roll(kap_halo, 23, 0)
    f = jnp.where(planes <= SX, f, 0.0)
    f = jnp.where(lines == SY, 0.0, 2.0 * f) + pltpu.roll(f, 1, 1) + pltpu.roll(f, 127, 1)
    f = f * (1.0 / 32.0)
    kap_face = kap_face * (1.0 / 16.0)
    rho_face = rho_face * (1.0 / 216.0)

    def column(grid):
        parts = [jnp.broadcast_to(grid[:, l : l + 1], (24, K)) for l in range(9)]
        return jnp.concatenate(parts + [jnp.zeros((8, K), jnp.float32)], axis=0)

    zf = jnp.concatenate([zf_ref[...], zl[0:32]], axis=0)
    uz = jnp.concatenate([column(f) * zf.astype(jnp.float32) - column(kap_face) * wz, column(rho_face) * tz], axis=1)
    u[MAIN:] = uz.astype(jnp.bfloat16)
    for load in loads:
        load.wait()

    def line(p, l):
        if l == 8:
            return v8[p * SZ : (p + 1) * SZ]
        if p >= 14:
            return vp[p - 14, place[l]]
        return v7[p] if l == 7 else v6[p]

    def filter_near(p):
        for g, (ins, outs) in enumerate(NEAR):
            size = len(outs) * SZ
            a, b = apply_band(bands[g][...], [line(p, l) for l in ins], size)
            w06[p - 14, outs[0] * SZ : outs[0] * SZ + size] = a
            t06[p - 14, outs[0] * SZ : outs[0] * SZ + size] = b

    def filter_edge(p):
        a, b = apply_band(band3[...], [line(p, l) for l in EDGE[0]], OUTER)
        w78[p] = a
        t78[p] = b

    def along_x(ref, p, lo, hi, rows, mid):
        if p == hi:
            return ref[p - 1 - lo, rows]
        r = mid * ref[p - lo, rows] + ref[p + 1 - lo, rows]
        if p > 0:
            r = r + ref[p - 1 - lo, rows]
        return r

    yz = [kappa_yz(mat_ref[0, p]) for p in range(17)]
    def make_products(p):
        if p == 16:
            f = yz[15]
        else:
            f = 2.0 * yz[p] + yz[p + 1]
            if p:
                f = f + yz[p - 1]
        c = weights(mat_ref[0, p], mat_ref[1, p], f, p != 16)
        for l in range(0 if p >= 15 else 7, 9):
            if p < 15:
                row = p * OUTER + (l - 7) * SZ
            else:
                row = 15 * OUTER + (p - 15) * 9 * SZ + l * SZ
            if l >= 7:
                rows = slice((l - 7) * SZ, (l - 6) * SZ)
                w3 = along_x(w78, p, 0, 16, rows, 2.0)
                t3 = along_x(t78, p, 0, 16, rows, 4.0)
            else:
                rows = slice(l * SZ, (l + 1) * SZ)
                w3 = along_x(w06, p, 14, 16, rows, 2.0)
                t3 = along_x(t06, p, 14, 16, rows, 4.0)
            store_products(u, row, line(p, l), w3, t3, c, l, 16)

    filter_edge(0)
    for p in range(17):
        if p < 16:
            filter_edge(p + 1)
            if p + 1 >= 14:
                filter_near(p + 1)
        make_products(p)
        if p == 7:
            load_m.wait()
            left = jnp.concatenate([line(q, l) for q in range(8) for l in (7, 8)], axis=0)
            acc[...] += gram(left, u[: 8 * OUTER])
    rows = [line(p, l) for p in range(8, 17) for l in range(0 if p >= 15 else 7, 9)]
    left = jnp.concatenate(rows + [zf], axis=0)
    acc[...] += gram(left, u[8 * OUTER :])

    def put(i, j, half, s):
        res[i % 2, half, (i // 2) * 128 : (i // 2 + 1) * 128, j * 128 : (j + 1) * 128] = s

    for half in range(2):
        for i in range(4):
            for j in range(i, 4):
                a = acc[i * 128 : (i + 1) * 128, half * K + j * 128 : half * K + (j + 1) * 128]
                b = acc[j * 128 : (j + 1) * 128, half * K + i * 128 : half * K + (i + 1) * 128]
                s = a + b.T
                put(i, j, half, s)
                if i != j:
                    put(j, i, half, s.T)
    for core in range(2):

        @pl.when(odd == core)
        def _():
            keep_s[...] = res[core, 0]
            send_s[...] = res[1 - core, 0]
            keep_m[...] = res[core, 1]
            send_m[...] = res[1 - core, 1]


HBM = pl.BlockSpec(memory_space=pltpu.HBM)
VMEM = pl.BlockSpec(memory_space=pltpu.VMEM)
SMEM = pl.BlockSpec(memory_space=pltpu.SMEM)


def inner_part(first, last, odd, m, v, mat, bands):
    def body(odd_ref, *refs):
        if m is None:
            refs = (None,) + refs
        inner_kernel(first, last, odd_ref, *refs)

    planes = BATCH * (last - first) + (2 if first else 1)
    operands = (odd,) + (() if m is None else (m,)) + (v, mat) + tuple(bands)
    specs = [SMEM] + [HBM] * (len(operands) - 1)
    return pl.pallas_call(
        body,
        out_shape=pltpu.HBM((K, 2 * K), jnp.float32),
        in_specs=specs,
        out_specs=HBM,
        scratch_shapes=[
            pltpu.VMEM((planes, SY, SZ, K), jnp.bfloat16),
            pltpu.VMEM((4, INNER, K), jnp.float32),
            pltpu.VMEM((4, INNER, K), jnp.float32),
            pltpu.VMEM((2, BATCH * INNER, 2 * K), jnp.bfloat16),
            pltpu.VMEM((K, 2 * K), jnp.float32),
            pltpu.VMEM((2, SX, SY, SZ), jnp.float32),
            pltpu.VMEM((2, SX, SY, 128), jnp.float32),
            pltpu.VMEM((6 * SZ, 4 * SZ), jnp.bfloat16),
            pltpu.VMEM((6 * SZ, 5 * SZ), jnp.bfloat16),
            pltpu.VMEM((2 * SZ, 3 * SZ), jnp.bfloat16),
            pltpu.SemaphoreType.DMA((planes,)),
            pltpu.SemaphoreType.DMA((9,)),
        ],
        compiler_params=pltpu.CompilerParams(vmem_limit_bytes=26 * 1024 * 1024),
        cost_estimate=pl.CostEstimate(
            flops=1_800_000_000 * (last - first), transcendentals=0, bytes_accessed=2_000_000 * (last - first)
        ),
        name=f"inner{first}",
    )(*operands)


def outer_part(odd, m, v, vx, vy, bands, zf, zh, face, mat):
    return pl.pallas_call(
        outer_kernel,
        out_shape=[jax.ShapeDtypeStruct((K // 2, K), jnp.float32)] * 4,
        in_specs=[SMEM] + [HBM] * 9 + [VMEM] * 4,
        out_specs=[VMEM] * 4,
        scratch_shapes=[
            pltpu.VMEM((14, SZ, K), jnp.bfloat16),
            pltpu.VMEM((14, SZ, K), jnp.bfloat16),
            pltpu.VMEM((17 * SZ, K), jnp.bfloat16),
            pltpu.VMEM((3, SY, SZ, K), jnp.bfloat16),
            pltpu.VMEM((64, K), jnp.bfloat16),
            pltpu.VMEM((17, OUTER, K), jnp.float32),
            pltpu.VMEM((17, OUTER, K), jnp.float32),
            pltpu.VMEM((3, INNER, K), jnp.float32),
            pltpu.VMEM((3, INNER, K), jnp.float32),
            pltpu.VMEM((MAIN + FACE, 2 * K), jnp.bfloat16),
            pltpu.SemaphoreType.DMA((20,)),
            pltpu.VMEM((K, 2 * K), jnp.float32),
            pltpu.VMEM((2, 2, K // 2, K), jnp.float32),
            pltpu.VMEM((6 * SZ, 4 * SZ), jnp.bfloat16),
            pltpu.VMEM((6 * SZ, 5 * SZ), jnp.bfloat16),
            pltpu.VMEM((2 * SZ, 3 * SZ), jnp.bfloat16),
            pltpu.VMEM((4 * SZ, 3 * SZ), jnp.bfloat16),
            pltpu.VMEM((2 * FACE, FACE), jnp.bfloat16),
        ],
        compiler_params=pltpu.CompilerParams(vmem_limit_bytes=32 * 1024 * 1024),
        cost_estimate=pl.CostEstimate(flops=4_000_000_000, transcendentals=0, bytes_accessed=6_000_000),
        name="outer",
    )(odd, m, v, vx, vy, *bands, zf, zh, face, mat)


def pick(x, index, dim):
    return lax.dynamic_index_in_dim(x, index, dim, keepdims=False)


def reduce_to_owner(part):
    halves = [keep + send(other, lambda x, y, z: (x ^ 1, y, z)) for keep, other in (part[:2], part[2:])]
    groups = [[linear(x, y, z) for x in (c, c + 2) for y in range(NGY) for z in range(NGZ)] for c in range(2)]
    blocks = jnp.concatenate(halves, axis=1).reshape(64, 4, 2 * K)
    blocks = lax.all_to_all(blocks, ALL, 0, 0, tiled=True, axis_index_groups=groups)
    return jnp.sum(blocks, axis=0)


def to_parts(x):
    high = lax.reduce_precision(x, 8, 7)
    rest = x - high
    mid = lax.reduce_precision(rest, 8, 7)
    parts = jnp.concatenate([high, mid, rest - mid, jnp.zeros_like(x)], axis=1)
    return parts.astype(jnp.bfloat16)


def from_parts(rows):
    x = rows.astype(jnp.float32)
    return (x[:, 256:384] + x[:, 128:256]) + x[:, :128]


def face_rows(rows):
    return jnp.pad(rows.transpose(1, 0, 2), ((0, 0), (0, 7), (0, 0))).reshape(192, K)


def per_device(eigvecs, material):
    odd = lax.axis_index("gx") % 2 == 1
    upper = lax.axis_index("gz") == 1
    side = jnp.where(odd, SY - 1, 0)
    face = jnp.where(upper, 0, SZ - 1)
    odd_flag = odd.astype(jnp.int32).reshape(1)
    in_hbm = lambda x: pltpu.with_memory_space_constraint(x, pltpu.HBM)
    vectors = in_hbm(eigvecs)

    def chain(x, dim):
        return jnp.where(odd, lax.rev(x, (dim,)), x)

    zf = pick(eigvecs, face, 2)
    kface = jnp.pad(pick(material[0], face, 2), ((0, 0), (0, 120)))
    zm = send(jnp.concatenate([zf.reshape(SX * SY, K), to_parts(kface)], axis=0), to_z)
    bands = [in_hbm(band_matrix(ins, outs)) for ins, outs in NEAR]
    raw = in_hbm(material)
    m = inner_part(*PIECES[0], odd_flag, None, vectors, raw, bands)
    zm, m = lax.optimization_barrier((zm, m))
    zh = zm[: SX * SY].reshape(SX, SY, K)
    kz = from_parts(zm[SX * SY :])[:, :SY]
    lanes = jnp.arange(128)
    own = jnp.pad(material, ((0, 0), (0, 0), (0, 0), (0, 128 - SZ)))
    matz = jnp.stack([jnp.where(lanes == 64, kz[..., None], own[0]), own[1]])
    plane = eigvecs[0].reshape(SY * SZ, K)
    vx = send(jnp.concatenate([plane, zf[0], zh[0], to_parts(matz[:, 0].reshape(16, 128))], axis=0), to_x)
    m = inner_part(*PIECES[1], odd_flag, in_hbm(m), vectors, raw, bands)
    vx, m = lax.optimization_barrier((vx, m))
    at = SY * SZ
    xf, xz = vx[at : at + SY], vx[at + SY : at + 2 * SY]
    xmat = from_parts(vx[at + 2 * SY :]).reshape(2, 1, SY, 128)
    matz = chain(jnp.concatenate([matz, xmat], axis=1), 2)
    frows = chain(jnp.concatenate([zf, xf[None]], axis=0), 1)
    zrows = chain(jnp.concatenate([zh, xz[None]], axis=0), 1)
    lines = pick(eigvecs, side, 1).reshape(SX * SZ, K)
    xline = lax.dynamic_slice_in_dim(vx, side * SZ, SZ, 0)
    gap = jnp.zeros((15, K), jnp.bfloat16)
    parts = to_parts(matz[:, :, 0].reshape(34, 128))
    vy = send(jnp.concatenate([lines, xline, frows[:, 0], gap, zrows[:, 0], gap, parts], axis=0), to_y)
    zf = face_rows(frows)
    zh = face_rows(zrows)
    m = inner_part(*PIECES[2], odd_flag, in_hbm(m), vectors, raw, bands)
    vy, m, zf, zh = lax.optimization_barrier((vy, m, zf, zh))
    my = from_parts(vy[17 * SZ + 64 :]).reshape(2, 17, 1, 128)
    matz = jnp.concatenate([matz, my], axis=2)
    grids = jnp.stack([pick(matz[0], face, 2), pick(matz[1], face, 2), matz[0, :, :, 64]])
    grids = jnp.pad(grids, ((0, 0), (0, 7), (0, 119)))
    mat = jnp.pad(matz, ((0, 0), (0, 0), (0, 7), (0, 0)))
    mat = jnp.where(lanes < SZ, mat, 0.0)
    bands = bands + [in_hbm(band_matrix(*EDGE)), in_hbm(face_matrix())]
    part = outer_part(odd_flag, in_hbm(m), vectors, vx, vy, bands, zf, zh, grids, mat)
    total = SX * SY * SZ * NGX * NGY * NGZ
    summed = reduce_to_owner(part) * (0.5 / total)
    return summed[:, :K], summed[:, K:]


def solution(mesh):
    return jax.shard_map(
        per_device,
        mesh=mesh,
        in_specs=(P("gx", "gy", "gz", None), P(None, "gx", "gy", "gz")),
        out_specs=(P(ALL, None), P(ALL, None)),
        check_vma=False,
    )
```

```python
import jax
import jax.numpy as jnp
import numpy as np
from jax import lax
from jax.experimental import pallas as pl
from jax.experimental.pallas import tpu as pltpu
from jax.sharding import PartitionSpec as P

ALL = ("gx", "gy", "gz")
NGX, NGY, NGZ = 4, 16, 2
SX, SY, SZ, K = 16, 8, 48, 512
NEAR = (((0, 1, 2, 3), (0, 1, 2)), ((2, 3, 4, 5, 6), (3, 4, 5)), ((5, 6, 7), (6,)))
EDGE = ((6, 7, 8), (7, 8))
INNER = 7 * SZ
OUTER = 2 * SZ
BATCH = 3
FACE = 224
MAIN = 15 * OUTER + 18 * SZ
PIECES = ((0, 1), (1, 2), (2, 5))


def linear(x, y, z):
    return (x * NGY + y) * NGZ + z


def send(value, move):
    links = []
    for x in range(NGX):
        for y in range(NGY):
            for z in range(NGZ):
                to = move(x, y, z)
                if 0 <= to[0] < NGX and 0 <= to[1] < NGY and 0 <= to[2] < NGZ:
                    links.append((linear(x, y, z), linear(*to)))
    return lax.ppermute(value, ALL, links)


def to_z(x, y, z):
    return (x, y, 1 - z)


def to_x(x, y, z):
    return (x - 1, y, z)


def to_y(x, y, z):
    return (x, y + 1, z) if x % 2 else (x, y - 1, z)


def chain_part(gap, ends, mid):
    return np.where(gap == 0, np.where(ends, 0.0, mid), np.where(gap == 1, 1.0, 0.0))


def band_matrix(lines_in, lines_out):
    size = len(lines_out) * SZ
    row, col = np.indices((2 * size, len(lines_in) * SZ))
    mid = np.where(row < size, 2.0, 4.0)
    cell = row % size
    line_out = lines_out[0] + cell // SZ
    line_in = lines_in[0] + col // SZ
    z_part = chain_part(np.abs(cell % SZ - col % SZ), False, mid)
    y_part = chain_part(np.abs(line_out - line_in), line_out == 8, mid)
    return jnp.asarray(y_part * z_part, jnp.bfloat16)


def face_matrix():
    row, col = np.indices((2 * FACE, FACE))
    mid = np.where(row < FACE, 2.0, 4.0)
    cell = row % FACE
    x_part = chain_part(np.abs(cell % 24 - col % 24), cell % 24 == SX, mid)
    y_part = chain_part(np.abs(cell // 24 - col // 24), cell // 24 == SY, mid)
    inside = (cell % 24 <= SX) & (col % 24 <= SX) & (cell // 24 <= SY) & (col // 24 <= SY)
    return jnp.asarray(np.where(inside, x_part * y_part, 0.0), jnp.bfloat16)


def apply_band(band, lines, size):
    r = jnp.dot(band, jnp.concatenate(lines, axis=0), preferred_element_type=jnp.float32)
    return r[:size], r[size:]


def kappa_yz(kappa):
    f = 2.0 * kappa + pltpu.roll(kappa, 1, 1) + pltpu.roll(kappa, 127, 1)
    rows = lax.broadcasted_iota(jnp.int32, f.shape, 0)
    below = jnp.where(rows == 0, 0.0, pltpu.roll(f, 1, 0))
    above = jnp.where(rows == f.shape[0] - 1, 0.0, pltpu.roll(f, f.shape[0] - 1, 0))
    mid = jnp.where(rows == 8, 0.0, 2.0 * f)
    return mid + below + above


def weights(kappa, rho, f, plane_own):
    own = 2.0 * kappa if plane_own else jnp.zeros_like(kappa)
    rows = lax.broadcasted_iota(jnp.int32, f.shape, 0)
    alpha = jnp.where(rows == 8, 0.0, own) + f * (1.0 / 32.0)
    return jnp.concatenate([alpha, kappa * (1.0 / 16.0), rho * (1.0 / 216.0)], axis=0).T[:SZ]


def store_products(u, row, v, w3, t3, c, line, stride):
    wide = (SZ, K)
    alpha = jnp.broadcast_to(c[:, line : line + 1], wide)
    kap = jnp.broadcast_to(c[:, stride + line : stride + line + 1], wide)
    rho = jnp.broadcast_to(c[:, 2 * stride + line : 2 * stride + line + 1], wide)
    u[row : row + SZ, 0:K] = (alpha * v.astype(jnp.float32) - kap * w3).astype(jnp.bfloat16)
    u[row : row + SZ, K : 2 * K] = (rho * t3).astype(jnp.bfloat16)


def gram(left, right):
    return lax.dot_general(left, right, (((0,), (0,)), ((), ())), preferred_element_type=jnp.float32)


def line_index(odd, c):
    return c + odd * (7 - 2 * c)


def mirror(x):
    rows = lax.broadcasted_iota(jnp.int32, x.shape, 0)
    for s in (4, 2, 1):
        x = jnp.where(rows % (2 * s) < s, pltpu.roll(x, 8 - s, 0), pltpu.roll(x, s, 0))
    return x


def inner_kernel(
    first, last, buf, odd_ref, m_hbm, v_hbm, raw_hbm, hbm0, hbm1, hbm2, out_hbm,
    ve, w2, t2, u, acc, raw, mat_ref, band0, band1, band2, sem, sem_m,
):
    odd = odd_ref[0]
    bands = (band0, band1, band2)
    low = max(BATCH * first - 1, 0)
    loads = {
        p: pltpu.make_async_copy(v_hbm.at[p], ve.at[p - low], sem.at[p - low]) for p in range(low, BATCH * last + 1)
    }
    side = [
        pltpu.make_async_copy(a, b, sem_m.at[5 + n])
        for n, (a, b) in enumerate(((hbm0, band0), (hbm1, band1), (hbm2, band2), (raw_hbm, raw)))
    ]
    loads[low].start()
    for load in side:
        load.start()
    for p in range(low + 1, BATCH * last + 1):
        loads[p].start()
    place = [line_index(odd, c) for c in range(8)]
    if m_hbm is not None:
        load_m = pltpu.make_async_copy(m_hbm, acc, sem_m.at[4])
        load_m.start()
    extra = []
    if first == 0:
        extra = [(v_hbm.at[0, y], buf.at[pl.ds(y * SZ, SZ)]) for y in range(SY)]
    elif buf is not None:
        extra = [(v_hbm.at[x, 7 * odd], buf.at[pl.ds(x * SZ, SZ)]) for x in range(SX)]
    extra = [pltpu.make_async_copy(a, b, sem_m.at[9 + n]) for n, (a, b) in enumerate(extra)]
    for copy in extra:
        copy.start()
    side[3].wait()
    for i in range(2):
        for p in range(low, BATCH * last + 1):
            mat_ref[i, p] = jnp.zeros((SY, 128), jnp.float32)
            mat_ref[i, p, :, 0:SZ] = raw[i, p]
            x = mat_ref[i, p]
            mat_ref[i, p] = jnp.where(odd == 1, mirror(x), x)
    for load in side[:3]:
        load.wait()
    yz = {}

    def kappa_of(p):
        if p not in yz:
            yz[p] = kappa_yz(mat_ref[0, p])
        return yz[p]

    def filter_plane(p):
        for g, (ins, outs) in enumerate(NEAR):
            size = len(outs) * SZ
            a, b = apply_band(bands[g][...], [ve[p - low, place[l]] for l in ins], size)
            w2[p % 4, outs[0] * SZ : outs[0] * SZ + size] = a
            t2[p % 4, outs[0] * SZ : outs[0] * SZ + size] = b

    def plane_weights(p):
        f = 2.0 * kappa_of(p) + kappa_of(p + 1)
        if p:
            f = f + kappa_of(p - 1)
        return weights(mat_ref[0, p], mat_ref[1, p], f, True)

    def make_products(p, l, c, buf, base):
        rows = slice(l * SZ, (l + 1) * SZ)
        mid = w2[p % 4, rows]
        w3 = (mid + mid) + w2[(p + 1) % 4, rows]
        t3 = 4.0 * t2[p % 4, rows] + t2[(p + 1) % 4, rows]
        if p:
            w3 = w3 + w2[(p - 1) % 4, rows]
            t3 = t3 + t2[(p - 1) % 4, rows]
        store_products(u.at[buf], base + l * SZ, ve[p - low, place[l]], w3, t3, c, l, 8)

    def gram_piece(k, piece):
        cols = slice(piece * K, (piece + 1) * K)
        left = jnp.concatenate([ve[BATCH * k + q - low, place[l]] for q in range(BATCH) for l in range(7)], axis=0)
        part = gram(left, u[k % 2, :, cols])
        if k == first and m_hbm is None:
            acc[:, cols] = part
        else:
            acc[:, cols] += part
        if k == last - 1:
            pltpu.make_async_copy(acc.at[:, cols], out_hbm.at[:, cols], sem_m.at[piece]).start()

    ready = min(low + 4, BATCH * last + 1)
    for p in range(low, ready):
        loads[p].wait()
    done = low
    for k in range(first, last):
        if k == first + 1:
            for p in range(ready, BATCH * last + 1):
                loads[p].wait()
            if m_hbm is not None:
                load_m.wait()
        elif last == first + 1:
            for p in range(ready, BATCH * last + 1):
                loads[p].wait()
        pieces = list(range(2)) if k > first else []
        for q in range(BATCH):
            p = BATCH * k + q
            while done <= p + 1:
                filter_plane(done)
                done += 1
            c = plane_weights(p)
            for l in range(7):
                make_products(p, l, c, k % 2, q * INNER)
                if pieces and (q * 7 + l) % 10 == 0:
                    gram_piece(k - 1, pieces.pop(0))
        while pieces:
            gram_piece(k - 1, pieces.pop(0))
    if m_hbm is not None and last == first + 1:
        load_m.wait()
    for piece in range(2):
        gram_piece(last - 1, piece)
    for copy in extra:
        copy.wait()
    for piece in range(2):
        cols = slice(piece * K, (piece + 1) * K)
        pltpu.make_async_copy(acc.at[:, cols], out_hbm.at[:, cols], sem_m.at[piece]).wait()


def outer_kernel(
    odd_ref, m_hbm, v_hbm, vx_hbm, vy_hbm, hbm0, hbm1, hbm2, hbm3, hbmz, zf_ref, zh_ref, face_ref, mat_ref,
    keep_s, send_s, keep_m, send_m,
    v6, v7, v8, vp, zl, w78, t78, w06, t06, u, sem, acc, res, band0, band1, band2, band3, bandz,
):
    odd = odd_ref[0]
    bands = (band0, band1, band2)
    loads = [
        pltpu.make_async_copy(v_hbm.at[pl.ds(0, 14), line_index(odd, 6)], v6, sem.at[0]),
        pltpu.make_async_copy(v_hbm.at[pl.ds(0, 14), line_index(odd, 7)], v7, sem.at[1]),
        pltpu.make_async_copy(vy_hbm.at[pl.ds(0, 17 * SZ)], v8, sem.at[2]),
        pltpu.make_async_copy(v_hbm.at[pl.ds(14, 2)], vp.at[pl.ds(0, 2)], sem.at[3]),
    ]
    for y in range(SY):
        loads.append(pltpu.make_async_copy(vx_hbm.at[pl.ds(y * SZ, SZ)], vp.at[2, y], sem.at[5 + y]))
    place = [line_index(odd, c) for c in range(8)]
    load_m = pltpu.make_async_copy(m_hbm, acc, sem.at[13])
    early = [
        pltpu.make_async_copy(hbmz, bandz, sem.at[14]),
        pltpu.make_async_copy(vy_hbm.at[pl.ds(17 * SZ, 64)], zl, sem.at[15]),
    ]
    for n, (a, b) in enumerate(((hbm0, band0), (hbm1, band1), (hbm2, band2), (hbm3, band3))):
        loads.append(pltpu.make_async_copy(a, b, sem.at[16 + n]))
    for load in early + loads + [load_m]:
        load.start()
    for load in early:
        load.wait()
    wz, tz = apply_band(bandz[...], [zh_ref[...], zl[32:64]], FACE)
    kap_face, rho_face, kap_halo = face_ref[0], face_ref[1], face_ref[2]
    planes = lax.broadcasted_iota(jnp.int32, kap_halo.shape, 0)
    lines = lax.broadcasted_iota(jnp.int32, kap_halo.shape, 1)
    f = jnp.where(planes == SX, 0.0, 2.0 * kap_halo) + pltpu.roll(kap_halo, 1, 0) + pltpu.roll(kap_halo, 23, 0)
    f = jnp.where(planes <= SX, f, 0.0)
    f = jnp.where(lines == SY, 0.0, 2.0 * f) + pltpu.roll(f, 1, 1) + pltpu.roll(f, 127, 1)
    f = f * (1.0 / 32.0)
    kap_face = kap_face * (1.0 / 16.0)
    rho_face = rho_face * (1.0 / 216.0)

    def column(grid):
        parts = [jnp.broadcast_to(grid[:, l : l + 1], (24, K)) for l in range(9)]
        return jnp.concatenate(parts + [jnp.zeros((8, K), jnp.float32)], axis=0)

    zf = jnp.concatenate([zf_ref[...], zl[0:32]], axis=0)
    uz = jnp.concatenate([column(f) * zf.astype(jnp.float32) - column(kap_face) * wz, column(rho_face) * tz], axis=1)
    u[MAIN:] = uz.astype(jnp.bfloat16)
    for load in loads:
        load.wait()

    def line(p, l):
        if l == 8:
            return v8[p * SZ : (p + 1) * SZ]
        if p >= 14:
            return vp[p - 14, place[l]]
        return v7[p] if l == 7 else v6[p]

    def filter_near(p):
        for g, (ins, outs) in enumerate(NEAR):
            size = len(outs) * SZ
            a, b = apply_band(bands[g][...], [line(p, l) for l in ins], size)
            w06[p - 14, outs[0] * SZ : outs[0] * SZ + size] = a
            t06[p - 14, outs[0] * SZ : outs[0] * SZ + size] = b

    def filter_edge(p):
        a, b = apply_band(band3[...], [line(p, l) for l in EDGE[0]], OUTER)
        w78[p] = a
        t78[p] = b

    def along_x(ref, p, lo, hi, rows, mid):
        if p == hi:
            return ref[p - 1 - lo, rows]
        r = mid * ref[p - lo, rows] + ref[p + 1 - lo, rows]
        if p > 0:
            r = r + ref[p - 1 - lo, rows]
        return r

    yz = [kappa_yz(mat_ref[0, p]) for p in range(17)]
    def make_products(p):
        if p == 16:
            f = yz[15]
        else:
            f = 2.0 * yz[p] + yz[p + 1]
            if p:
                f = f + yz[p - 1]
        c = weights(mat_ref[0, p], mat_ref[1, p], f, p != 16)
        for l in range(0 if p >= 15 else 7, 9):
            if p < 15:
                row = p * OUTER + (l - 7) * SZ
            else:
                row = 15 * OUTER + (p - 15) * 9 * SZ + l * SZ
            if l >= 7:
                rows = slice((l - 7) * SZ, (l - 6) * SZ)
                w3 = along_x(w78, p, 0, 16, rows, 2.0)
                t3 = along_x(t78, p, 0, 16, rows, 4.0)
            else:
                rows = slice(l * SZ, (l + 1) * SZ)
                w3 = along_x(w06, p, 14, 16, rows, 2.0)
                t3 = along_x(t06, p, 14, 16, rows, 4.0)
            store_products(u, row, line(p, l), w3, t3, c, l, 16)

    filter_edge(0)
    for p in range(17):
        if p < 16:
            filter_edge(p + 1)
            if p + 1 >= 14:
                filter_near(p + 1)
        make_products(p)
        if p == 7:
            load_m.wait()
            left = jnp.concatenate([line(q, l) for q in range(8) for l in (7, 8)], axis=0)
            acc[...] += gram(left, u[: 8 * OUTER])
    rows = [line(p, l) for p in range(8, 17) for l in range(0 if p >= 15 else 7, 9)]
    left = jnp.concatenate(rows + [zf], axis=0)
    acc[...] += gram(left, u[8 * OUTER :])

    def put(i, j, half, s):
        res[i % 2, half, (i // 2) * 128 : (i // 2 + 1) * 128, j * 128 : (j + 1) * 128] = s

    for half in range(2):
        for i in range(4):
            for j in range(i, 4):
                a = acc[i * 128 : (i + 1) * 128, half * K + j * 128 : half * K + (j + 1) * 128]
                b = acc[j * 128 : (j + 1) * 128, half * K + i * 128 : half * K + (i + 1) * 128]
                s = a + b.T
                put(i, j, half, s)
                if i != j:
                    put(j, i, half, s.T)
    for core in range(2):

        @pl.when(odd == core)
        def _():
            keep_s[...] = res[core, 0]
            send_s[...] = res[1 - core, 0]
            keep_m[...] = res[core, 1]
            send_m[...] = res[1 - core, 1]


HBM = pl.BlockSpec(memory_space=pltpu.HBM)
VMEM = pl.BlockSpec(memory_space=pltpu.VMEM)
SMEM = pl.BlockSpec(memory_space=pltpu.SMEM)


def inner_part(first, last, odd, m, v, mat, bands):
    rows = {0: 416, 1: 914}.get(first)

    def body(odd_ref, *refs):
        refs = list(refs)
        if m is None:
            refs = [None] + refs
        buf = refs.pop(7) if rows else None
        inner_kernel(first, last, buf, odd_ref, *refs)

    planes = BATCH * (last - first) + (2 if first else 1)
    operands = (odd,) + (() if m is None else (m,)) + (v, mat) + tuple(bands)
    specs = [SMEM] + [HBM] * (len(operands) - 1)
    return pl.pallas_call(
        body,
        out_shape=[pltpu.HBM((K, 2 * K), jnp.float32)]
        + ([jax.ShapeDtypeStruct((rows, K), jnp.bfloat16)] if rows else []),
        in_specs=specs,
        out_specs=[HBM] + ([pl.BlockSpec(memory_space=pl.ANY)] if rows else []),
        scratch_shapes=[
            pltpu.VMEM((planes, SY, SZ, K), jnp.bfloat16),
            pltpu.VMEM((4, INNER, K), jnp.float32),
            pltpu.VMEM((4, INNER, K), jnp.float32),
            pltpu.VMEM((2, BATCH * INNER, 2 * K), jnp.bfloat16),
            pltpu.VMEM((K, 2 * K), jnp.float32),
            pltpu.VMEM((2, SX, SY, SZ), jnp.float32),
            pltpu.VMEM((2, SX, SY, 128), jnp.float32),
            pltpu.VMEM((6 * SZ, 4 * SZ), jnp.bfloat16),
            pltpu.VMEM((6 * SZ, 5 * SZ), jnp.bfloat16),
            pltpu.VMEM((2 * SZ, 3 * SZ), jnp.bfloat16),
            pltpu.SemaphoreType.DMA((planes,)),
            pltpu.SemaphoreType.DMA((25,)),
        ],
        compiler_params=pltpu.CompilerParams(vmem_limit_bytes=26 * 1024 * 1024),
        cost_estimate=pl.CostEstimate(
            flops=1_800_000_000 * (last - first), transcendentals=0, bytes_accessed=2_000_000 * (last - first)
        ),
        name=f"inner{first}",
    )(*operands)


def outer_part(odd, m, v, vx, vy, bands, zf, zh, face, mat):
    return pl.pallas_call(
        outer_kernel,
        out_shape=[jax.ShapeDtypeStruct((K // 2, K), jnp.float32)] * 4,
        in_specs=[SMEM] + [HBM] * 9 + [VMEM] * 4,
        out_specs=[VMEM] * 4,
        scratch_shapes=[
            pltpu.VMEM((14, SZ, K), jnp.bfloat16),
            pltpu.VMEM((14, SZ, K), jnp.bfloat16),
            pltpu.VMEM((17 * SZ, K), jnp.bfloat16),
            pltpu.VMEM((3, SY, SZ, K), jnp.bfloat16),
            pltpu.VMEM((64, K), jnp.bfloat16),
            pltpu.VMEM((17, OUTER, K), jnp.float32),
            pltpu.VMEM((17, OUTER, K), jnp.float32),
            pltpu.VMEM((3, INNER, K), jnp.float32),
            pltpu.VMEM((3, INNER, K), jnp.float32),
            pltpu.VMEM((MAIN + FACE, 2 * K), jnp.bfloat16),
            pltpu.SemaphoreType.DMA((20,)),
            pltpu.VMEM((K, 2 * K), jnp.float32),
            pltpu.VMEM((2, 2, K // 2, K), jnp.float32),
            pltpu.VMEM((6 * SZ, 4 * SZ), jnp.bfloat16),
            pltpu.VMEM((6 * SZ, 5 * SZ), jnp.bfloat16),
            pltpu.VMEM((2 * SZ, 3 * SZ), jnp.bfloat16),
            pltpu.VMEM((4 * SZ, 3 * SZ), jnp.bfloat16),
            pltpu.VMEM((2 * FACE, FACE), jnp.bfloat16),
        ],
        compiler_params=pltpu.CompilerParams(vmem_limit_bytes=32 * 1024 * 1024),
        cost_estimate=pl.CostEstimate(flops=4_000_000_000, transcendentals=0, bytes_accessed=6_000_000),
        name="outer",
    )(odd, m, v, vx, vy, *bands, zf, zh, face, mat)


def pick(x, index, dim):
    return lax.dynamic_index_in_dim(x, index, dim, keepdims=False)


def reduce_to_owner(part):
    halves = [keep + send(other, lambda x, y, z: (x ^ 1, y, z)) for keep, other in (part[:2], part[2:])]
    groups = [[linear(x, y, z) for x in (c, c + 2) for y in range(NGY) for z in range(NGZ)] for c in range(2)]
    blocks = jnp.concatenate(halves, axis=1).reshape(64, 4, 2 * K)
    blocks = lax.all_to_all(blocks, ALL, 0, 0, tiled=True, axis_index_groups=groups)
    return jnp.sum(blocks, axis=0)


def to_parts(x):
    high = lax.reduce_precision(x, 8, 7)
    rest = x - high
    mid = lax.reduce_precision(rest, 8, 7)
    parts = jnp.concatenate([high, mid, rest - mid, jnp.zeros_like(x)], axis=1)
    return parts.astype(jnp.bfloat16)


def from_parts(rows):
    x = rows.astype(jnp.float32)
    return (x[:, 256:384] + x[:, 128:256]) + x[:, :128]


def face_rows(rows):
    return jnp.pad(rows.transpose(1, 0, 2), ((0, 0), (0, 7), (0, 0))).reshape(192, K)


def per_device(eigvecs, material):
    odd = lax.axis_index("gx") % 2 == 1
    upper = lax.axis_index("gz") == 1
    side = jnp.where(odd, SY - 1, 0)
    face = jnp.where(upper, 0, SZ - 1)
    odd_flag = odd.astype(jnp.int32).reshape(1)
    in_hbm = lambda x: pltpu.with_memory_space_constraint(x, pltpu.HBM)
    vectors = in_hbm(eigvecs)

    def chain(x, dim):
        return jnp.where(odd, lax.rev(x, (dim,)), x)

    zf = pick(eigvecs, face, 2)
    kface = jnp.pad(pick(material[0], face, 2), ((0, 0), (0, 120)))
    zm = send(jnp.concatenate([zf.reshape(SX * SY, K), to_parts(kface)], axis=0), to_z)
    bands = [in_hbm(band_matrix(ins, outs)) for ins, outs in NEAR]
    raw = in_hbm(material)
    m, xbuf = inner_part(*PIECES[0], odd_flag, None, vectors, raw, bands)
    zm, m = lax.optimization_barrier((zm, m))
    zh = zm[: SX * SY].reshape(SX, SY, K)
    kz = from_parts(zm[SX * SY :])[:, :SY]
    lanes = jnp.arange(128)
    own = jnp.pad(material, ((0, 0), (0, 0), (0, 0), (0, 128 - SZ)))
    matz = jnp.stack([jnp.where(lanes == 64, kz[..., None], own[0]), own[1]])
    rest = jnp.concatenate([zf[0], zh[0], to_parts(matz[:, 0].reshape(16, 128))], axis=0)
    vx = send(lax.dynamic_update_slice(xbuf, rest, (SY * SZ, 0)), to_x)
    m, ybuf = inner_part(*PIECES[1], odd_flag, in_hbm(m), vectors, raw, bands)
    vx, m = lax.optimization_barrier((vx, m))
    at = SY * SZ
    xf, xz = vx[at : at + SY], vx[at + SY : at + 2 * SY]
    xmat = from_parts(vx[at + 2 * SY :]).reshape(2, 1, SY, 128)
    matz = chain(jnp.concatenate([matz, xmat], axis=1), 2)
    frows = chain(jnp.concatenate([zf, xf[None]], axis=0), 1)
    zrows = chain(jnp.concatenate([zh, xz[None]], axis=0), 1)
    xline = lax.dynamic_slice_in_dim(vx, side * SZ, SZ, 0)
    gap = jnp.zeros((15, K), jnp.bfloat16)
    parts = to_parts(matz[:, :, 0].reshape(34, 128))
    rest = jnp.concatenate([xline, frows[:, 0], gap, zrows[:, 0], gap, parts], axis=0)
    vy = send(lax.dynamic_update_slice(ybuf, rest, (SX * SZ, 0)), to_y)
    zf = face_rows(frows)
    zh = face_rows(zrows)
    (m,) = inner_part(*PIECES[2], odd_flag, in_hbm(m), vectors, raw, bands)
    vy, m, zf, zh = lax.optimization_barrier((vy, m, zf, zh))
    my = from_parts(vy[17 * SZ + 64 :]).reshape(2, 17, 1, 128)
    matz = jnp.concatenate([matz, my], axis=2)
    grids = jnp.stack([pick(matz[0], face, 2), pick(matz[1], face, 2), matz[0, :, :, 64]])
    grids = jnp.pad(grids, ((0, 0), (0, 7), (0, 119)))
    mat = jnp.pad(matz, ((0, 0), (0, 0), (0, 7), (0, 0)))
    mat = jnp.where(lanes < SZ, mat, 0.0)
    bands = bands + [in_hbm(band_matrix(*EDGE)), in_hbm(face_matrix())]
    part = outer_part(odd_flag, in_hbm(m), vectors, vx, vy, bands, zf, zh, grids, mat)
    total = SX * SY * SZ * NGX * NGY * NGZ
    summed = reduce_to_owner(part) * (0.5 / total)
    return summed[:, :K], summed[:, K:]


def solution(mesh):
    return jax.shard_map(
        per_device,
        mesh=mesh,
        in_specs=(P("gx", "gy", "gz", None), P(None, "gx", "gy", "gz")),
        out_specs=(P(ALL, None), P(ALL, None)),
        check_vma=False,
    )
```

```python
import jax
import jax.numpy as jnp
import numpy as np
from jax import lax
from jax.experimental import pallas as pl
from jax.experimental.pallas import tpu as pltpu
from jax.sharding import PartitionSpec as P

ALL = ("gx", "gy", "gz")
NGX, NGY, NGZ = 4, 16, 2
SX, SY, SZ, K = 16, 8, 48, 512
NEAR = (((0, 1, 2, 3), (0, 1, 2)), ((2, 3, 4, 5, 6), (3, 4, 5)), ((5, 6, 7), (6,)))
EDGE = ((6, 7, 8), (7, 8))
INNER = 7 * SZ
OUTER = 2 * SZ
BATCH = 3
FACE = 224
MAIN = 15 * OUTER + 18 * SZ
PIECES = ((0, 1), (1, 2), (2, 5))


def linear(x, y, z):
    return (x * NGY + y) * NGZ + z


def send(value, move):
    links = []
    for x in range(NGX):
        for y in range(NGY):
            for z in range(NGZ):
                to = move(x, y, z)
                if 0 <= to[0] < NGX and 0 <= to[1] < NGY and 0 <= to[2] < NGZ:
                    links.append((linear(x, y, z), linear(*to)))
    return lax.ppermute(value, ALL, links)


def to_z(x, y, z):
    return (x, y, 1 - z)


def to_x(x, y, z):
    return (x - 1, y, z)


def to_y(x, y, z):
    return (x, y + 1, z) if x % 2 else (x, y - 1, z)


def chain_part(gap, ends, mid):
    return np.where(gap == 0, np.where(ends, 0.0, mid), np.where(gap == 1, 1.0, 0.0))


def band_matrix(lines_in, lines_out):
    size = len(lines_out) * SZ
    row, col = np.indices((2 * size, len(lines_in) * SZ))
    mid = np.where(row < size, 2.0, 4.0)
    cell = row % size
    line_out = lines_out[0] + cell // SZ
    line_in = lines_in[0] + col // SZ
    z_part = chain_part(np.abs(cell % SZ - col % SZ), False, mid)
    y_part = chain_part(np.abs(line_out - line_in), line_out == 8, mid)
    return jnp.asarray(y_part * z_part, jnp.bfloat16)


def face_matrix():
    row, col = np.indices((2 * FACE, FACE))
    mid = np.where(row < FACE, 2.0, 4.0)
    cell = row % FACE
    x_part = chain_part(np.abs(cell % 24 - col % 24), cell % 24 == SX, mid)
    y_part = chain_part(np.abs(cell // 24 - col // 24), cell // 24 == SY, mid)
    inside = (cell % 24 <= SX) & (col % 24 <= SX) & (cell // 24 <= SY) & (col // 24 <= SY)
    return jnp.asarray(np.where(inside, x_part * y_part, 0.0), jnp.bfloat16)


def apply_band(band, lines, size):
    r = jnp.dot(band, jnp.concatenate(lines, axis=0), preferred_element_type=jnp.float32)
    return r[:size], r[size:]


def kappa_yz(kappa):
    f = 2.0 * kappa + pltpu.roll(kappa, 1, 1) + pltpu.roll(kappa, 127, 1)
    rows = lax.broadcasted_iota(jnp.int32, f.shape, 0)
    below = jnp.where(rows == 0, 0.0, pltpu.roll(f, 1, 0))
    above = jnp.where(rows == f.shape[0] - 1, 0.0, pltpu.roll(f, f.shape[0] - 1, 0))
    mid = jnp.where(rows == 8, 0.0, 2.0 * f)
    return mid + below + above


def weights(kappa, rho, f, plane_own):
    own = 2.0 * kappa if plane_own else jnp.zeros_like(kappa)
    rows = lax.broadcasted_iota(jnp.int32, f.shape, 0)
    alpha = jnp.where(rows == 8, 0.0, own) + f * (1.0 / 32.0)
    return jnp.concatenate([alpha, kappa * (1.0 / 16.0), rho * (1.0 / 216.0)], axis=0).T[:SZ]


def store_products(u, row, v, w3, t3, c, line, stride):
    wide = (SZ, K)
    alpha = jnp.broadcast_to(c[:, line : line + 1], wide)
    kap = jnp.broadcast_to(c[:, stride + line : stride + line + 1], wide)
    rho = jnp.broadcast_to(c[:, 2 * stride + line : 2 * stride + line + 1], wide)
    u[row : row + SZ, 0:K] = (alpha * v.astype(jnp.float32) - kap * w3).astype(jnp.bfloat16)
    u[row : row + SZ, K : 2 * K] = (rho * t3).astype(jnp.bfloat16)


def gram(left, right):
    return lax.dot_general(left, right, (((0,), (0,)), ((), ())), preferred_element_type=jnp.float32)


def line_index(odd, c):
    return c + odd * (7 - 2 * c)


def mirror(x):
    rows = lax.broadcasted_iota(jnp.int32, x.shape, 0)
    for s in (4, 2, 1):
        x = jnp.where(rows % (2 * s) < s, pltpu.roll(x, 8 - s, 0), pltpu.roll(x, s, 0))
    return x


def inner_kernel(
    first, last, odd_ref, m_hbm, v_hbm, raw_hbm, hbm0, hbm1, hbm2, out_hbm,
    ve, w2, t2, u, acc, raw, mat_ref, band0, band1, band2, sem, sem_m,
):
    odd = odd_ref[0]
    bands = (band0, band1, band2)
    low = max(BATCH * first - 1, 0)
    loads = {
        p: pltpu.make_async_copy(v_hbm.at[p], ve.at[p - low], sem.at[p - low]) for p in range(low, BATCH * last + 1)
    }
    side = [
        pltpu.make_async_copy(a, b, sem_m.at[5 + n])
        for n, (a, b) in enumerate(((hbm0, band0), (hbm1, band1), (hbm2, band2), (raw_hbm, raw)))
    ]
    loads[low].start()
    for load in side:
        load.start()
    for p in range(low + 1, BATCH * last + 1):
        loads[p].start()
    place = [line_index(odd, c) for c in range(8)]
    if m_hbm is not None:
        load_m = pltpu.make_async_copy(m_hbm, acc, sem_m.at[4])
        load_m.start()
    side[3].wait()
    for i in range(2):
        for p in range(low, BATCH * last + 1):
            mat_ref[i, p] = jnp.zeros((SY, 128), jnp.float32)
            mat_ref[i, p, :, 0:SZ] = raw[i, p]
            x = mat_ref[i, p]
            mat_ref[i, p] = jnp.where(odd == 1, mirror(x), x)
    for load in side[:3]:
        load.wait()
    yz = {}

    def kappa_of(p):
        if p not in yz:
            yz[p] = kappa_yz(mat_ref[0, p])
        return yz[p]

    def filter_plane(p):
        for g, (ins, outs) in enumerate(NEAR):
            size = len(outs) * SZ
            a, b = apply_band(bands[g][...], [ve[p - low, place[l]] for l in ins], size)
            w2[p % 4, outs[0] * SZ : outs[0] * SZ + size] = a
            t2[p % 4, outs[0] * SZ : outs[0] * SZ + size] = b

    def plane_weights(p):
        f = 2.0 * kappa_of(p) + kappa_of(p + 1)
        if p:
            f = f + kappa_of(p - 1)
        return weights(mat_ref[0, p], mat_ref[1, p], f, True)

    def make_products(p, l, c, buf, base):
        rows = slice(l * SZ, (l + 1) * SZ)
        mid = w2[p % 4, rows]
        w3 = (mid + mid) + w2[(p + 1) % 4, rows]
        t3 = 4.0 * t2[p % 4, rows] + t2[(p + 1) % 4, rows]
        if p:
            w3 = w3 + w2[(p - 1) % 4, rows]
            t3 = t3 + t2[(p - 1) % 4, rows]
        store_products(u.at[buf], base + l * SZ, ve[p - low, place[l]], w3, t3, c, l, 8)

    def gram_piece(k, piece):
        cols = slice(piece * K, (piece + 1) * K)
        left = jnp.concatenate([ve[BATCH * k + q - low, place[l]] for q in range(BATCH) for l in range(7)], axis=0)
        part = gram(left, u[k % 2, :, cols])
        if k == first and m_hbm is None:
            acc[:, cols] = part
        else:
            acc[:, cols] += part
        if k == last - 1:
            pltpu.make_async_copy(acc.at[:, cols], out_hbm.at[:, cols], sem_m.at[piece]).start()

    ready = min(low + 4, BATCH * last + 1)
    for p in range(low, ready):
        loads[p].wait()
    done = low
    for k in range(first, last):
        if k == first + 1:
            for p in range(ready, BATCH * last + 1):
                loads[p].wait()
            if m_hbm is not None:
                load_m.wait()
        elif last == first + 1:
            for p in range(ready, BATCH * last + 1):
                loads[p].wait()
        pieces = list(range(2)) if k > first else []
        for q in range(BATCH):
            p = BATCH * k + q
            while done <= p + 1:
                filter_plane(done)
                done += 1
            c = plane_weights(p)
            for l in range(7):
                make_products(p, l, c, k % 2, q * INNER)
                if pieces and (q * 7 + l) % 10 == 0:
                    gram_piece(k - 1, pieces.pop(0))
        while pieces:
            gram_piece(k - 1, pieces.pop(0))
    if m_hbm is not None and last == first + 1:
        load_m.wait()
    for piece in range(2):
        gram_piece(last - 1, piece)
    for piece in range(2):
        cols = slice(piece * K, (piece + 1) * K)
        pltpu.make_async_copy(acc.at[:, cols], out_hbm.at[:, cols], sem_m.at[piece]).wait()


def outer_kernel(
    odd_ref, m_hbm, v_hbm, vx_hbm, vy_hbm, hbm0, hbm1, hbm2, hbm3, hbmz, zf_ref, zh_ref, face_ref, mat_ref,
    keep_s, send_s, keep_m, send_m,
    v6, v7, v8, vp, zl, w78, t78, w06, t06, u, sem, acc, res, band0, band1, band2, band3, bandz,
):
    odd = odd_ref[0]
    bands = (band0, band1, band2)
    early = [
        pltpu.make_async_copy(hbmz, bandz, sem.at[14]),
        pltpu.make_async_copy(vy_hbm.at[pl.ds(17 * SZ, 64)], zl, sem.at[15]),
    ]
    loads = [
        pltpu.make_async_copy(hbm3, band3, sem.at[19]),
        pltpu.make_async_copy(v_hbm.at[pl.ds(0, 14), line_index(odd, 6)], v6, sem.at[0]),
        pltpu.make_async_copy(v_hbm.at[pl.ds(0, 14), line_index(odd, 7)], v7, sem.at[1]),
        pltpu.make_async_copy(vy_hbm.at[pl.ds(0, 17 * SZ)], v8, sem.at[2]),
    ]
    late = [pltpu.make_async_copy(v_hbm.at[pl.ds(14, 2)], vp.at[pl.ds(0, 2)], sem.at[3])]
    for y in range(SY):
        late.append(pltpu.make_async_copy(vx_hbm.at[pl.ds(y * SZ, SZ)], vp.at[2, y], sem.at[5 + y]))
    for n, (a, b) in enumerate(((hbm0, band0), (hbm1, band1), (hbm2, band2))):
        late.append(pltpu.make_async_copy(a, b, sem.at[16 + n]))
    load_m = pltpu.make_async_copy(m_hbm, acc, sem.at[13])
    place = [line_index(odd, c) for c in range(8)]
    for load in early + loads + [load_m] + late:
        load.start()
    for load in early:
        load.wait()
    wz, tz = apply_band(bandz[...], [zh_ref[...], zl[32:64]], FACE)
    kap_face, rho_face, kap_halo = face_ref[0], face_ref[1], face_ref[2]
    planes = lax.broadcasted_iota(jnp.int32, kap_halo.shape, 0)
    lines = lax.broadcasted_iota(jnp.int32, kap_halo.shape, 1)
    f = jnp.where(planes == SX, 0.0, 2.0 * kap_halo) + pltpu.roll(kap_halo, 1, 0) + pltpu.roll(kap_halo, 23, 0)
    f = jnp.where(planes <= SX, f, 0.0)
    f = jnp.where(lines == SY, 0.0, 2.0 * f) + pltpu.roll(f, 1, 1) + pltpu.roll(f, 127, 1)
    f = f * (1.0 / 32.0)
    kap_face = kap_face * (1.0 / 16.0)
    rho_face = rho_face * (1.0 / 216.0)

    def column(grid):
        parts = [jnp.broadcast_to(grid[:, l : l + 1], (24, K)) for l in range(9)]
        return jnp.concatenate(parts + [jnp.zeros((8, K), jnp.float32)], axis=0)

    zf = jnp.concatenate([zf_ref[...], zl[0:32]], axis=0)
    uz = jnp.concatenate([column(f) * zf.astype(jnp.float32) - column(kap_face) * wz, column(rho_face) * tz], axis=1)
    u[MAIN:] = uz.astype(jnp.bfloat16)
    for load in loads:
        load.wait()

    def line(p, l):
        if l == 8:
            return v8[p * SZ : (p + 1) * SZ]
        if p >= 14:
            return vp[p - 14, place[l]]
        return v7[p] if l == 7 else v6[p]

    def filter_near(p):
        for g, (ins, outs) in enumerate(NEAR):
            size = len(outs) * SZ
            a, b = apply_band(bands[g][...], [line(p, l) for l in ins], size)
            w06[p - 14, outs[0] * SZ : outs[0] * SZ + size] = a
            t06[p - 14, outs[0] * SZ : outs[0] * SZ + size] = b

    def filter_edge(p):
        a, b = apply_band(band3[...], [line(p, l) for l in EDGE[0]], OUTER)
        w78[p] = a
        t78[p] = b

    def along_x(ref, p, lo, hi, rows, mid):
        if p == hi:
            return ref[p - 1 - lo, rows]
        r = mid * ref[p - lo, rows] + ref[p + 1 - lo, rows]
        if p > 0:
            r = r + ref[p - 1 - lo, rows]
        return r

    yz = [kappa_yz(mat_ref[0, p]) for p in range(17)]
    def make_products(p):
        if p == 16:
            f = yz[15]
        else:
            f = 2.0 * yz[p] + yz[p + 1]
            if p:
                f = f + yz[p - 1]
        c = weights(mat_ref[0, p], mat_ref[1, p], f, p != 16)
        for l in range(0 if p >= 15 else 7, 9):
            if p < 15:
                row = p * OUTER + (l - 7) * SZ
            else:
                row = 15 * OUTER + (p - 15) * 9 * SZ + l * SZ
            if l >= 7:
                rows = slice((l - 7) * SZ, (l - 6) * SZ)
                w3 = along_x(w78, p, 0, 16, rows, 2.0)
                t3 = along_x(t78, p, 0, 16, rows, 4.0)
            else:
                rows = slice(l * SZ, (l + 1) * SZ)
                w3 = along_x(w06, p, 14, 16, rows, 2.0)
                t3 = along_x(t06, p, 14, 16, rows, 4.0)
            store_products(u, row, line(p, l), w3, t3, c, l, 16)

    filter_edge(0)
    for p in range(17):
        if p < 16:
            filter_edge(p + 1)
            if p + 1 >= 14:
                filter_near(p + 1)
        make_products(p)
        if p == 7:
            load_m.wait()
            for load in late:
                load.wait()
            left = jnp.concatenate([line(q, l) for q in range(8) for l in (7, 8)], axis=0)
            acc[...] += gram(left, u[: 8 * OUTER])
    rows = [line(p, l) for p in range(8, 17) for l in range(0 if p >= 15 else 7, 9)]
    left = jnp.concatenate(rows + [zf], axis=0)
    acc[...] += gram(left, u[8 * OUTER :])

    def put(i, j, half, s):
        res[i % 2, half, (i // 2) * 128 : (i // 2 + 1) * 128, j * 128 : (j + 1) * 128] = s

    for half in range(2):
        for i in range(4):
            for j in range(i, 4):
                a = acc[i * 128 : (i + 1) * 128, half * K + j * 128 : half * K + (j + 1) * 128]
                b = acc[j * 128 : (j + 1) * 128, half * K + i * 128 : half * K + (i + 1) * 128]
                s = a + b.T
                put(i, j, half, s)
                if i != j:
                    put(j, i, half, s.T)
    for core in range(2):

        @pl.when(odd == core)
        def _():
            keep_s[...] = res[core, 0]
            send_s[...] = res[1 - core, 0]
            keep_m[...] = res[core, 1]
            send_m[...] = res[1 - core, 1]


HBM = pl.BlockSpec(memory_space=pltpu.HBM)
VMEM = pl.BlockSpec(memory_space=pltpu.VMEM)
SMEM = pl.BlockSpec(memory_space=pltpu.SMEM)


def inner_part(first, last, odd, m, v, mat, bands):
    def body(odd_ref, *refs):
        if m is None:
            refs = (None,) + refs
        inner_kernel(first, last, odd_ref, *refs)

    planes = BATCH * (last - first) + (2 if first else 1)
    operands = (odd,) + (() if m is None else (m,)) + (v, mat) + tuple(bands)
    specs = [SMEM] + [HBM] * (len(operands) - 1)
    return pl.pallas_call(
        body,
        out_shape=pltpu.HBM((K, 2 * K), jnp.float32),
        in_specs=specs,
        out_specs=HBM,
        scratch_shapes=[
            pltpu.VMEM((planes, SY, SZ, K), jnp.bfloat16),
            pltpu.VMEM((4, INNER, K), jnp.float32),
            pltpu.VMEM((4, INNER, K), jnp.float32),
            pltpu.VMEM((2, BATCH * INNER, 2 * K), jnp.bfloat16),
            pltpu.VMEM((K, 2 * K), jnp.float32),
            pltpu.VMEM((2, SX, SY, SZ), jnp.float32),
            pltpu.VMEM((2, SX, SY, 128), jnp.float32),
            pltpu.VMEM((6 * SZ, 4 * SZ), jnp.bfloat16),
            pltpu.VMEM((6 * SZ, 5 * SZ), jnp.bfloat16),
            pltpu.VMEM((2 * SZ, 3 * SZ), jnp.bfloat16),
            pltpu.SemaphoreType.DMA((planes,)),
            pltpu.SemaphoreType.DMA((9,)),
        ],
        compiler_params=pltpu.CompilerParams(vmem_limit_bytes=26 * 1024 * 1024),
        cost_estimate=pl.CostEstimate(
            flops=1_800_000_000 * (last - first), transcendentals=0, bytes_accessed=2_000_000 * (last - first)
        ),
        name=f"inner{first}",
    )(*operands)


def outer_part(odd, m, v, vx, vy, bands, zf, zh, face, mat):
    return pl.pallas_call(
        outer_kernel,
        out_shape=[jax.ShapeDtypeStruct((K // 2, K), jnp.float32)] * 4,
        in_specs=[SMEM] + [HBM] * 9 + [VMEM] * 4,
        out_specs=[VMEM] * 4,
        scratch_shapes=[
            pltpu.VMEM((14, SZ, K), jnp.bfloat16),
            pltpu.VMEM((14, SZ, K), jnp.bfloat16),
            pltpu.VMEM((17 * SZ, K), jnp.bfloat16),
            pltpu.VMEM((3, SY, SZ, K), jnp.bfloat16),
            pltpu.VMEM((64, K), jnp.bfloat16),
            pltpu.VMEM((17, OUTER, K), jnp.float32),
            pltpu.VMEM((17, OUTER, K), jnp.float32),
            pltpu.VMEM((3, INNER, K), jnp.float32),
            pltpu.VMEM((3, INNER, K), jnp.float32),
            pltpu.VMEM((MAIN + FACE, 2 * K), jnp.bfloat16),
            pltpu.SemaphoreType.DMA((20,)),
            pltpu.VMEM((K, 2 * K), jnp.float32),
            pltpu.VMEM((2, 2, K // 2, K), jnp.float32),
            pltpu.VMEM((6 * SZ, 4 * SZ), jnp.bfloat16),
            pltpu.VMEM((6 * SZ, 5 * SZ), jnp.bfloat16),
            pltpu.VMEM((2 * SZ, 3 * SZ), jnp.bfloat16),
            pltpu.VMEM((4 * SZ, 3 * SZ), jnp.bfloat16),
            pltpu.VMEM((2 * FACE, FACE), jnp.bfloat16),
        ],
        compiler_params=pltpu.CompilerParams(vmem_limit_bytes=32 * 1024 * 1024),
        cost_estimate=pl.CostEstimate(flops=4_000_000_000, transcendentals=0, bytes_accessed=6_000_000),
        name="outer",
    )(odd, m, v, vx, vy, *bands, zf, zh, face, mat)


def pick(x, index, dim):
    return lax.dynamic_index_in_dim(x, index, dim, keepdims=False)


def reduce_to_owner(part):
    halves = [keep + send(other, lambda x, y, z: (x ^ 1, y, z)) for keep, other in (part[:2], part[2:])]
    groups = [[linear(x, y, z) for x in (c, c + 2) for y in range(NGY) for z in range(NGZ)] for c in range(2)]
    blocks = jnp.concatenate(halves, axis=1).reshape(64, 4, 2 * K)
    blocks = lax.all_to_all(blocks, ALL, 0, 0, tiled=True, axis_index_groups=groups)
    return jnp.sum(blocks, axis=0)


def to_parts(x):
    high = lax.reduce_precision(x, 8, 7)
    rest = x - high
    mid = lax.reduce_precision(rest, 8, 7)
    parts = jnp.concatenate([high, mid, rest - mid, jnp.zeros_like(x)], axis=1)
    return parts.astype(jnp.bfloat16)


def from_parts(rows):
    x = rows.astype(jnp.float32)
    return (x[:, 256:384] + x[:, 128:256]) + x[:, :128]


def face_rows(rows):
    return jnp.pad(rows.transpose(1, 0, 2), ((0, 0), (0, 7), (0, 0))).reshape(192, K)


def per_device(eigvecs, material):
    odd = lax.axis_index("gx") % 2 == 1
    upper = lax.axis_index("gz") == 1
    side = jnp.where(odd, SY - 1, 0)
    face = jnp.where(upper, 0, SZ - 1)
    odd_flag = odd.astype(jnp.int32).reshape(1)
    in_hbm = lambda x: pltpu.with_memory_space_constraint(x, pltpu.HBM)
    vectors = in_hbm(eigvecs)

    def chain(x, dim):
        return jnp.where(odd, lax.rev(x, (dim,)), x)

    zf = pick(eigvecs, face, 2)
    kface = lax.dynamic_slice(material, (0, 0, 0, face), (1, SX, SY, 1)).reshape(SX, SY)
    kface = jnp.pad(kface, ((0, 0), (0, 120)))
    zm = send(jnp.concatenate([zf.reshape(SX * SY, K), to_parts(kface)], axis=0), to_z)
    bands = [in_hbm(band_matrix(ins, outs)) for ins, outs in NEAR]
    raw = in_hbm(material)
    m = inner_part(*PIECES[0], odd_flag, None, vectors, raw, bands)
    zm, m = lax.optimization_barrier((zm, m))
    zh = zm[: SX * SY].reshape(SX, SY, K)
    kz = from_parts(zm[SX * SY :])[:, :SY]
    lanes = jnp.arange(128)
    own = jnp.pad(material, ((0, 0), (0, 0), (0, 0), (0, 128 - SZ)))
    matz = jnp.stack([jnp.where(lanes == 64, kz[..., None], own[0]), own[1]])
    plane = eigvecs[0].reshape(SY * SZ, K)
    vx = send(jnp.concatenate([plane, zf[0], zh[0], to_parts(matz[:, 0].reshape(16, 128))], axis=0), to_x)
    m = inner_part(*PIECES[1], odd_flag, in_hbm(m), vectors, raw, bands)
    vx, m = lax.optimization_barrier((vx, m))
    at = SY * SZ
    xf, xz = vx[at : at + SY], vx[at + SY : at + 2 * SY]
    xmat = from_parts(vx[at + 2 * SY :]).reshape(2, 1, SY, 128)
    matz = chain(jnp.concatenate([matz, xmat], axis=1), 2)
    frows = chain(jnp.concatenate([zf, xf[None]], axis=0), 1)
    zrows = chain(jnp.concatenate([zh, xz[None]], axis=0), 1)
    lines = pick(eigvecs, side, 1).reshape(SX * SZ, K)
    xline = lax.dynamic_slice_in_dim(vx, side * SZ, SZ, 0)
    gap = jnp.zeros((15, K), jnp.bfloat16)
    parts = to_parts(matz[:, :, 0].reshape(34, 128))
    vy = send(jnp.concatenate([lines, xline, frows[:, 0], gap, zrows[:, 0], gap, parts], axis=0), to_y)
    zf = face_rows(frows)
    zh = face_rows(zrows)
    m = inner_part(*PIECES[2], odd_flag, in_hbm(m), vectors, raw, bands)
    vy, m, zf, zh = lax.optimization_barrier((vy, m, zf, zh))
    my = from_parts(vy[17 * SZ + 64 :]).reshape(2, 17, 1, 128)
    matz = jnp.concatenate([matz, my], axis=2)
    grids = jnp.stack([pick(matz[0], face, 2), pick(matz[1], face, 2), matz[0, :, :, 64]])
    grids = jnp.pad(grids, ((0, 0), (0, 7), (0, 119)))
    mat = jnp.pad(matz, ((0, 0), (0, 0), (0, 7), (0, 0)))
    mat = jnp.where(lanes < SZ, mat, 0.0)
    bands = bands + [in_hbm(band_matrix(*EDGE)), in_hbm(face_matrix())]
    part = outer_part(odd_flag, in_hbm(m), vectors, vx, vy, bands, zf, zh, grids, mat)
    total = SX * SY * SZ * NGX * NGY * NGZ
    summed = reduce_to_owner(part) * (0.5 / total)
    return summed[:, :K], summed[:, K:]


def solution(mesh):
    return jax.shard_map(
        per_device,
        mesh=mesh,
        in_specs=(P("gx", "gy", "gz", None), P(None, "gx", "gy", "gz")),
        out_specs=(P(ALL, None), P(ALL, None)),
        check_vma=False,
    )
```

```python
import jax
import jax.numpy as jnp
import numpy as np
from jax import lax
from jax.experimental import pallas as pl
from jax.experimental.pallas import tpu as pltpu
from jax.sharding import PartitionSpec as P

ALL = ("gx", "gy", "gz")
NGX, NGY, NGZ = 4, 16, 2
SX, SY, SZ, K = 16, 8, 48, 512
NEAR = (((0, 1, 2, 3), (0, 1, 2)), ((2, 3, 4, 5, 6), (3, 4, 5)), ((5, 6, 7), (6,)))
EDGE = ((6, 7, 8), (7, 8))
INNER = 7 * SZ
OUTER = 2 * SZ
BATCH = 3
FACE = 224
MAIN = 15 * OUTER + 18 * SZ
PIECES = ((0, 1), (1, 5))


def linear(x, y, z):
    return (x * NGY + y) * NGZ + z


def send(value, move):
    links = []
    for x in range(NGX):
        for y in range(NGY):
            for z in range(NGZ):
                to = move(x, y, z)
                if 0 <= to[0] < NGX and 0 <= to[1] < NGY and 0 <= to[2] < NGZ:
                    links.append((linear(x, y, z), linear(*to)))
    return lax.ppermute(value, ALL, links)


def to_z(x, y, z):
    return (x, y, 1 - z)


def to_x(x, y, z):
    return (x - 1, y, z)


def to_y(x, y, z):
    return (x, y + 1, z) if x % 2 else (x, y - 1, z)


def chain_part(gap, ends, mid):
    return np.where(gap == 0, np.where(ends, 0.0, mid), np.where(gap == 1, 1.0, 0.0))


def band_matrix(lines_in, lines_out):
    size = len(lines_out) * SZ
    row, col = np.indices((2 * size, len(lines_in) * SZ))
    mid = np.where(row < size, 2.0, 4.0)
    cell = row % size
    line_out = lines_out[0] + cell // SZ
    line_in = lines_in[0] + col // SZ
    z_part = chain_part(np.abs(cell % SZ - col % SZ), False, mid)
    y_part = chain_part(np.abs(line_out - line_in), line_out == 8, mid)
    return jnp.asarray(y_part * z_part, jnp.bfloat16)


def face_matrix():
    row, col = np.indices((2 * FACE, FACE))
    mid = np.where(row < FACE, 2.0, 4.0)
    cell = row % FACE
    x_part = chain_part(np.abs(cell % 24 - col % 24), cell % 24 == SX, mid)
    y_part = chain_part(np.abs(cell // 24 - col // 24), cell // 24 == SY, mid)
    inside = (cell % 24 <= SX) & (col % 24 <= SX) & (cell // 24 <= SY) & (col // 24 <= SY)
    return jnp.asarray(np.where(inside, x_part * y_part, 0.0), jnp.bfloat16)


def apply_band(band, lines, size):
    r = jnp.dot(band, jnp.concatenate(lines, axis=0), preferred_element_type=jnp.float32)
    return r[:size], r[size:]


def kappa_yz(kappa):
    f = 2.0 * kappa + pltpu.roll(kappa, 1, 1) + pltpu.roll(kappa, 127, 1)
    rows = lax.broadcasted_iota(jnp.int32, f.shape, 0)
    below = jnp.where(rows == 0, 0.0, pltpu.roll(f, 1, 0))
    above = jnp.where(rows == f.shape[0] - 1, 0.0, pltpu.roll(f, f.shape[0] - 1, 0))
    mid = jnp.where(rows == 8, 0.0, 2.0 * f)
    return mid + below + above


def weights(kappa, rho, f, plane_own):
    own = 2.0 * kappa if plane_own else jnp.zeros_like(kappa)
    rows = lax.broadcasted_iota(jnp.int32, f.shape, 0)
    alpha = jnp.where(rows == 8, 0.0, own) + f * (1.0 / 32.0)
    return jnp.concatenate([alpha, kappa * (1.0 / 16.0), rho * (1.0 / 216.0)], axis=0).T[:SZ]


def store_products(u, row, v, w3, t3, c, line, stride):
    wide = (SZ, K)
    alpha = jnp.broadcast_to(c[:, line : line + 1], wide)
    kap = jnp.broadcast_to(c[:, stride + line : stride + line + 1], wide)
    rho = jnp.broadcast_to(c[:, 2 * stride + line : 2 * stride + line + 1], wide)
    u[row : row + SZ, 0:K] = (alpha * v.astype(jnp.float32) - kap * w3).astype(jnp.bfloat16)
    u[row : row + SZ, K : 2 * K] = (rho * t3).astype(jnp.bfloat16)


def gram(left, right):
    return lax.dot_general(left, right, (((0,), (0,)), ((), ())), preferred_element_type=jnp.float32)


def line_index(odd, c):
    return c + odd * (7 - 2 * c)


def mirror(x):
    rows = lax.broadcasted_iota(jnp.int32, x.shape, 0)
    for s in (4, 2, 1):
        x = jnp.where(rows % (2 * s) < s, pltpu.roll(x, 8 - s, 0), pltpu.roll(x, s, 0))
    return x


def inner_kernel(
    first, last, odd_ref, m_hbm, v_hbm, raw_hbm, hbm0, hbm1, hbm2, out_hbm,
    ve, w2, t2, u, acc, raw, mat_ref, band0, band1, band2, sem, sem_m,
):
    odd = odd_ref[0]
    bands = (band0, band1, band2)
    low = max(BATCH * first - 1, 0)
    loads = {
        p: pltpu.make_async_copy(v_hbm.at[p], ve.at[p - low], sem.at[p - low]) for p in range(low, BATCH * last + 1)
    }
    side = [
        pltpu.make_async_copy(a, b, sem_m.at[5 + n])
        for n, (a, b) in enumerate(((hbm0, band0), (hbm1, band1), (hbm2, band2), (raw_hbm, raw)))
    ]
    loads[low].start()
    for load in side:
        load.start()
    for p in range(low + 1, BATCH * last + 1):
        loads[p].start()
    place = [line_index(odd, c) for c in range(8)]
    if m_hbm is not None:
        load_m = pltpu.make_async_copy(m_hbm, acc, sem_m.at[4])
        load_m.start()
    side[3].wait()
    for i in range(2):
        for p in range(low, BATCH * last + 1):
            mat_ref[i, p] = jnp.zeros((SY, 128), jnp.float32)
            mat_ref[i, p, :, 0:SZ] = raw[i, p]
            x = mat_ref[i, p]
            mat_ref[i, p] = jnp.where(odd == 1, mirror(x), x)
    for load in side[:3]:
        load.wait()
    yz = {}

    def kappa_of(p):
        if p not in yz:
            yz[p] = kappa_yz(mat_ref[0, p])
        return yz[p]

    def filter_plane(p):
        for g, (ins, outs) in enumerate(NEAR):
            size = len(outs) * SZ
            a, b = apply_band(bands[g][...], [ve[p - low, place[l]] for l in ins], size)
            w2[p % 4, outs[0] * SZ : outs[0] * SZ + size] = a
            t2[p % 4, outs[0] * SZ : outs[0] * SZ + size] = b

    def plane_weights(p):
        f = 2.0 * kappa_of(p) + kappa_of(p + 1)
        if p:
            f = f + kappa_of(p - 1)
        return weights(mat_ref[0, p], mat_ref[1, p], f, True)

    def make_products(p, l, c, buf, base):
        rows = slice(l * SZ, (l + 1) * SZ)
        mid = w2[p % 4, rows]
        w3 = (mid + mid) + w2[(p + 1) % 4, rows]
        t3 = 4.0 * t2[p % 4, rows] + t2[(p + 1) % 4, rows]
        if p:
            w3 = w3 + w2[(p - 1) % 4, rows]
            t3 = t3 + t2[(p - 1) % 4, rows]
        store_products(u.at[buf], base + l * SZ, ve[p - low, place[l]], w3, t3, c, l, 8)

    def gram_piece(k, piece):
        cols = slice(piece * K, (piece + 1) * K)
        left = jnp.concatenate([ve[BATCH * k + q - low, place[l]] for q in range(BATCH) for l in range(7)], axis=0)
        part = gram(left, u[k % 2, :, cols])
        if k == first and m_hbm is None:
            acc[:, cols] = part
        else:
            acc[:, cols] += part
        if k == last - 1:
            pltpu.make_async_copy(acc.at[:, cols], out_hbm.at[:, cols], sem_m.at[piece]).start()

    ready = min(low + 4, BATCH * last + 1)
    for p in range(low, ready):
        loads[p].wait()
    done = low
    for k in range(first, last):
        if k == first + 1:
            for p in range(ready, BATCH * last + 1):
                loads[p].wait()
            if m_hbm is not None:
                load_m.wait()
        elif last == first + 1:
            for p in range(ready, BATCH * last + 1):
                loads[p].wait()
        pieces = list(range(2)) if k > first else []
        for q in range(BATCH):
            p = BATCH * k + q
            while done <= p + 1:
                filter_plane(done)
                done += 1
            c = plane_weights(p)
            for l in range(7):
                make_products(p, l, c, k % 2, q * INNER)
                if pieces and (q * 7 + l) % 10 == 0:
                    gram_piece(k - 1, pieces.pop(0))
        while pieces:
            gram_piece(k - 1, pieces.pop(0))
    if m_hbm is not None and last == first + 1:
        load_m.wait()
    for piece in range(2):
        gram_piece(last - 1, piece)
    for piece in range(2):
        cols = slice(piece * K, (piece + 1) * K)
        pltpu.make_async_copy(acc.at[:, cols], out_hbm.at[:, cols], sem_m.at[piece]).wait()


def outer_kernel(
    odd_ref, m_hbm, v_hbm, vx_hbm, vy_hbm, hbm0, hbm1, hbm2, hbm3, hbmz, zf_ref, zh_ref, face_ref, mat_ref,
    keep_s, send_s, keep_m, send_m,
    v6, v7, v8, vp, zl, w78, t78, w06, t06, u, sem, acc, res, band0, band1, band2, band3, bandz,
):
    odd = odd_ref[0]
    bands = (band0, band1, band2)
    early = [
        pltpu.make_async_copy(hbmz, bandz, sem.at[14]),
        pltpu.make_async_copy(vy_hbm.at[pl.ds(17 * SZ, 64)], zl, sem.at[15]),
    ]
    loads = [
        pltpu.make_async_copy(hbm3, band3, sem.at[19]),
        pltpu.make_async_copy(v_hbm.at[pl.ds(0, 14), line_index(odd, 6)], v6, sem.at[0]),
        pltpu.make_async_copy(v_hbm.at[pl.ds(0, 14), line_index(odd, 7)], v7, sem.at[1]),
        pltpu.make_async_copy(vy_hbm.at[pl.ds(0, 17 * SZ)], v8, sem.at[2]),
    ]
    late = [pltpu.make_async_copy(v_hbm.at[pl.ds(14, 2)], vp.at[pl.ds(0, 2)], sem.at[3])]
    for y in range(SY):
        late.append(pltpu.make_async_copy(vx_hbm.at[pl.ds(y * SZ, SZ)], vp.at[2, y], sem.at[5 + y]))
    for n, (a, b) in enumerate(((hbm0, band0), (hbm1, band1), (hbm2, band2))):
        late.append(pltpu.make_async_copy(a, b, sem.at[16 + n]))
    load_m = pltpu.make_async_copy(m_hbm, acc, sem.at[13])
    place = [line_index(odd, c) for c in range(8)]
    for load in early + loads + [load_m] + late:
        load.start()
    for load in early:
        load.wait()
    wz, tz = apply_band(bandz[...], [zh_ref[...], zl[32:64]], FACE)
    kap_face, rho_face, kap_halo = face_ref[0], face_ref[1], face_ref[2]
    planes = lax.broadcasted_iota(jnp.int32, kap_halo.shape, 0)
    lines = lax.broadcasted_iota(jnp.int32, kap_halo.shape, 1)
    f = jnp.where(planes == SX, 0.0, 2.0 * kap_halo) + pltpu.roll(kap_halo, 1, 0) + pltpu.roll(kap_halo, 23, 0)
    f = jnp.where(planes <= SX, f, 0.0)
    f = jnp.where(lines == SY, 0.0, 2.0 * f) + pltpu.roll(f, 1, 1) + pltpu.roll(f, 127, 1)
    f = f * (1.0 / 32.0)
    kap_face = kap_face * (1.0 / 16.0)
    rho_face = rho_face * (1.0 / 216.0)

    def column(grid):
        parts = [jnp.broadcast_to(grid[:, l : l + 1], (24, K)) for l in range(9)]
        return jnp.concatenate(parts + [jnp.zeros((8, K), jnp.float32)], axis=0)

    zf = jnp.concatenate([zf_ref[...], zl[0:32]], axis=0)
    uz = jnp.concatenate([column(f) * zf.astype(jnp.float32) - column(kap_face) * wz, column(rho_face) * tz], axis=1)
    u[MAIN:] = uz.astype(jnp.bfloat16)
    for load in loads:
        load.wait()

    def line(p, l):
        if l == 8:
            return v8[p * SZ : (p + 1) * SZ]
        if p >= 14:
            return vp[p - 14, place[l]]
        return v7[p] if l == 7 else v6[p]

    def filter_near(p):
        for g, (ins, outs) in enumerate(NEAR):
            size = len(outs) * SZ
            a, b = apply_band(bands[g][...], [line(p, l) for l in ins], size)
            w06[p - 14, outs[0] * SZ : outs[0] * SZ + size] = a
            t06[p - 14, outs[0] * SZ : outs[0] * SZ + size] = b

    def filter_edge(p):
        a, b = apply_band(band3[...], [line(p, l) for l in EDGE[0]], OUTER)
        w78[p] = a
        t78[p] = b

    def along_x(ref, p, lo, hi, rows, mid):
        if p == hi:
            return ref[p - 1 - lo, rows]
        r = mid * ref[p - lo, rows] + ref[p + 1 - lo, rows]
        if p > 0:
            r = r + ref[p - 1 - lo, rows]
        return r

    yz = [kappa_yz(mat_ref[0, p]) for p in range(17)]
    def make_products(p):
        if p == 16:
            f = yz[15]
        else:
            f = 2.0 * yz[p] + yz[p + 1]
            if p:
                f = f + yz[p - 1]
        c = weights(mat_ref[0, p], mat_ref[1, p], f, p != 16)
        for l in range(0 if p >= 15 else 7, 9):
            if p < 15:
                row = p * OUTER + (l - 7) * SZ
            else:
                row = 15 * OUTER + (p - 15) * 9 * SZ + l * SZ
            if l >= 7:
                rows = slice((l - 7) * SZ, (l - 6) * SZ)
                w3 = along_x(w78, p, 0, 16, rows, 2.0)
                t3 = along_x(t78, p, 0, 16, rows, 4.0)
            else:
                rows = slice(l * SZ, (l + 1) * SZ)
                w3 = along_x(w06, p, 14, 16, rows, 2.0)
                t3 = along_x(t06, p, 14, 16, rows, 4.0)
            store_products(u, row, line(p, l), w3, t3, c, l, 16)

    filter_edge(0)
    for p in range(17):
        if p < 16:
            filter_edge(p + 1)
            if p + 1 >= 14:
                filter_near(p + 1)
        make_products(p)
        if p == 7:
            load_m.wait()
            for load in late:
                load.wait()
            left = jnp.concatenate([line(q, l) for q in range(8) for l in (7, 8)], axis=0)
            acc[...] += gram(left, u[: 8 * OUTER])
    rows = [line(p, l) for p in range(8, 17) for l in range(0 if p >= 15 else 7, 9)]
    left = jnp.concatenate(rows + [zf], axis=0)
    acc[...] += gram(left, u[8 * OUTER :])

    def put(i, j, half, s):
        res[i % 2, half, (i // 2) * 128 : (i // 2 + 1) * 128, j * 128 : (j + 1) * 128] = s

    for half in range(2):
        for i in range(4):
            for j in range(i, 4):
                a = acc[i * 128 : (i + 1) * 128, half * K + j * 128 : half * K + (j + 1) * 128]
                b = acc[j * 128 : (j + 1) * 128, half * K + i * 128 : half * K + (i + 1) * 128]
                s = a + b.T
                put(i, j, half, s)
                if i != j:
                    put(j, i, half, s.T)
    for core in range(2):

        @pl.when(odd == core)
        def _():
            keep_s[...] = res[core, 0]
            send_s[...] = res[1 - core, 0]
            keep_m[...] = res[core, 1]
            send_m[...] = res[1 - core, 1]


HBM = pl.BlockSpec(memory_space=pltpu.HBM)
VMEM = pl.BlockSpec(memory_space=pltpu.VMEM)
SMEM = pl.BlockSpec(memory_space=pltpu.SMEM)


def inner_part(first, last, odd, m, v, mat, bands):
    def body(odd_ref, *refs):
        if m is None:
            refs = (None,) + refs
        inner_kernel(first, last, odd_ref, *refs)

    planes = BATCH * (last - first) + (2 if first else 1)
    operands = (odd,) + (() if m is None else (m,)) + (v, mat) + tuple(bands)
    specs = [SMEM] + [HBM] * (len(operands) - 1)
    return pl.pallas_call(
        body,
        out_shape=pltpu.HBM((K, 2 * K), jnp.float32),
        in_specs=specs,
        out_specs=HBM,
        scratch_shapes=[
            pltpu.VMEM((planes, SY, SZ, K), jnp.bfloat16),
            pltpu.VMEM((4, INNER, K), jnp.float32),
            pltpu.VMEM((4, INNER, K), jnp.float32),
            pltpu.VMEM((2, BATCH * INNER, 2 * K), jnp.bfloat16),
            pltpu.VMEM((K, 2 * K), jnp.float32),
            pltpu.VMEM((2, SX, SY, SZ), jnp.float32),
            pltpu.VMEM((2, SX, SY, 128), jnp.float32),
            pltpu.VMEM((6 * SZ, 4 * SZ), jnp.bfloat16),
            pltpu.VMEM((6 * SZ, 5 * SZ), jnp.bfloat16),
            pltpu.VMEM((2 * SZ, 3 * SZ), jnp.bfloat16),
            pltpu.SemaphoreType.DMA((planes,)),
            pltpu.SemaphoreType.DMA((9,)),
        ],
        compiler_params=pltpu.CompilerParams(vmem_limit_bytes=26 * 1024 * 1024),
        cost_estimate=pl.CostEstimate(
            flops=1_800_000_000 * (last - first), transcendentals=0, bytes_accessed=2_000_000 * (last - first)
        ),
        name=f"inner{first}",
    )(*operands)


def outer_part(odd, m, v, vx, vy, bands, zf, zh, face, mat):
    return pl.pallas_call(
        outer_kernel,
        out_shape=[jax.ShapeDtypeStruct((K // 2, K), jnp.float32)] * 4,
        in_specs=[SMEM] + [HBM] * 9 + [VMEM] * 4,
        out_specs=[VMEM] * 4,
        scratch_shapes=[
            pltpu.VMEM((14, SZ, K), jnp.bfloat16),
            pltpu.VMEM((14, SZ, K), jnp.bfloat16),
            pltpu.VMEM((17 * SZ, K), jnp.bfloat16),
            pltpu.VMEM((3, SY, SZ, K), jnp.bfloat16),
            pltpu.VMEM((64, K), jnp.bfloat16),
            pltpu.VMEM((17, OUTER, K), jnp.float32),
            pltpu.VMEM((17, OUTER, K), jnp.float32),
            pltpu.VMEM((3, INNER, K), jnp.float32),
            pltpu.VMEM((3, INNER, K), jnp.float32),
            pltpu.VMEM((MAIN + FACE, 2 * K), jnp.bfloat16),
            pltpu.SemaphoreType.DMA((20,)),
            pltpu.VMEM((K, 2 * K), jnp.float32),
            pltpu.VMEM((2, 2, K // 2, K), jnp.float32),
            pltpu.VMEM((6 * SZ, 4 * SZ), jnp.bfloat16),
            pltpu.VMEM((6 * SZ, 5 * SZ), jnp.bfloat16),
            pltpu.VMEM((2 * SZ, 3 * SZ), jnp.bfloat16),
            pltpu.VMEM((4 * SZ, 3 * SZ), jnp.bfloat16),
            pltpu.VMEM((2 * FACE, FACE), jnp.bfloat16),
        ],
        compiler_params=pltpu.CompilerParams(vmem_limit_bytes=32 * 1024 * 1024),
        cost_estimate=pl.CostEstimate(flops=4_000_000_000, transcendentals=0, bytes_accessed=6_000_000),
        name="outer",
    )(odd, m, v, vx, vy, *bands, zf, zh, face, mat)


def pick(x, index, dim):
    return lax.dynamic_index_in_dim(x, index, dim, keepdims=False)


def reduce_to_owner(part):
    halves = [keep + send(other, lambda x, y, z: (x ^ 1, y, z)) for keep, other in (part[:2], part[2:])]
    groups = [[linear(x, y, z) for x in (c, c + 2) for y in range(NGY) for z in range(NGZ)] for c in range(2)]
    blocks = jnp.concatenate(halves, axis=1).reshape(64, 4, 2 * K)
    blocks = lax.all_to_all(blocks, ALL, 0, 0, tiled=True, axis_index_groups=groups)
    return jnp.sum(blocks, axis=0)


def to_parts(x):
    high = lax.reduce_precision(x, 8, 7)
    rest = x - high
    mid = lax.reduce_precision(rest, 8, 7)
    parts = jnp.concatenate([high, mid, rest - mid, jnp.zeros_like(x)], axis=1)
    return parts.astype(jnp.bfloat16)


def from_parts(rows):
    x = rows.astype(jnp.float32)
    return (x[:, 256:384] + x[:, 128:256]) + x[:, :128]


def face_rows(rows):
    return jnp.pad(rows.transpose(1, 0, 2), ((0, 0), (0, 7), (0, 0))).reshape(192, K)


def per_device(eigvecs, material):
    odd = lax.axis_index("gx") % 2 == 1
    upper = lax.axis_index("gz") == 1
    side = jnp.where(odd, SY - 1, 0)
    face = jnp.where(upper, 0, SZ - 1)
    odd_flag = odd.astype(jnp.int32).reshape(1)
    in_hbm = lambda x: pltpu.with_memory_space_constraint(x, pltpu.HBM)
    vectors = in_hbm(eigvecs)

    def chain(x, dim):
        return jnp.where(odd, lax.rev(x, (dim,)), x)

    zf = pick(eigvecs, face, 2)
    kface = lax.dynamic_slice(material, (0, 0, 0, face), (1, SX, SY, 1)).reshape(SX, SY)
    kface = jnp.pad(kface, ((0, 0), (0, 120)))
    zm = send(jnp.concatenate([zf.reshape(SX * SY, K), to_parts(kface)], axis=0), to_z)
    zm, odd_flag = lax.optimization_barrier((zm, odd_flag))
    bands = [in_hbm(band_matrix(ins, outs)) for ins, outs in NEAR]
    raw = in_hbm(material)
    zh = zm[: SX * SY].reshape(SX, SY, K)
    kz = from_parts(zm[SX * SY :])[:, :SY]
    lanes = jnp.arange(128)
    own = jnp.pad(material, ((0, 0), (0, 0), (0, 0), (0, 128 - SZ)))
    matz = jnp.stack([jnp.where(lanes == 64, kz[..., None], own[0]), own[1]])
    plane = eigvecs[0].reshape(SY * SZ, K)
    vx = send(jnp.concatenate([plane, zf[0], zh[0], to_parts(matz[:, 0].reshape(16, 128))], axis=0), to_x)
    m = inner_part(*PIECES[0], odd_flag, None, vectors, raw, bands)
    vx, m = lax.optimization_barrier((vx, m))
    at = SY * SZ
    xf, xz = vx[at : at + SY], vx[at + SY : at + 2 * SY]
    xmat = from_parts(vx[at + 2 * SY :]).reshape(2, 1, SY, 128)
    matz = chain(jnp.concatenate([matz, xmat], axis=1), 2)
    frows = chain(jnp.concatenate([zf, xf[None]], axis=0), 1)
    zrows = chain(jnp.concatenate([zh, xz[None]], axis=0), 1)
    lines = pick(eigvecs, side, 1).reshape(SX * SZ, K)
    xline = lax.dynamic_slice_in_dim(vx, side * SZ, SZ, 0)
    gap = jnp.zeros((15, K), jnp.bfloat16)
    parts = to_parts(matz[:, :, 0].reshape(34, 128))
    vy = send(jnp.concatenate([lines, xline, frows[:, 0], gap, zrows[:, 0], gap, parts], axis=0), to_y)
    zf = face_rows(frows)
    zh = face_rows(zrows)
    m = inner_part(*PIECES[1], odd_flag, in_hbm(m), vectors, raw, bands)
    vy, m, zf, zh = lax.optimization_barrier((vy, m, zf, zh))
    my = from_parts(vy[17 * SZ + 64 :]).reshape(2, 17, 1, 128)
    matz = jnp.concatenate([matz, my], axis=2)
    grids = jnp.stack([pick(matz[0], face, 2), pick(matz[1], face, 2), matz[0, :, :, 64]])
    grids = jnp.pad(grids, ((0, 0), (0, 7), (0, 119)))
    mat = jnp.pad(matz, ((0, 0), (0, 0), (0, 7), (0, 0)))
    mat = jnp.where(lanes < SZ, mat, 0.0)
    bands = bands + [in_hbm(band_matrix(*EDGE)), in_hbm(face_matrix())]
    part = outer_part(odd_flag, in_hbm(m), vectors, vx, vy, bands, zf, zh, grids, mat)
    total = SX * SY * SZ * NGX * NGY * NGZ
    summed = reduce_to_owner(part) * (0.5 / total)
    return summed[:, :K], summed[:, K:]


def solution(mesh):
    return jax.shard_map(
        per_device,
        mesh=mesh,
        in_specs=(P("gx", "gy", "gz", None), P(None, "gx", "gy", "gz")),
        out_specs=(P(ALL, None), P(ALL, None)),
        check_vma=False,
    )
```

```python
import jax
import jax.numpy as jnp
import numpy as np
from jax import lax
from jax.experimental import pallas as pl
from jax.experimental.pallas import tpu as pltpu
from jax.sharding import PartitionSpec as P

ALL = ("gx", "gy", "gz")
NGX, NGY, NGZ = 4, 16, 2
SX, SY, SZ, K = 16, 8, 48, 512
NEAR = (((0, 1, 2, 3), (0, 1, 2)), ((2, 3, 4, 5, 6), (3, 4, 5)), ((5, 6, 7), (6,)))
EDGE = ((6, 7, 8), (7, 8))
INNER = 7 * SZ
OUTER = 2 * SZ
BATCH = 3
FACE = 224
MAIN = 15 * OUTER + 18 * SZ
PIECES = ((0, 1), (1, 5))


def linear(x, y, z):
    return (x * NGY + y) * NGZ + z


def send(value, move):
    links = []
    for x in range(NGX):
        for y in range(NGY):
            for z in range(NGZ):
                to = move(x, y, z)
                if 0 <= to[0] < NGX and 0 <= to[1] < NGY and 0 <= to[2] < NGZ:
                    links.append((linear(x, y, z), linear(*to)))
    return lax.ppermute(value, ALL, links)


def to_z(x, y, z):
    return (x, y, 1 - z)


def to_x(x, y, z):
    return (x - 1, y, z)


def to_y(x, y, z):
    return (x, y + 1, z) if x % 2 else (x, y - 1, z)


def chain_part(gap, ends, mid):
    return np.where(gap == 0, np.where(ends, 0.0, mid), np.where(gap == 1, 1.0, 0.0))


def band_matrix(lines_in, lines_out):
    size = len(lines_out) * SZ
    row, col = np.indices((2 * size, len(lines_in) * SZ))
    mid = np.where(row < size, 2.0, 4.0)
    cell = row % size
    line_out = lines_out[0] + cell // SZ
    line_in = lines_in[0] + col // SZ
    z_part = chain_part(np.abs(cell % SZ - col % SZ), False, mid)
    y_part = chain_part(np.abs(line_out - line_in), line_out == 8, mid)
    return jnp.asarray(y_part * z_part, jnp.bfloat16)


def face_matrix():
    row, col = np.indices((2 * FACE, FACE))
    mid = np.where(row < FACE, 2.0, 4.0)
    cell = row % FACE
    x_part = chain_part(np.abs(cell % 24 - col % 24), cell % 24 == SX, mid)
    y_part = chain_part(np.abs(cell // 24 - col // 24), cell // 24 == SY, mid)
    inside = (cell % 24 <= SX) & (col % 24 <= SX) & (cell // 24 <= SY) & (col // 24 <= SY)
    return jnp.asarray(np.where(inside, x_part * y_part, 0.0), jnp.bfloat16)


def apply_band(band, lines, size):
    r = jnp.dot(band, jnp.concatenate(lines, axis=0), preferred_element_type=jnp.float32)
    return r[:size], r[size:]


def kappa_yz(kappa):
    f = 2.0 * kappa + pltpu.roll(kappa, 1, 1) + pltpu.roll(kappa, 127, 1)
    rows = lax.broadcasted_iota(jnp.int32, f.shape, 0)
    below = jnp.where(rows == 0, 0.0, pltpu.roll(f, 1, 0))
    above = jnp.where(rows == f.shape[0] - 1, 0.0, pltpu.roll(f, f.shape[0] - 1, 0))
    mid = jnp.where(rows == 8, 0.0, 2.0 * f)
    return mid + below + above


def weights(kappa, rho, f, plane_own):
    own = 2.0 * kappa if plane_own else jnp.zeros_like(kappa)
    rows = lax.broadcasted_iota(jnp.int32, f.shape, 0)
    alpha = jnp.where(rows == 8, 0.0, own) + f * (1.0 / 32.0)
    return jnp.concatenate([alpha, kappa * (1.0 / 16.0), rho * (1.0 / 216.0)], axis=0).T[:SZ]


def store_products(u, row, v, w3, t3, c, line, stride):
    wide = (SZ, K)
    alpha = jnp.broadcast_to(c[:, line : line + 1], wide)
    kap = jnp.broadcast_to(c[:, stride + line : stride + line + 1], wide)
    rho = jnp.broadcast_to(c[:, 2 * stride + line : 2 * stride + line + 1], wide)
    u[row : row + SZ, 0:K] = (alpha * v.astype(jnp.float32) - kap * w3).astype(jnp.bfloat16)
    u[row : row + SZ, K : 2 * K] = (rho * t3).astype(jnp.bfloat16)


def gram(left, right):
    return lax.dot_general(left, right, (((0,), (0,)), ((), ())), preferred_element_type=jnp.float32)


def line_index(odd, c):
    return c + odd * (7 - 2 * c)


def mirror(x):
    rows = lax.broadcasted_iota(jnp.int32, x.shape, 0)
    for s in (4, 2, 1):
        x = jnp.where(rows % (2 * s) < s, pltpu.roll(x, 8 - s, 0), pltpu.roll(x, s, 0))
    return x


def inner_kernel(
    first, last, odd_ref, m_hbm, v_hbm, raw_hbm, hbm0, hbm1, hbm2, out_hbm,
    ve, w2, t2, u, acc, raw, mat_ref, band0, band1, band2, sem, sem_m,
):
    odd = odd_ref[0]
    bands = (band0, band1, band2)
    low = max(BATCH * first - 1, 0)
    loads = {
        p: pltpu.make_async_copy(v_hbm.at[p], ve.at[p - low], sem.at[p - low]) for p in range(low, BATCH * last + 1)
    }
    side = [
        pltpu.make_async_copy(a, b, sem_m.at[5 + n])
        for n, (a, b) in enumerate(((hbm0, band0), (hbm1, band1), (hbm2, band2), (raw_hbm, raw)))
    ]
    loads[low].start()
    for load in side:
        load.start()
    for p in range(low + 1, BATCH * last + 1):
        loads[p].start()
    place = [line_index(odd, c) for c in range(8)]
    if m_hbm is not None:
        load_m = pltpu.make_async_copy(m_hbm, acc, sem_m.at[4])
        load_m.start()
    side[3].wait()
    for i in range(2):
        for p in range(low, BATCH * last + 1):
            mat_ref[i, p] = jnp.zeros((SY, 128), jnp.float32)
            mat_ref[i, p, :, 0:SZ] = raw[i, p]
            x = mat_ref[i, p]
            mat_ref[i, p] = jnp.where(odd == 1, mirror(x), x)
    for load in side[:3]:
        load.wait()
    yz = {}

    def kappa_of(p):
        if p not in yz:
            yz[p] = kappa_yz(mat_ref[0, p])
        return yz[p]

    def filter_plane(p):
        for g, (ins, outs) in enumerate(NEAR):
            size = len(outs) * SZ
            a, b = apply_band(bands[g][...], [ve[p - low, place[l]] for l in ins], size)
            w2[p % 4, outs[0] * SZ : outs[0] * SZ + size] = a
            t2[p % 4, outs[0] * SZ : outs[0] * SZ + size] = b

    def plane_weights(p):
        f = 2.0 * kappa_of(p) + kappa_of(p + 1)
        if p:
            f = f + kappa_of(p - 1)
        return weights(mat_ref[0, p], mat_ref[1, p], f, True)

    def make_products(p, l, c, buf, base):
        rows = slice(l * SZ, (l + 1) * SZ)
        mid = w2[p % 4, rows]
        w3 = (mid + mid) + w2[(p + 1) % 4, rows]
        t3 = 4.0 * t2[p % 4, rows] + t2[(p + 1) % 4, rows]
        if p:
            w3 = w3 + w2[(p - 1) % 4, rows]
            t3 = t3 + t2[(p - 1) % 4, rows]
        store_products(u.at[buf], base + l * SZ, ve[p - low, place[l]], w3, t3, c, l, 8)

    def gram_piece(k, piece):
        cols = slice(piece * K, (piece + 1) * K)
        left = jnp.concatenate([ve[BATCH * k + q - low, place[l]] for q in range(BATCH) for l in range(7)], axis=0)
        part = gram(left, u[k % 2, :, cols])
        if k == first and m_hbm is None:
            acc[:, cols] = part
        else:
            acc[:, cols] += part
        if k == last - 1:
            pltpu.make_async_copy(acc.at[:, cols], out_hbm.at[:, cols], sem_m.at[piece]).start()

    ready = min(low + 4, BATCH * last + 1)
    for p in range(low, ready):
        loads[p].wait()
    done = low
    for k in range(first, last):
        if k == first + 1:
            for p in range(ready, BATCH * last + 1):
                loads[p].wait()
            if m_hbm is not None:
                load_m.wait()
        elif last == first + 1:
            for p in range(ready, BATCH * last + 1):
                loads[p].wait()
        pieces = list(range(2)) if k > first else []
        for q in range(BATCH):
            p = BATCH * k + q
            while done <= p + 1:
                filter_plane(done)
                done += 1
            c = plane_weights(p)
            for l in range(7):
                make_products(p, l, c, k % 2, q * INNER)
                if pieces and (q * 7 + l) % 10 == 0:
                    gram_piece(k - 1, pieces.pop(0))
        while pieces:
            gram_piece(k - 1, pieces.pop(0))
    if m_hbm is not None and last == first + 1:
        load_m.wait()
    for piece in range(2):
        gram_piece(last - 1, piece)
    for piece in range(2):
        cols = slice(piece * K, (piece + 1) * K)
        pltpu.make_async_copy(acc.at[:, cols], out_hbm.at[:, cols], sem_m.at[piece]).wait()


def outer_kernel(
    odd_ref, m_hbm, v_hbm, vx_hbm, vy_hbm, hbm0, hbm1, hbm2, hbm3, hbmz, zf_ref, zh_ref, face_ref, mat_ref,
    keep_s, send_s, keep_m, send_m,
    v6, v7, v8, vp, zl, w78, t78, w06, t06, u, sem, acc, res, band0, band1, band2, band3, bandz,
):
    odd = odd_ref[0]
    bands = (band0, band1, band2)
    early = [
        pltpu.make_async_copy(hbmz, bandz, sem.at[14]),
        pltpu.make_async_copy(vy_hbm.at[pl.ds(17 * SZ, 64)], zl, sem.at[15]),
    ]
    loads = [
        pltpu.make_async_copy(hbm3, band3, sem.at[19]),
        pltpu.make_async_copy(v_hbm.at[pl.ds(0, 14), line_index(odd, 6)], v6, sem.at[0]),
        pltpu.make_async_copy(v_hbm.at[pl.ds(0, 14), line_index(odd, 7)], v7, sem.at[1]),
        pltpu.make_async_copy(vy_hbm.at[pl.ds(0, 17 * SZ)], v8, sem.at[2]),
    ]
    late = [pltpu.make_async_copy(v_hbm.at[pl.ds(14, 2)], vp.at[pl.ds(0, 2)], sem.at[3])]
    for y in range(SY):
        late.append(pltpu.make_async_copy(vx_hbm.at[pl.ds(y * SZ, SZ)], vp.at[2, y], sem.at[5 + y]))
    for n, (a, b) in enumerate(((hbm0, band0), (hbm1, band1), (hbm2, band2))):
        late.append(pltpu.make_async_copy(a, b, sem.at[16 + n]))
    load_m = pltpu.make_async_copy(m_hbm, acc, sem.at[13])
    place = [line_index(odd, c) for c in range(8)]
    for load in early + loads + [load_m] + late:
        load.start()
    for load in early:
        load.wait()
    wz, tz = apply_band(bandz[...], [zh_ref[...], zl[32:64]], FACE)
    kap_face, rho_face, kap_halo = face_ref[0], face_ref[1], face_ref[2]
    planes = lax.broadcasted_iota(jnp.int32, kap_halo.shape, 0)
    lines = lax.broadcasted_iota(jnp.int32, kap_halo.shape, 1)
    f = jnp.where(planes == SX, 0.0, 2.0 * kap_halo) + pltpu.roll(kap_halo, 1, 0) + pltpu.roll(kap_halo, 23, 0)
    f = jnp.where(planes <= SX, f, 0.0)
    f = jnp.where(lines == SY, 0.0, 2.0 * f) + pltpu.roll(f, 1, 1) + pltpu.roll(f, 127, 1)
    f = f * (1.0 / 32.0)
    kap_face = kap_face * (1.0 / 16.0)
    rho_face = rho_face * (1.0 / 216.0)

    def column(grid):
        parts = [jnp.broadcast_to(grid[:, l : l + 1], (24, K)) for l in range(9)]
        return jnp.concatenate(parts + [jnp.zeros((8, K), jnp.float32)], axis=0)

    zf = jnp.concatenate([zf_ref[...], zl[0:32]], axis=0)
    uz = jnp.concatenate([column(f) * zf.astype(jnp.float32) - column(kap_face) * wz, column(rho_face) * tz], axis=1)
    u[MAIN:] = uz.astype(jnp.bfloat16)
    for load in loads:
        load.wait()

    def line(p, l):
        if l == 8:
            return v8[p * SZ : (p + 1) * SZ]
        if p >= 14:
            return vp[p - 14, place[l]]
        return v7[p] if l == 7 else v6[p]

    def filter_near(p):
        for g, (ins, outs) in enumerate(NEAR):
            size = len(outs) * SZ
            a, b = apply_band(bands[g][...], [line(p, l) for l in ins], size)
            w06[p - 14, outs[0] * SZ : outs[0] * SZ + size] = a
            t06[p - 14, outs[0] * SZ : outs[0] * SZ + size] = b

    def filter_edge(p):
        a, b = apply_band(band3[...], [line(p, l) for l in EDGE[0]], OUTER)
        w78[p] = a
        t78[p] = b

    def along_x(ref, p, lo, hi, rows, mid):
        if p == hi:
            return ref[p - 1 - lo, rows]
        r = mid * ref[p - lo, rows] + ref[p + 1 - lo, rows]
        if p > 0:
            r = r + ref[p - 1 - lo, rows]
        return r

    yz = [kappa_yz(mat_ref[0, p]) for p in range(17)]
    def make_products(p):
        if p == 16:
            f = yz[15]
        else:
            f = 2.0 * yz[p] + yz[p + 1]
            if p:
                f = f + yz[p - 1]
        c = weights(mat_ref[0, p], mat_ref[1, p], f, p != 16)
        for l in range(0 if p >= 15 else 7, 9):
            if p < 15:
                row = p * OUTER + (l - 7) * SZ
            else:
                row = 15 * OUTER + (p - 15) * 9 * SZ + l * SZ
            if l >= 7:
                rows = slice((l - 7) * SZ, (l - 6) * SZ)
                w3 = along_x(w78, p, 0, 16, rows, 2.0)
                t3 = along_x(t78, p, 0, 16, rows, 4.0)
            else:
                rows = slice(l * SZ, (l + 1) * SZ)
                w3 = along_x(w06, p, 14, 16, rows, 2.0)
                t3 = along_x(t06, p, 14, 16, rows, 4.0)
            store_products(u, row, line(p, l), w3, t3, c, l, 16)

    filter_edge(0)
    for p in range(17):
        if p < 16:
            filter_edge(p + 1)
            if p + 1 >= 14:
                filter_near(p + 1)
        make_products(p)
        if p == 7:
            load_m.wait()
            for load in late:
                load.wait()
            left = jnp.concatenate([line(q, l) for q in range(8) for l in (7, 8)], axis=0)
            acc[...] += gram(left, u[: 8 * OUTER])
    rows = [line(p, l) for p in range(8, 17) for l in range(0 if p >= 15 else 7, 9)]
    left = jnp.concatenate(rows + [zf], axis=0)
    acc[...] += gram(left, u[8 * OUTER :])

    def put(i, j, half, s):
        res[i % 2, half, (i // 2) * 128 : (i // 2 + 1) * 128, j * 128 : (j + 1) * 128] = s

    for half in range(2):
        for i in range(4):
            for j in range(i, 4):
                a = acc[i * 128 : (i + 1) * 128, half * K + j * 128 : half * K + (j + 1) * 128]
                b = acc[j * 128 : (j + 1) * 128, half * K + i * 128 : half * K + (i + 1) * 128]
                s = a + b.T
                put(i, j, half, s)
                if i != j:
                    put(j, i, half, s.T)
    for core in range(2):

        @pl.when(odd == core)
        def _():
            keep_s[...] = res[core, 0]
            send_s[...] = res[1 - core, 0]
            keep_m[...] = res[core, 1]
            send_m[...] = res[1 - core, 1]


HBM = pl.BlockSpec(memory_space=pltpu.HBM)
VMEM = pl.BlockSpec(memory_space=pltpu.VMEM)
SMEM = pl.BlockSpec(memory_space=pltpu.SMEM)


def inner_part(first, last, odd, m, v, mat, bands):
    def body(odd_ref, *refs):
        if m is None:
            refs = (None,) + refs
        inner_kernel(first, last, odd_ref, *refs)

    planes = BATCH * (last - first) + (2 if first else 1)
    operands = (odd,) + (() if m is None else (m,)) + (v, mat) + tuple(bands)
    specs = [SMEM] + [HBM] * (len(operands) - 1)
    return pl.pallas_call(
        body,
        out_shape=pltpu.HBM((K, 2 * K), jnp.float32),
        in_specs=specs,
        out_specs=HBM,
        scratch_shapes=[
            pltpu.VMEM((planes, SY, SZ, K), jnp.bfloat16),
            pltpu.VMEM((4, INNER, K), jnp.float32),
            pltpu.VMEM((4, INNER, K), jnp.float32),
            pltpu.VMEM((2, BATCH * INNER, 2 * K), jnp.bfloat16),
            pltpu.VMEM((K, 2 * K), jnp.float32),
            pltpu.VMEM((2, SX, SY, SZ), jnp.float32),
            pltpu.VMEM((2, SX, SY, 128), jnp.float32),
            pltpu.VMEM((6 * SZ, 4 * SZ), jnp.bfloat16),
            pltpu.VMEM((6 * SZ, 5 * SZ), jnp.bfloat16),
            pltpu.VMEM((2 * SZ, 3 * SZ), jnp.bfloat16),
            pltpu.SemaphoreType.DMA((planes,)),
            pltpu.SemaphoreType.DMA((9,)),
        ],
        compiler_params=pltpu.CompilerParams(vmem_limit_bytes=26 * 1024 * 1024),
        cost_estimate=pl.CostEstimate(
            flops=1_800_000_000 * (last - first), transcendentals=0, bytes_accessed=2_000_000 * (last - first)
        ),
        name=f"inner{first}",
    )(*operands)


def outer_part(odd, m, v, vx, vy, bands, zf, zh, face, mat):
    return pl.pallas_call(
        outer_kernel,
        out_shape=[jax.ShapeDtypeStruct((K // 2, K), jnp.float32)] * 4,
        in_specs=[SMEM] + [HBM] * 9 + [VMEM] * 4,
        out_specs=[VMEM] * 4,
        scratch_shapes=[
            pltpu.VMEM((14, SZ, K), jnp.bfloat16),
            pltpu.VMEM((14, SZ, K), jnp.bfloat16),
            pltpu.VMEM((17 * SZ, K), jnp.bfloat16),
            pltpu.VMEM((3, SY, SZ, K), jnp.bfloat16),
            pltpu.VMEM((64, K), jnp.bfloat16),
            pltpu.VMEM((17, OUTER, K), jnp.float32),
            pltpu.VMEM((17, OUTER, K), jnp.float32),
            pltpu.VMEM((3, INNER, K), jnp.float32),
            pltpu.VMEM((3, INNER, K), jnp.float32),
            pltpu.VMEM((MAIN + FACE, 2 * K), jnp.bfloat16),
            pltpu.SemaphoreType.DMA((20,)),
            pltpu.VMEM((K, 2 * K), jnp.float32),
            pltpu.VMEM((2, 2, K // 2, K), jnp.float32),
            pltpu.VMEM((6 * SZ, 4 * SZ), jnp.bfloat16),
            pltpu.VMEM((6 * SZ, 5 * SZ), jnp.bfloat16),
            pltpu.VMEM((2 * SZ, 3 * SZ), jnp.bfloat16),
            pltpu.VMEM((4 * SZ, 3 * SZ), jnp.bfloat16),
            pltpu.VMEM((2 * FACE, FACE), jnp.bfloat16),
        ],
        compiler_params=pltpu.CompilerParams(vmem_limit_bytes=32 * 1024 * 1024),
        cost_estimate=pl.CostEstimate(flops=4_000_000_000, transcendentals=0, bytes_accessed=6_000_000),
        name="outer",
    )(odd, m, v, vx, vy, *bands, zf, zh, face, mat)


def pick(x, index, dim):
    return lax.dynamic_index_in_dim(x, index, dim, keepdims=False)


def reduce_to_owner(part):
    halves = [keep + send(other, lambda x, y, z: (x ^ 1, y, z)) for keep, other in (part[:2], part[2:])]
    groups = [[linear(x, y, z) for x in (c, c + 2) for y in range(NGY) for z in range(NGZ)] for c in range(2)]
    blocks = jnp.concatenate(halves, axis=1).reshape(64, 4, 2 * K)
    blocks = lax.all_to_all(blocks, ALL, 0, 0, tiled=True, axis_index_groups=groups)
    return jnp.sum(blocks, axis=0)


def to_parts(x):
    high = lax.reduce_precision(x, 8, 7)
    rest = x - high
    mid = lax.reduce_precision(rest, 8, 7)
    parts = jnp.concatenate([high, mid, rest - mid, jnp.zeros_like(x)], axis=1)
    return parts.astype(jnp.bfloat16)


def from_parts(rows):
    x = rows.astype(jnp.float32)
    return (x[:, 256:384] + x[:, 128:256]) + x[:, :128]


def face_rows(rows):
    return jnp.pad(rows.transpose(1, 0, 2), ((0, 0), (0, 7), (0, 0))).reshape(192, K)


def per_device(eigvecs, material):
    odd = lax.axis_index("gx") % 2 == 1
    upper = lax.axis_index("gz") == 1
    side = jnp.where(odd, SY - 1, 0)
    face = jnp.where(upper, 0, SZ - 1)
    odd_flag = odd.astype(jnp.int32).reshape(1)
    in_hbm = lambda x: pltpu.with_memory_space_constraint(x, pltpu.HBM)
    vectors = in_hbm(eigvecs)

    def chain(x, dim):
        return jnp.where(odd, lax.rev(x, (dim,)), x)

    zf = pick(eigvecs, face, 2)
    kface = lax.dynamic_slice(material, (0, 0, 0, face), (1, SX, SY, 1)).reshape(SX, SY)
    kface = jnp.pad(kface, ((0, 0), (0, 120)))
    zm = send(jnp.concatenate([zf.reshape(SX * SY, K), to_parts(kface)], axis=0), to_z)
    zm, odd_flag = lax.optimization_barrier((zm, odd_flag))
    bands = [in_hbm(band_matrix(ins, outs)) for ins, outs in NEAR]
    raw = in_hbm(material)
    zh = zm[: SX * SY].reshape(SX, SY, K)
    kz = from_parts(zm[SX * SY :])[:, :SY]
    lanes = jnp.arange(128)
    first = jnp.pad(material[:, 0], ((0, 0), (0, 0), (0, 128 - SZ)))
    first = jnp.stack([jnp.where(lanes == 64, kz[0][:, None], first[0]), first[1]])
    plane = eigvecs[0].reshape(SY * SZ, K)
    vx = send(jnp.concatenate([plane, zf[0], zh[0], to_parts(first.reshape(16, 128))], axis=0), to_x)
    m = inner_part(*PIECES[0], odd_flag, None, vectors, raw, bands)
    vx, m = lax.optimization_barrier((vx, m))
    at = SY * SZ
    xf, xz = vx[at : at + SY], vx[at + SY : at + 2 * SY]
    own = jnp.pad(material, ((0, 0), (0, 0), (0, 0), (0, 128 - SZ)))
    matz = jnp.stack([jnp.where(lanes == 64, kz[..., None], own[0]), own[1]])
    xmat = from_parts(vx[at + 2 * SY :]).reshape(2, 1, SY, 128)
    matz = chain(jnp.concatenate([matz, xmat], axis=1), 2)
    frows = chain(jnp.concatenate([zf, xf[None]], axis=0), 1)
    zrows = chain(jnp.concatenate([zh, xz[None]], axis=0), 1)
    lines = pick(eigvecs, side, 1).reshape(SX * SZ, K)
    xline = lax.dynamic_slice_in_dim(vx, side * SZ, SZ, 0)
    gap = jnp.zeros((15, K), jnp.bfloat16)
    parts = to_parts(matz[:, :, 0].reshape(34, 128))
    vy = send(jnp.concatenate([lines, xline, frows[:, 0], gap, zrows[:, 0], gap, parts], axis=0), to_y)
    zf = face_rows(frows)
    zh = face_rows(zrows)
    m = inner_part(*PIECES[1], odd_flag, in_hbm(m), vectors, raw, bands)
    vy, m, zf, zh = lax.optimization_barrier((vy, m, zf, zh))
    my = from_parts(vy[17 * SZ + 64 :]).reshape(2, 17, 1, 128)
    matz = jnp.concatenate([matz, my], axis=2)
    grids = jnp.stack([pick(matz[0], face, 2), pick(matz[1], face, 2), matz[0, :, :, 64]])
    grids = jnp.pad(grids, ((0, 0), (0, 7), (0, 119)))
    mat = jnp.pad(matz, ((0, 0), (0, 0), (0, 7), (0, 0)))
    mat = jnp.where(lanes < SZ, mat, 0.0)
    bands = bands + [in_hbm(band_matrix(*EDGE)), in_hbm(face_matrix())]
    part = outer_part(odd_flag, in_hbm(m), vectors, vx, vy, bands, zf, zh, grids, mat)
    total = SX * SY * SZ * NGX * NGY * NGZ
    summed = reduce_to_owner(part) * (0.5 / total)
    return summed[:, :K], summed[:, K:]


def solution(mesh):
    return jax.shard_map(
        per_device,
        mesh=mesh,
        in_specs=(P("gx", "gy", "gz", None), P(None, "gx", "gy", "gz")),
        out_specs=(P(ALL, None), P(ALL, None)),
        check_vma=False,
    )
```
